32 devices in a mesh: seq: 8 (over z, core), tp: 4 (over y, x).
Axes of the slice: x: 2, y: 2, z: 4, core: 2. Of those that a mesh axis runs over, the one named last changes fastest.
Arguments:
- tokens: bfloat16 [2048, 4608], P('seq', 'tp'), may hold values from -6 to 6
- attention_gain: float32 [4608], replicated, may hold values from 0.25 to 1.75
- query_weight: bfloat16 [4608, 4096], P(None, 'tp'), may hold values from -0.09375 to 0.09375
- key_weight: bfloat16 [4608, 2048], P(None, 'tp'), may hold values from -0.09375 to 0.09375
- value_weight: bfloat16 [4608, 2048], P(None, 'tp'), may hold values from -0.09375 to 0.09375
- output_weight: bfloat16 [4096, 4608], P('tp'), may hold values from -0.09375 to 0.09375
- post_gain: float32 [4608], replicated, may hold values from 0.25 to 1.75
- local_gain: float32 [4608], replicated, may hold values from 0.25 to 1.75
- local_query_weight: bfloat16 [4608, 4096], P(None, 'tp'), may hold values from -0.09375 to 0.09375
- local_key_weight: bfloat16 [4608, 2048], P(None, 'tp'), may hold values from -0.09375 to 0.09375
- local_value_weight: bfloat16 [4608, 2048], P(None, 'tp'), may hold values from -0.09375 to 0.09375
Outputs:
- hidden: bfloat16 [2048, 4608], P('seq', 'tp')
- local_heads: bfloat16 [2048, 4096], P('seq', 'tp')
The draws below stay inside these ranges and needn't reach their ends.
All inputs are finite; a program needn't handle non-finite values.
Results may differ from the reference program's by a relative error of at most 0.02.
Values may be sent and summed in bfloat16 or wider, within the bound.
A program may use at most 128 MiB of HBM per device.

```python
import jax
import jax.numpy as jnp
from jax import lax

D = 4608
HEADS = 32
KV_HEADS = 16
HEAD_DIM = 128
WINDOW = 128
TOKENS = 2048


def block_scale(stream_key, dims, shards, least, largest):
    level, own = 1.0, jax.random.fold_in(stream_key, 6)
    for dim, blocks in shards:
        heights = jnp.exp(jax.random.uniform(jax.random.fold_in(own, dim), (blocks,), jnp.float32, least / len(shards), largest / len(shards)))
        level = level * jnp.repeat(heights, dims[dim] // blocks).reshape([-1 if axis == dim else 1 for axis in range(len(dims))])
    return level


def centred(rng, dims, deviation, bound, shards=(), held_as=jnp.bfloat16):
    values = jax.random.normal(rng, dims, jnp.float32) * deviation
    if len(shards) > 0:
        values = block_scale(rng, dims, shards, -0.22, 0.18) * values
    return jnp.clip(values, min=-bound, max=bound).astype(held_as)


def setup_inputs(seed: int = 0) -> dict:
    arg_keys = jax.random.split(jax.random.key(seed), 12)
    return {
        "tokens": centred(arg_keys[0], (TOKENS, D), 1.0, 6.0, ((0, 8), (1, 4))),
        "attention_gain": jnp.clip(1.0 + 0.15 * jax.random.normal(arg_keys[1], (D,), jnp.float32), 0.25, 1.75),
        "query_weight": centred(arg_keys[2], (D, HEADS * HEAD_DIM), D ** -0.5, 0.09375, ((1, 4),)),
        "key_weight": centred(arg_keys[3], (D, KV_HEADS * HEAD_DIM), D ** -0.5, 0.09375, ((1, 4),)),
        "value_weight": centred(arg_keys[4], (D, KV_HEADS * HEAD_DIM), D ** -0.5, 0.09375, ((1, 4),)),
        "output_weight": centred(arg_keys[5], (HEADS * HEAD_DIM, D), (HEADS * HEAD_DIM) ** -0.5, 0.09375, ((0, 4),)),
        "post_gain": jnp.clip(1.0 + 0.15 * jax.random.normal(arg_keys[6], (D,), jnp.float32), 0.25, 1.75),
        "local_gain": jnp.clip(1.0 + 0.15 * jax.random.normal(arg_keys[7], (D,), jnp.float32), 0.25, 1.75),
        "local_query_weight": centred(arg_keys[8], (D, HEADS * HEAD_DIM), D ** -0.5, 0.09375, ((1, 4),)),
        "local_key_weight": centred(arg_keys[9], (D, KV_HEADS * HEAD_DIM), D ** -0.5, 0.09375, ((1, 4),)),
        "local_value_weight": centred(arg_keys[10], (D, KV_HEADS * HEAD_DIM), D ** -0.5, 0.09375, ((1, 4),)),
    }


SOFT_CAP = 50.0
NORM_EPS = 1e-06

def rms_scaled(values, weights):
    widened = values.astype(jnp.float32)
    factor = lax.rsqrt(lax.optimization_barrier(jnp.mean(widened * widened, axis=-1, keepdims=True)) + NORM_EPS)
    return widened * factor * weights.astype(jnp.float32)

def rotate(vectors, places):
    head_size = vectors.shape[-1]
    halfway = head_size // 2
    exponents = jnp.arange(halfway, dtype=jnp.float32) * (2.0 / head_size)
    frequency = jnp.power(jnp.float32(10000.0), -exponents)
    angles = places.astype(jnp.float32)[:, None] * frequency[None, :]
    cosine_part = jnp.cos(angles)[:, None, :]
    sine_part = jnp.sin(angles)[:, None, :]
    first_half = vectors[..., :halfway]
    second_half = vectors[..., halfway:]
    return jnp.concatenate([first_half * cosine_part - second_half * sine_part, second_half * cosine_part + first_half * sine_part], axis=-1)

def project_heads(normed, weight_query, weight_key, weight_value, places):
    row_count = normed.shape[0]
    queries = jnp.dot(normed, weight_query, preferred_element_type=jnp.float32).reshape(row_count, -1, HEAD_DIM)
    key_heads = jnp.dot(normed, weight_key, preferred_element_type=jnp.float32).reshape(row_count, -1, HEAD_DIM)
    value_heads = jnp.dot(normed, weight_value, preferred_element_type=jnp.float32).reshape(row_count, -1, HEAD_DIM)
    return (rotate(queries, places).astype(jnp.bfloat16), rotate(key_heads, places).astype(jnp.bfloat16), value_heads.astype(jnp.bfloat16))

def attention(queries, key_heads, value_heads, window_size):
    row_count = queries.shape[0]
    groups = HEADS // KV_HEADS
    grouped = jnp.transpose(queries.reshape(row_count, KV_HEADS, groups, HEAD_DIM), (1, 0, 2, 3))
    keys_first = jnp.transpose(key_heads, (1, 0, 2))
    values_first = jnp.transpose(value_heads, (1, 0, 2))
    places = jnp.arange(row_count, dtype=jnp.int32)
    offset = places[:, None] - places[None, :]
    allowed = (offset >= 0) & (offset < window_size)
    scale = float(D // HEADS) ** (-0.5)

    def one_head(operands):
        query_block, key_block, value_block = operands
        scores = jnp.einsum('qrd,kd->rqk', query_block.astype(jnp.float32), key_block.astype(jnp.float32)) * scale
        scores = SOFT_CAP * jnp.tanh(scores / SOFT_CAP)
        weights = jnp.where(allowed[None], jnp.exp(scores), jnp.float32(0.0))
        denominator = lax.optimization_barrier(jnp.sum(weights, axis=-1))
        probs = weights.astype(jnp.bfloat16)
        numerator = jnp.einsum('rqk,kd->qrd', probs.astype(jnp.float32), value_block.astype(jnp.float32))
        return (numerator / jnp.transpose(denominator)[:, :, None]).astype(jnp.bfloat16)
    stacked = lax.map(one_head, (grouped, keys_first, values_first))
    return jnp.transpose(stacked, (1, 0, 2, 3)).reshape(row_count, HEADS * HEAD_DIM)

def reference(tokens, attention_gain, query_weight, key_weight, value_weight, output_weight, post_gain, local_gain, local_query_weight, local_key_weight, local_value_weight):
    places = jnp.arange(TOKENS, dtype=jnp.int32)
    normed = rms_scaled(tokens, attention_gain).astype(jnp.bfloat16)
    queries, key_heads, value_heads = project_heads(normed, query_weight, key_weight, value_weight, places)
    attended = attention(queries, key_heads, value_heads, TOKENS)
    projected = jnp.dot(attended, output_weight, preferred_element_type=jnp.float32)
    hidden = (tokens.astype(jnp.float32) + rms_scaled(projected, post_gain)).astype(jnp.bfloat16)
    local_normed = rms_scaled(hidden, local_gain).astype(jnp.bfloat16)
    local_queries, local_keys, local_values = project_heads(local_normed, local_query_weight, local_key_weight, local_value_weight, places)
    local_heads = attention(local_queries, local_keys, local_values, WINDOW)
    return (hidden, local_heads)
```

```python
import functools
import math

import jax
import jax.numpy as jnp
from jax import lax
from jax.experimental import pallas as pl
from jax.experimental.pallas import tpu as pltpu
from jax.sharding import PartitionSpec as P

D = 4608
HEADS = 32
HEAD_DIM = 128
WINDOW = 128

SOFT_CAP = 50.0
NORM_EPS = 1e-06
MESH = pl.DeviceIdType.MESH
VMEM = pltpu.VMEM
F32 = jnp.float32
BF16 = jnp.bfloat16
PARTS = 4
INNER = float(D // HEADS) ** (-0.5) / SOFT_CAP
OUTER = SOFT_CAP * math.log2(math.e)


def greet(peers):
    barrier = pltpu.get_barrier_semaphore()
    for peer in peers:
        pl.semaphore_signal(barrier, inc=1, device_id=peer, device_id_type=MESH)
    pl.semaphore_wait(barrier, len(peers))


def remote(source, target, send_sem, recv_sem, device):
    return pltpu.make_async_remote_copy(
        src_ref=source,
        dst_ref=target,
        send_sem=send_sem,
        recv_sem=recv_sem,
        device_id=device,
        device_id_type=MESH,
    )


def xor(index, bits):
    low, high = index % 2, index // 2
    if bits & 1:
        low = 1 - low
    if bits & 2:
        high = 1 - high
    return high * 2 + low


def attend(q_ref, keys, values, acc, lsum, h, group, allowed, first, row_span=None):
    q = q_ref[pl.ds(h * group, group)]
    if row_span is not None:
        q = q[:, row_span[0] : row_span[1]]
    rows = q.shape[1]
    q = q.reshape(group * rows, HEAD_DIM)
    scores = lax.dot_general(q, keys, (((1,), (1,)), ((), ())), preferred_element_type=F32)
    weights = jnp.exp2(jnp.tanh(scores * INNER) * OUTER)
    if allowed is not None:
        count = keys.shape[0]
        row = lax.broadcasted_iota(jnp.int32, (rows, count), 0)
        col = lax.broadcasted_iota(jnp.int32, (rows, count), 1)
        mask = allowed(row, col)
        weights = jnp.concatenate(
            [jnp.where(mask, weights[g * rows : (g + 1) * rows], 0.0) for g in range(group)], axis=0
        )
    lanes = weights[:, :HEAD_DIM]
    for begin in range(HEAD_DIM, keys.shape[0], HEAD_DIM):
        lanes = lanes + weights[:, begin : begin + HEAD_DIM]
    product = jnp.dot(weights.astype(BF16), values, preferred_element_type=F32)
    lanes = lanes.reshape(group, rows, HEAD_DIM)
    product = product.reshape(group, rows, HEAD_DIM)
    heads = pl.ds(h * group, group)
    span = pl.ds(0, rows)
    if first:
        lsum[heads, span] = lanes
        acc[heads, span] = product
    else:
        lsum[heads, span] += lanes
        acc[heads, span] += product


def write_heads(o_ref, acc, lsum):
    for h in range(acc.shape[0]):
        denominator = jnp.sum(lsum[h], axis=-1, keepdims=True)
        o_ref[:, h * HEAD_DIM : (h + 1) * HEAD_DIM] = (acc[h] / denominator).astype(BF16)


def causal_kernel(levels, q_ref, kv_ref, o_ref, buf, acc, lsum, up_sem, side_sem, recv):
    s = lax.axis_index("seq")
    z, c = s // 2, s % 2
    mate = s + 1 - 2 * c
    kv_heads = kv_ref.shape[1]
    group = q_ref.shape[0] // kv_heads
    has_up, has_down = z < levels - 1, z > 0

    barrier = pltpu.get_barrier_semaphore()
    pl.semaphore_signal(barrier, inc=1, device_id={"seq": mate}, device_id_type=MESH)

    @pl.when(has_up)
    def _():
        pl.semaphore_signal(barrier, inc=1, device_id={"seq": s + 2}, device_id_type=MESH)

    @pl.when(has_down)
    def _():
        pl.semaphore_signal(barrier, inc=1, device_id={"seq": s - 2}, device_id_type=MESH)

    pl.semaphore_wait(barrier, 1 + has_up.astype(jnp.int32) + has_down.astype(jnp.int32))

    def up(owner, source):
        return remote(source, buf.at[owner], up_sem.at[owner], recv.at[owner], {"seq": s + 2})

    def side(owner, source):
        return remote(source, buf.at[owner], side_sem.at[owner], recv.at[owner], {"seq": mate})

    @pl.when(has_up)
    def _():
        up(s, kv_ref).start()

    @pl.when(c == 0)
    def _():
        side(s, kv_ref).start()

    def own(h, carry):
        attend(
            q_ref, kv_ref[0, h], kv_ref[1, h], acc, lsum, h, group,
            lambda row, col: col <= row, True,
        )
        return carry

    lax.fori_loop(0, kv_heads, own, 0)

    def visit(owner):
        def body(h, carry):
            attend(
                q_ref, buf[owner, 0, h], buf[owner, 1, h], acc, lsum, h, group, None, False
            )
            return carry

        lax.fori_loop(0, kv_heads, body, 0)

    @pl.when(c == 1)
    def _():
        side(s - 1, buf.at[s - 1]).wait_recv()
        visit(s - 1)

    def level(k, carry):
        owner, other = s - 2 * k, mate - 2 * k
        up(owner, buf.at[owner]).wait_recv()

        @pl.when(has_up)
        def _():
            up(owner, buf.at[owner]).start()

        side(owner, buf.at[owner]).start()
        visit(owner)
        side(other, buf.at[other]).wait_recv()
        visit(other)
        return carry

    lax.fori_loop(1, z + 1, level, 0)
    write_heads(o_ref, acc, lsum)

    @pl.when(has_up)
    def _():
        up(s, kv_ref).wait_send()

    @pl.when(c == 0)
    def _():
        side(s, kv_ref).wait_send()

    def drain(k, carry):
        owner = s - 2 * k

        @pl.when(has_up)
        def _():
            up(owner, buf.at[owner]).wait_send()

        side(owner, buf.at[owner]).wait_send()
        return carry

    lax.fori_loop(1, z + 1, drain, 0)


def causal_attention(q, kv, count, collective_id):
    heads, rows, _ = q.shape
    vmem = pl.BlockSpec(memory_space=VMEM)
    return pl.pallas_call(
        functools.partial(causal_kernel, count // 2),
        out_shape=jax.ShapeDtypeStruct((rows, heads * HEAD_DIM), BF16),
        in_specs=[vmem] * 2,
        out_specs=vmem,
        scratch_shapes=[
            VMEM((count,) + kv.shape, BF16),
            VMEM(q.shape, F32),
            VMEM(q.shape, F32),
            pltpu.SemaphoreType.DMA((count,)),
            pltpu.SemaphoreType.DMA((count,)),
            pltpu.SemaphoreType.DMA((count,)),
        ],
        compiler_params=pltpu.CompilerParams(
            collective_id=collective_id, has_side_effects=True, vmem_limit_bytes=32 * 2**20
        ),
        name="causal_attention",
    )(q, kv)


def window_kernel(count, q_ref, kv_ref, o_ref, tail, acc, lsum, send, recv):
    s = lax.axis_index("seq")
    kv_heads, rows = kv_ref.shape[1], kv_ref.shape[2]
    group = q_ref.shape[0] // kv_heads
    has_next, has_last = s < count - 1, s > 0
    barrier = pltpu.get_barrier_semaphore()

    @pl.when(has_next)
    def _():
        pl.semaphore_signal(barrier, inc=1, device_id={"seq": s + 1}, device_id_type=MESH)

    @pl.when(has_last)
    def _():
        pl.semaphore_signal(barrier, inc=1, device_id={"seq": s - 1}, device_id_type=MESH)

    pl.semaphore_wait(barrier, has_next.astype(jnp.int32) + has_last.astype(jnp.int32))
    copy = remote(
        kv_ref.at[:, :, pl.ds(rows - WINDOW, WINDOW), :], tail, send.at[0], recv.at[0],
        {"seq": s + 1},
    )

    @pl.when(has_next)
    def _():
        copy.start()

    def own(h, carry):
        attend(
            q_ref, kv_ref[0, h], kv_ref[1, h], acc, lsum, h, group,
            lambda row, col: (col <= row) & (row - col < WINDOW), True,
        )
        return carry

    lax.fori_loop(0, kv_heads, own, 0)

    @pl.when(has_last)
    def _():
        copy.wait_recv()

        def body(h, carry):
            attend(
                q_ref, tail[0, h], tail[1, h], acc, lsum, h, group,
                lambda row, col: col > row, False, (0, WINDOW),
            )
            return carry

        lax.fori_loop(0, kv_heads, body, 0)

    write_heads(o_ref, acc, lsum)

    @pl.when(has_next)
    def _():
        copy.wait_send()


def window_attention(q, kv, count, collective_id):
    heads, rows, _ = q.shape
    vmem = pl.BlockSpec(memory_space=VMEM)
    return pl.pallas_call(
        functools.partial(window_kernel, count),
        out_shape=jax.ShapeDtypeStruct((rows, heads * HEAD_DIM), BF16),
        in_specs=[vmem] * 2,
        out_specs=vmem,
        scratch_shapes=[
            VMEM((2, kv.shape[1], WINDOW, HEAD_DIM), BF16),
            VMEM(q.shape, F32),
            VMEM(q.shape, F32),
            pltpu.SemaphoreType.DMA((1,)),
            pltpu.SemaphoreType.DMA((1,)),
        ],
        compiler_params=pltpu.CompilerParams(
            collective_id=collective_id, has_side_effects=True, vmem_limit_bytes=24 * 2**20
        ),
        name="window_attention",
    )(q, kv)


def fused_kernel(
    levels, heads, kv_heads,
    x_hbm, gain1_hbm, gain2_hbm, gain3_hbm, cos_ref, sin_ref,
    wq_hbm, wk_hbm, wv_hbm, wo_hbm, lwq_hbm, lwk_hbm, lwv_hbm,
    hidden_ref, o_ref,
    buf, w, wo, gains, xg, acc, ss, q_all, kv_buf, out, lsum, att,
    terms, own, landed, passed, proj, mine, stats, kv2,
    x_sem, gain_sem, w_sem, wo_sem, ag_send, ag_recv, up_sem, side_sem, kv_sem,
    rs_send, rs_recv, st_send, st_recv, tail_sem,
):
    me = lax.axis_index("tp")
    s = lax.axis_index("seq")
    z, c = s // 2, s % 2
    mate = s + 1 - 2 * c
    has_up, has_down = z < levels - 1, z > 0
    next_row, prev_row = s < 2 * levels - 1, s > 0
    rows, cols = hidden_ref.shape
    chunk_rows, half_rows = rows // PARTS, rows // PARTS // 2
    block, half = rows // 2, rows // 4
    chunks = cols // HEAD_DIM
    owners = [xor(me, bits) for bits in range(4)]
    peers = [{"tp": owner} for owner in owners]
    along_x, along_y = peers[1], peers[2]
    qc, kc = heads * HEAD_DIM, kv_heads * HEAD_DIM
    kvc = 2 * kc
    group = heads // kv_heads

    x_loads = []
    for part in range(PARTS):
        span = pl.ds(part * chunk_rows, chunk_rows)
        copy = pltpu.make_async_copy(x_hbm.at[span], buf.at[0, span], x_sem.at[part])
        copy.start()
        x_loads.append(copy)
    gain_loads = []
    for i, ref in enumerate((gain1_hbm, gain2_hbm, gain3_hbm)):
        copy = pltpu.make_async_copy(ref, gains.at[i], gain_sem.at[i])
        copy.start()
        gain_loads.append(copy)

    def weight_loads(key, value, query):
        loads = []
        for slot in range(4):
            span = pl.ds(pl.multiple_of(owners[slot] * cols, cols), cols)
            spec = ((key, 0, kc), (value, kc, kc), (query, kvc, qc))
            loads.append(
                [
                    pltpu.make_async_copy(
                        ref.at[span, :], w.at[slot, :, pl.ds(begin, width)], w_sem.at[slot, i]
                    )
                    for i, (ref, begin, width) in enumerate(spec)
                ]
            )
        return loads

    first_loads = weight_loads(wk_hbm, wv_hbm, wq_hbm)
    for bundle in first_loads:
        for copy in bundle:
            copy.start()
    wo_loads = []
    for bits in (3, 1, 2, 0):
        span = pl.ds(pl.multiple_of(owners[bits] * cols, cols), cols)
        copy = pltpu.make_async_copy(wo_hbm.at[:, span], wo.at[bits], wo_sem.at[bits])
        copy.start()
        wo_loads.append(copy)

    barrier = pltpu.get_barrier_semaphore()
    for peer in (*peers[1:], {"seq": mate}):
        pl.semaphore_signal(barrier, inc=1, device_id=peer, device_id_type=MESH)

    @pl.when(has_up)
    def _():
        pl.semaphore_signal(barrier, inc=1, device_id={"seq": s + 2}, device_id_type=MESH)

    @pl.when(has_down)
    def _():
        pl.semaphore_signal(barrier, inc=1, device_id={"seq": s - 2}, device_id_type=MESH)

    @pl.when(has_up & (c == 1))
    def _():
        pl.semaphore_signal(barrier, inc=1, device_id={"seq": s + 1}, device_id_type=MESH)

    @pl.when(has_down & (c == 0))
    def _():
        pl.semaphore_signal(barrier, inc=1, device_id={"seq": s - 1}, device_id_type=MESH)

    far = (has_up & (c == 1)) | (has_down & (c == 0))
    pl.semaphore_wait(
        barrier,
        4 + has_up.astype(jnp.int32) + has_down.astype(jnp.int32) + far.astype(jnp.int32),
    )

    def gather_moves(store, first, count, part, base):
        begin = pl.multiple_of(part * count, count)
        top, bottom = pl.ds(begin, count // 2), pl.ds(begin + count // 2, count // 2)
        spec = (
            (store.at[0, top], store.at[1, top], along_x),
            (store.at[0, bottom], store.at[2, bottom], along_y),
            (store.at[0, bottom], store.at[1, bottom], along_x),
            (store.at[0, top], store.at[2, top], along_y),
            (store.at[1, top], store.at[3, top], along_y),
            (store.at[2, bottom], store.at[3, bottom], along_x),
        )
        at = first + part * 6 + base
        return [
            remote(source, target, ag_send.at[at + i], ag_recv.at[at + i], device)
            for i, (source, target, device) in enumerate(spec)
        ]

    def moves(part):
        return gather_moves(buf, 0, chunk_rows, part, 0)

    def moves2(part):
        return gather_moves(proj, 6 * PARTS, block, part, 0)

    def kv_part(owner, part):
        return kv_buf.at[owner, :, :, pl.ds(pl.multiple_of(part * chunk_rows, chunk_rows), chunk_rows)]

    def up(owner, part):
        at, ref = owner * PARTS + part, kv_part(owner, part)
        return remote(ref, ref, up_sem.at[at], kv_sem.at[at], {"seq": s + 2})

    def side(owner, part):
        at, ref = owner * PARTS + part, kv_part(owner, part)
        return remote(ref, ref, side_sem.at[at], kv_sem.at[at], {"seq": mate})

    def arrive(owner, part):
        up(owner, part).wait_recv()

        @pl.when(has_up)
        def _():
            up(owner, part).start()

        side(owner, part).start()

    def multiply(slot, count, begin, width, fresh):
        product = jnp.dot(
            xg[0:count, :], w[slot, :, begin : begin + width], preferred_element_type=F32
        )
        if fresh:
            acc[0:count, begin : begin + width] = product
        else:
            acc[0:count, begin : begin + width] += product

    def gain_row(which, slot, j):
        return gains[which, pl.ds(owners[slot] * chunks + j, 1), :]

    def prepare(slot, part):
        here = pl.ds(pl.multiple_of(part * chunk_rows, chunk_rows), chunk_rows)
        squares = None
        for j in range(chunks):
            lanes = slice(j * HEAD_DIM, (j + 1) * HEAD_DIM)
            wide = buf[slot, here, lanes].astype(F32)
            squares = wide * wide if squares is None else squares + wide * wide
            xg[0:chunk_rows, lanes] = (wide * gain_row(0, slot, j)).astype(BF16)
        if slot == 0:
            ss[0:chunk_rows, :] = squares
        else:
            ss[0:chunk_rows, :] += squares

    def row_factor(count):
        total = jnp.sum(ss[0:count, :], axis=-1, keepdims=True)
        return lax.rsqrt(jnp.broadcast_to(total, (count, HEAD_DIM)) * (1.0 / D) + NORM_EPS)

    def rotated(begin, count, factor, span):
        u = acc[0:count, begin : begin + HEAD_DIM] * factor
        turned = pltpu.roll(u, HEAD_DIM // 2, 1)
        return (u * cos_ref[span, :] + turned * sin_ref[span, :]).astype(BF16)

    for copy in x_loads[:1]:
        copy.wait()
    for copy in moves(0)[:4]:
        copy.start()
    for copy in x_loads[1:]:
        copy.wait()
    for copy in gain_loads:
        copy.wait()

    def first_part(part, carry):
        def take(slot):
            prepare(slot, part)

            @pl.when(part == 0)
            def _():
                for copy in first_loads[slot]:
                    copy.wait()

            multiply(slot, chunk_rows, 0, kvc, slot == 0)

        sends = moves(part)
        take(0)
        multiply(0, chunk_rows, kvc, qc, True)
        sends[0].wait_recv()
        sends[4].start()
        sends[1].wait_recv()
        sends[5].start()

        @pl.when(part < PARTS - 1)
        def _():
            for copy in moves(part + 1)[:4]:
                copy.start()

        sends[2].wait_recv()
        take(1)
        multiply(1, chunk_rows, kvc, qc, False)
        sends[3].wait_recv()
        take(2)
        multiply(2, chunk_rows, kvc, qc, False)

        def forward(k, carry):
            @pl.when(part >= k)
            def _():
                arrive(s - 2 * k, part - k)

            return carry

        @pl.when(has_up)
        def _():
            lax.fori_loop(1, z + 1, forward, 0)

        sends[4].wait_recv()
        sends[5].wait_recv()
        take(3)
        span = pl.ds(pl.multiple_of(part * chunk_rows, chunk_rows), chunk_rows)
        factor = row_factor(chunk_rows)
        for h in range(kv_heads):
            kv_buf[s, 0, h, span, :] = rotated(h * HEAD_DIM, chunk_rows, factor, span)
            place = kc + h * HEAD_DIM
            kv_buf[s, 1, h, span, :] = (
                acc[0:chunk_rows, place : place + HEAD_DIM] * factor
            ).astype(BF16)

        @pl.when(has_up)
        def _():
            up(s, part).start()

        @pl.when(c == 0)
        def _():
            side(s, part).start()

        multiply(3, chunk_rows, kvc, qc, False)
        for h in range(heads):
            q_all[h, span, :] = rotated(kvc + h * HEAD_DIM, chunk_rows, factor, span)
        return carry

    lax.fori_loop(0, PARTS, first_part, 0)

    second_loads = weight_loads(lwk_hbm, lwv_hbm, lwq_hbm)
    for bundle in second_loads:
        for copy in bundle:
            copy.start()

    for h in range(kv_heads):
        attend(
            q_all, kv_buf[s, 0, h], kv_buf[s, 1, h], out, lsum, h, group,
            lambda row, col: col <= row, True,
        )

    def visit(owner):
        for h in range(kv_heads):
            attend(
                q_all, kv_buf[owner, 0, h], kv_buf[owner, 1, h], out, lsum, h, group, None, False
            )

    @pl.when(c == 1)
    def _():
        for part in range(PARTS):
            side(s - 1, part).wait_recv()
        visit(s - 1)

    def turn(r, carry):
        def level(k, carry):
            part = r - k

            @pl.when((part >= 0) & (part < PARTS))
            def _():
                owner, other = s - 2 * k, mate - 2 * k

                @pl.when((r >= PARTS) | (z == levels - 1))
                def _():
                    arrive(owner, part)

                @pl.when(part == PARTS - 1)
                def _():
                    def both(j, carry):
                        @pl.when(j == 1)
                        def _():
                            for p in range(PARTS):
                                side(other, p).wait_recv()

                        visit(owner + j * (other - owner))
                        return carry

                    lax.fori_loop(0, 2, both, 0)

            return carry

        lax.fori_loop(1, z + 1, level, 0)
        return carry

    lax.fori_loop(1, PARTS + z, turn, 0)
    write_heads(att, out, lsum)

    def reduce_moves(part):
        base = part * block
        top, bottom = pl.ds(base, half), pl.ds(base + half, half)
        spec = (
            (terms.at[2, top], along_x),
            (terms.at[2, bottom], along_y),
            (terms.at[0, top], along_x),
            (terms.at[1, bottom], along_y),
            (passed.at[part, 1], along_x),
            (passed.at[part, 0], along_y),
        )
        return [
            remote(
                source, landed.at[part, i], rs_send.at[part * 6 + i], rs_recv.at[part * 6 + i], device
            )
            for i, (source, device) in enumerate(spec)
        ]

    def product(bits, part):
        span = slice(part * block, (part + 1) * block)
        value = jnp.dot(att[span, :], wo[bits], preferred_element_type=F32)
        if bits == 0:
            own[span, :] = value
        else:
            terms[bits - 1, span, :] = value.astype(BF16)

    def pass_on(part):
        copies = reduce_moves(part)
        base = part * block
        copies[0].wait_recv()
        passed[part, 0] = (
            terms[1, base : base + half].astype(F32) + landed[part, 0].astype(F32)
        ).astype(BF16)
        copies[5].start()
        copies[1].wait_recv()
        passed[part, 1] = (
            terms[0, base + half : base + block].astype(F32) + landed[part, 1].astype(F32)
        ).astype(BF16)
        copies[4].start()

    ones = jnp.ones((8, HEAD_DIM), F32)
    highest = lax.Precision.HIGHEST

    def swaps(part):
        return [
            remote(
                mine.at[part], stats.at[part, bits - 1],
                st_send.at[part * 3 + bits - 1], st_recv.at[part * 3 + bits - 1], peers[bits],
            )
            for bits in (3, 1, 2)
        ]

    def finalize(part):
        copies = reduce_moves(part)
        for i in (2, 3, 5, 4):
            copies[i].wait_recv()
        base = part * block
        span = slice(base, base + block)
        lanes = None
        for j in range(chunks):
            cut = slice(j * HEAD_DIM, (j + 1) * HEAD_DIM)
            above = landed[part, 2, :, cut].astype(F32) + landed[part, 5, :, cut].astype(F32)
            below = landed[part, 3, :, cut].astype(F32) + landed[part, 4, :, cut].astype(F32)
            value = own[span, cut] + jnp.concatenate([above, below], axis=0)
            own[span, cut] = value
            proj[0, span, cut] = value.astype(BF16)
            lanes = value * value if lanes is None else lanes + value * value
        for copy in moves2(part)[:2]:
            copy.start()
        mine[part] = lax.dot_general(
            ones, lanes, (((1,), (1,)), ((), ())), precision=highest, preferred_element_type=F32
        )
        for swap in swaps(part):
            swap.start()
        for copy in moves2(part)[2:4]:
            copy.start()

    def forward_rows(part):
        copies = moves2(part)
        copies[0].wait_recv()
        copies[4].start()
        copies[1].wait_recv()
        copies[5].start()

    def post_factor(part):
        for swap in swaps(part):
            swap.wait_recv()
        summed = mine[part] + stats[part, 0] + stats[part, 1] + stats[part, 2]
        column = lax.dot_general(
            summed, ones * 0.125, (((0,), (0,)), ((), ())), precision=highest,
            preferred_element_type=F32,
        )
        return lax.rsqrt(column * (1.0 / D) + NORM_EPS)

    def take2(slot, part, factor):
        span = slice(part * block, (part + 1) * block)
        squares = None
        for j in range(chunks):
            cut = slice(j * HEAD_DIM, (j + 1) * HEAD_DIM)
            summed = own[span, cut] if slot == 0 else proj[slot, span, cut].astype(F32)
            added = buf[slot, span, cut].astype(F32) + summed * factor * gain_row(1, slot, j)
            rounded = added.astype(BF16)
            if slot == 0:
                hidden_ref[span, cut] = rounded
            wide = rounded.astype(F32)
            squares = wide * wide if squares is None else squares + wide * wide
            xg[:, cut] = (wide * gain_row(2, slot, j)).astype(BF16)
        if slot == 0:
            ss[...] = squares
        else:
            ss[...] += squares
        if part == 1:
            for copy in second_loads[slot]:
                copy.wait()
        multiply(slot, block, 0, kvc, slot == 0)
        multiply(slot, block, kvc, qc, slot == 0)

    def finish2(part):
        span = pl.ds(part * block, block)
        place_rows = pl.ds(WINDOW + part * block, block)
        factor = row_factor(block)
        for h in range(kv_heads):
            kv2[0, h, place_rows, :] = rotated(h * HEAD_DIM, block, factor, span)
            place = kc + h * HEAD_DIM
            kv2[1, h, place_rows, :] = (acc[:, place : place + HEAD_DIM] * factor).astype(BF16)
        for h in range(heads):
            q_all[h, span, :] = rotated(kvc + h * HEAD_DIM, block, factor, span)

    tail = remote(
        kv2.at[:, :, pl.ds(rows, WINDOW)], kv2.at[:, :, pl.ds(0, WINDOW)],
        tail_sem.at[0], tail_sem.at[1], {"seq": s + 1},
    )

    for copy in wo_loads:
        copy.wait()
    late, soon = 0, 1
    copies = reduce_moves(soon)
    product(3, soon)
    copies[0].start()
    copies[1].start()
    product(1, soon)
    copies[2].start()
    product(2, soon)
    copies[3].start()
    product(0, soon)
    for bits in (3, 1, 2, 0):
        product(bits, late)
    pass_on(soon)
    for copy in reduce_moves(late)[:4]:
        copy.start()
    finalize(soon)
    pass_on(late)
    factor = post_factor(soon)
    take2(0, soon, factor)
    forward_rows(soon)
    moves2(soon)[2].wait_recv()
    take2(1, soon, factor)
    moves2(soon)[3].wait_recv()
    take2(2, soon, factor)
    finalize(late)
    moves2(soon)[4].wait_recv()
    moves2(soon)[5].wait_recv()
    take2(3, soon, factor)
    finish2(soon)

    @pl.when(next_row)
    def _():
        tail.start()

    @pl.when(s == 0)
    def _():
        kv2[:, :, 0:WINDOW, :] = jnp.zeros((2, kv_heads, WINDOW, HEAD_DIM), BF16)

    factor = post_factor(late)
    take2(0, late, factor)
    forward_rows(late)
    moves2(late)[2].wait_recv()
    take2(1, late, factor)
    moves2(late)[3].wait_recv()
    take2(2, late, factor)
    moves2(late)[4].wait_recv()
    moves2(late)[5].wait_recv()
    take2(3, late, factor)
    finish2(late)

    @pl.when(prev_row)
    def _():
        tail.wait_recv()

    for h in range(kv_heads):
        for part in range(2):
            q = q_all[h * group : (h + 1) * group, part * block : (part + 1) * block]
            q = q.reshape(group * block, HEAD_DIM)
            keys = kv2[0, h, part * block : part * block + WINDOW + block]
            values = kv2[1, h, part * block : part * block + WINDOW + block]
            scores = lax.dot_general(
                q, keys, (((1,), (1,)), ((), ())), preferred_element_type=F32
            )
            weights = jnp.exp2(jnp.tanh(scores * INNER) * OUTER)
            row = lax.broadcasted_iota(jnp.int32, (block, WINDOW + block), 0)
            col = lax.broadcasted_iota(jnp.int32, (block, WINDOW + block), 1)
            least = row
            if part == 0:
                least = jnp.maximum(row, jnp.where(prev_row, 0, WINDOW - 1))
            mask = (col > least) & (col <= row + WINDOW)
            weights = jnp.concatenate(
                [jnp.where(mask, weights[g * block : (g + 1) * block], 0.0) for g in range(group)],
                axis=0,
            )
            denominator = jnp.sum(weights, axis=-1, keepdims=True)
            numerator = jnp.dot(weights.astype(BF16), values, preferred_element_type=F32)
            result = (numerator / denominator).astype(BF16)
            for g in range(group):
                head = h * group + g
                o_ref[part * block : (part + 1) * block, head * HEAD_DIM : (head + 1) * HEAD_DIM] = (
                    result[g * block : (g + 1) * block]
                )

    def drain_first(part, carry):
        for copy in moves(part):
            copy.wait_send()

        @pl.when(has_up)
        def _():
            up(s, part).wait_send()

        @pl.when(c == 0)
        def _():
            side(s, part).wait_send()

        def drain_level(k, carry):
            @pl.when(has_up)
            def _():
                up(s - 2 * k, part).wait_send()

            side(s - 2 * k, part).wait_send()
            return carry

        lax.fori_loop(1, z + 1, drain_level, 0)
        return carry

    lax.fori_loop(0, PARTS, drain_first, 0)
    for part in range(2):
        for copy in (*reduce_moves(part), *swaps(part), *moves2(part)):
            copy.wait_send()

    @pl.when(next_row)
    def _():
        tail.wait_send()


def fused(x, gains, cos, sin, first, wo, second, count, collective_id):
    rows, cols = x.shape
    wq, wk, wv = first
    heads, kv_heads = wq.shape[1] // HEAD_DIM, wk.shape[1] // HEAD_DIM
    total = wq.shape[1] + 2 * wk.shape[1]
    depth = wo.shape[0]
    chunk, block = rows // PARTS, rows // 2
    vmem = pl.BlockSpec(memory_space=VMEM)
    hbm = pl.BlockSpec(memory_space=pltpu.HBM)
    dma = pltpu.SemaphoreType.DMA
    folded = [gain.reshape(-1, HEAD_DIM) for gain in gains]
    return pl.pallas_call(
        functools.partial(fused_kernel, count // 2, heads, kv_heads),
        out_shape=(
            jax.ShapeDtypeStruct((rows, cols), BF16),
            jax.ShapeDtypeStruct((rows, heads * HEAD_DIM), BF16),
        ),
        in_specs=[hbm] * 4 + [vmem] * 2 + [hbm] * 7,
        out_specs=(vmem, vmem),
        scratch_shapes=[
            VMEM((4, rows, cols), BF16),
            VMEM((4, cols, total), BF16),
            VMEM((4, depth, cols), BF16),
            VMEM((3,) + folded[0].shape, F32),
            VMEM((block, cols), BF16),
            VMEM((block, total), F32),
            VMEM((block, HEAD_DIM), F32),
            VMEM((heads, rows, HEAD_DIM), BF16),
            VMEM((count, 2, kv_heads, rows, HEAD_DIM), BF16),
            VMEM((heads, rows, HEAD_DIM), F32),
            VMEM((heads, rows, HEAD_DIM), F32),
            VMEM((rows, depth), BF16),
            VMEM((3, rows, cols), BF16),
            VMEM((rows, cols), F32),
            VMEM((2, 6, block // 2, cols), BF16),
            VMEM((2, 2, block // 2, cols), BF16),
            VMEM((4, rows, cols), BF16),
            VMEM((2, 8, block), F32),
            VMEM((2, 3, 8, block), F32),
            VMEM((2, kv_heads, WINDOW + rows, HEAD_DIM), BF16),
            dma((PARTS,)),
            dma((3,)),
            dma((4, 3)),
            dma((4,)),
            dma((6 * PARTS + 12,)),
            dma((6 * PARTS + 12,)),
            dma((count * PARTS,)),
            dma((count * PARTS,)),
            dma((count * PARTS,)),
            dma((12,)),
            dma((12,)),
            dma((6,)),
            dma((6,)),
            dma((2,)),
        ],
        compiler_params=pltpu.CompilerParams(
            collective_id=collective_id, has_side_effects=True, vmem_limit_bytes=58 * 2**20
        ),
        name="fused",
    )(x, *folded, cos, sin, wq, wk, wv, wo, *second)


def rms_scaled(values, weights):
    widened = values.astype(F32)
    factor = lax.rsqrt(jnp.mean(widened * widened, axis=-1, keepdims=True) + NORM_EPS)
    return widened * factor * weights


def plain_gather_project(x, gain, cos, sin, wq, wk, wv):
    full = lax.all_gather(x, "tp", axis=1, tiled=True)
    normed = rms_scaled(full, gain).astype(BF16)

    def heads_of(weight):
        product = jnp.dot(normed, weight, preferred_element_type=F32)
        return jnp.swapaxes(product.reshape(x.shape[0], -1, HEAD_DIM), 0, 1)

    def rotated(u):
        return (u * cos + jnp.roll(u, HEAD_DIM // 2, axis=-1) * sin).astype(BF16)

    keys, values = rotated(heads_of(wk)), heads_of(wv).astype(BF16)
    return rotated(heads_of(wq)), jnp.stack([keys, values])


def plain_output_project(attended, tokens, gain, wo):
    cols = tokens.shape[1]
    partial_sum = jnp.dot(attended, wo, preferred_element_type=F32).astype(BF16)
    summed = lax.psum(partial_sum, "tp").astype(F32)
    added = rms_scaled(summed, gain)
    mine = lax.dynamic_slice_in_dim(added, lax.axis_index("tp") * cols, cols, 1)
    return (tokens.astype(F32) + mine).astype(BF16)


def local(
    sizes,
    tokens,
    attention_gain,
    query_weight,
    key_weight,
    value_weight,
    output_weight,
    post_gain,
    local_gain,
    local_query_weight,
    local_key_weight,
    local_value_weight,
):
    seq, tp = sizes
    rows, cols = tokens.shape
    places = lax.axis_index("seq") * rows + lax.iota(jnp.int32, rows)
    halfway = HEAD_DIM // 2
    exponents = jnp.arange(halfway, dtype=F32) * (2.0 / HEAD_DIM)
    frequency = jnp.power(F32(10000.0), -exponents)
    angles = places.astype(F32)[:, None] * frequency[None, :]
    cosine, sine = jnp.cos(angles), jnp.sin(angles)
    cos = jnp.concatenate([cosine, cosine], axis=-1)
    sin = jnp.concatenate([-sine, sine], axis=-1)
    first = (query_weight, key_weight, value_weight)
    second = (local_query_weight, local_key_weight, local_value_weight)
    if tp == 4 and cols % HEAD_DIM == 0 and rows == 2 * WINDOW and seq % 2 == 0:
        gains = (attention_gain, post_gain, local_gain)
        return fused(tokens, gains, cos, sin, first, output_weight, second, seq, 0)
    lead = plain_gather_project(tokens, attention_gain, cos, sin, *first)
    attended = causal_attention(*lead, seq, 1)
    hidden = plain_output_project(attended, tokens, post_gain, output_weight)
    lq, lkv = plain_gather_project(hidden, local_gain, cos, sin, *second)
    return hidden, window_attention(lq, lkv, seq, 4)


def solution(mesh):
    in_specs = (
        P("seq", "tp"),
        P(),
        P(None, "tp"),
        P(None, "tp"),
        P(None, "tp"),
        P("tp", None),
        P(),
        P(),
        P(None, "tp"),
        P(None, "tp"),
        P(None, "tp"),
    )
    out_specs = (P("seq", "tp"), P("seq", "tp"))
    sizes = (mesh.shape["seq"], mesh.shape["tp"])
    body = functools.partial(local, sizes)
    return jax.shard_map(body, mesh=mesh, in_specs=in_specs, out_specs=out_specs, check_vma=False)
```

```python
import functools
import math

import jax
import jax.numpy as jnp
from jax import lax
from jax.experimental import pallas as pl
from jax.experimental.pallas import tpu as pltpu
from jax.sharding import PartitionSpec as P

D = 4608
HEADS = 32
HEAD_DIM = 128
WINDOW = 128

SOFT_CAP = 50.0
NORM_EPS = 1e-06
MESH = pl.DeviceIdType.MESH
VMEM = pltpu.VMEM
F32 = jnp.float32
BF16 = jnp.bfloat16
PARTS = 4
INNER = float(D // HEADS) ** (-0.5) / SOFT_CAP
OUTER = SOFT_CAP * math.log2(math.e)


def greet(peers):
    barrier = pltpu.get_barrier_semaphore()
    for peer in peers:
        pl.semaphore_signal(barrier, inc=1, device_id=peer, device_id_type=MESH)
    pl.semaphore_wait(barrier, len(peers))


def remote(source, target, send_sem, recv_sem, device):
    return pltpu.make_async_remote_copy(
        src_ref=source,
        dst_ref=target,
        send_sem=send_sem,
        recv_sem=recv_sem,
        device_id=device,
        device_id_type=MESH,
    )


def xor(index, bits):
    low, high = index % 2, index // 2
    if bits & 1:
        low = 1 - low
    if bits & 2:
        high = 1 - high
    return high * 2 + low


def attend(q_ref, keys, values, acc, lsum, h, group, allowed, first, row_span=None):
    q = q_ref[pl.ds(h * group, group)]
    if row_span is not None:
        q = q[:, row_span[0] : row_span[1]]
    rows = q.shape[1]
    q = q.reshape(group * rows, HEAD_DIM)
    scores = lax.dot_general(q, keys, (((1,), (1,)), ((), ())), preferred_element_type=F32)
    weights = jnp.exp2(jnp.tanh(scores * INNER) * OUTER)
    if allowed is not None:
        count = keys.shape[0]
        row = lax.broadcasted_iota(jnp.int32, (rows, count), 0)
        col = lax.broadcasted_iota(jnp.int32, (rows, count), 1)
        mask = allowed(row, col)
        weights = jnp.concatenate(
            [jnp.where(mask, weights[g * rows : (g + 1) * rows], 0.0) for g in range(group)], axis=0
        )
    lanes = weights[:, :HEAD_DIM]
    for begin in range(HEAD_DIM, keys.shape[0], HEAD_DIM):
        lanes = lanes + weights[:, begin : begin + HEAD_DIM]
    product = jnp.dot(weights.astype(BF16), values, preferred_element_type=F32)
    lanes = lanes.reshape(group, rows, HEAD_DIM)
    product = product.reshape(group, rows, HEAD_DIM)
    heads = pl.ds(h * group, group)
    span = pl.ds(0, rows)
    if first:
        lsum[heads, span] = lanes
        acc[heads, span] = product
    else:
        lsum[heads, span] += lanes
        acc[heads, span] += product


def write_heads(o_ref, acc, lsum):
    for h in range(acc.shape[0]):
        denominator = jnp.sum(lsum[h], axis=-1, keepdims=True)
        o_ref[:, h * HEAD_DIM : (h + 1) * HEAD_DIM] = (acc[h] / denominator).astype(BF16)


def causal_kernel(levels, q_ref, kv_ref, o_ref, buf, acc, lsum, up_sem, side_sem, recv):
    s = lax.axis_index("seq")
    z, c = s // 2, s % 2
    mate = s + 1 - 2 * c
    kv_heads = kv_ref.shape[1]
    group = q_ref.shape[0] // kv_heads
    has_up, has_down = z < levels - 1, z > 0

    barrier = pltpu.get_barrier_semaphore()
    pl.semaphore_signal(barrier, inc=1, device_id={"seq": mate}, device_id_type=MESH)

    @pl.when(has_up)
    def _():
        pl.semaphore_signal(barrier, inc=1, device_id={"seq": s + 2}, device_id_type=MESH)

    @pl.when(has_down)
    def _():
        pl.semaphore_signal(barrier, inc=1, device_id={"seq": s - 2}, device_id_type=MESH)

    pl.semaphore_wait(barrier, 1 + has_up.astype(jnp.int32) + has_down.astype(jnp.int32))

    def up(owner, source):
        return remote(source, buf.at[owner], up_sem.at[owner], recv.at[owner], {"seq": s + 2})

    def side(owner, source):
        return remote(source, buf.at[owner], side_sem.at[owner], recv.at[owner], {"seq": mate})

    @pl.when(has_up)
    def _():
        up(s, kv_ref).start()

    @pl.when(c == 0)
    def _():
        side(s, kv_ref).start()

    def own(h, carry):
        attend(
            q_ref, kv_ref[0, h], kv_ref[1, h], acc, lsum, h, group,
            lambda row, col: col <= row, True,
        )
        return carry

    lax.fori_loop(0, kv_heads, own, 0)

    def visit(owner):
        def body(h, carry):
            attend(
                q_ref, buf[owner, 0, h], buf[owner, 1, h], acc, lsum, h, group, None, False
            )
            return carry

        lax.fori_loop(0, kv_heads, body, 0)

    @pl.when(c == 1)
    def _():
        side(s - 1, buf.at[s - 1]).wait_recv()
        visit(s - 1)

    def level(k, carry):
        owner, other = s - 2 * k, mate - 2 * k
        up(owner, buf.at[owner]).wait_recv()

        @pl.when(has_up)
        def _():
            up(owner, buf.at[owner]).start()

        side(owner, buf.at[owner]).start()
        visit(owner)
        side(other, buf.at[other]).wait_recv()
        visit(other)
        return carry

    lax.fori_loop(1, z + 1, level, 0)
    write_heads(o_ref, acc, lsum)

    @pl.when(has_up)
    def _():
        up(s, kv_ref).wait_send()

    @pl.when(c == 0)
    def _():
        side(s, kv_ref).wait_send()

    def drain(k, carry):
        owner = s - 2 * k

        @pl.when(has_up)
        def _():
            up(owner, buf.at[owner]).wait_send()

        side(owner, buf.at[owner]).wait_send()
        return carry

    lax.fori_loop(1, z + 1, drain, 0)


def causal_attention(q, kv, count, collective_id):
    heads, rows, _ = q.shape
    vmem = pl.BlockSpec(memory_space=VMEM)
    return pl.pallas_call(
        functools.partial(causal_kernel, count // 2),
        out_shape=jax.ShapeDtypeStruct((rows, heads * HEAD_DIM), BF16),
        in_specs=[vmem] * 2,
        out_specs=vmem,
        scratch_shapes=[
            VMEM((count,) + kv.shape, BF16),
            VMEM(q.shape, F32),
            VMEM(q.shape, F32),
            pltpu.SemaphoreType.DMA((count,)),
            pltpu.SemaphoreType.DMA((count,)),
            pltpu.SemaphoreType.DMA((count,)),
        ],
        compiler_params=pltpu.CompilerParams(
            collective_id=collective_id, has_side_effects=True, vmem_limit_bytes=32 * 2**20
        ),
        name="causal_attention",
    )(q, kv)


def window_kernel(count, q_ref, kv_ref, o_ref, tail, acc, lsum, send, recv):
    s = lax.axis_index("seq")
    kv_heads, rows = kv_ref.shape[1], kv_ref.shape[2]
    group = q_ref.shape[0] // kv_heads
    has_next, has_last = s < count - 1, s > 0
    barrier = pltpu.get_barrier_semaphore()

    @pl.when(has_next)
    def _():
        pl.semaphore_signal(barrier, inc=1, device_id={"seq": s + 1}, device_id_type=MESH)

    @pl.when(has_last)
    def _():
        pl.semaphore_signal(barrier, inc=1, device_id={"seq": s - 1}, device_id_type=MESH)

    pl.semaphore_wait(barrier, has_next.astype(jnp.int32) + has_last.astype(jnp.int32))
    copy = remote(
        kv_ref.at[:, :, pl.ds(rows - WINDOW, WINDOW), :], tail, send.at[0], recv.at[0],
        {"seq": s + 1},
    )

    @pl.when(has_next)
    def _():
        copy.start()

    def own(h, carry):
        attend(
            q_ref, kv_ref[0, h], kv_ref[1, h], acc, lsum, h, group,
            lambda row, col: (col <= row) & (row - col < WINDOW), True,
        )
        return carry

    lax.fori_loop(0, kv_heads, own, 0)

    @pl.when(has_last)
    def _():
        copy.wait_recv()

        def body(h, carry):
            attend(
                q_ref, tail[0, h], tail[1, h], acc, lsum, h, group,
                lambda row, col: col > row, False, (0, WINDOW),
            )
            return carry

        lax.fori_loop(0, kv_heads, body, 0)

    write_heads(o_ref, acc, lsum)

    @pl.when(has_next)
    def _():
        copy.wait_send()


def window_attention(q, kv, count, collective_id):
    heads, rows, _ = q.shape
    vmem = pl.BlockSpec(memory_space=VMEM)
    return pl.pallas_call(
        functools.partial(window_kernel, count),
        out_shape=jax.ShapeDtypeStruct((rows, heads * HEAD_DIM), BF16),
        in_specs=[vmem] * 2,
        out_specs=vmem,
        scratch_shapes=[
            VMEM((2, kv.shape[1], WINDOW, HEAD_DIM), BF16),
            VMEM(q.shape, F32),
            VMEM(q.shape, F32),
            pltpu.SemaphoreType.DMA((1,)),
            pltpu.SemaphoreType.DMA((1,)),
        ],
        compiler_params=pltpu.CompilerParams(
            collective_id=collective_id, has_side_effects=True, vmem_limit_bytes=24 * 2**20
        ),
        name="window_attention",
    )(q, kv)


def fused_kernel(
    levels, heads, kv_heads, keep,
    x_hbm, gain1_hbm, gain2_hbm, gain3_hbm, cos_ref, sin_ref,
    wq_hbm, wk_hbm, wv_hbm, wo_hbm, lwq_hbm, lwk_hbm, lwv_hbm,
    hidden_ref, lq_ref, kv2,
    buf, w, wo, gains, xg, acc, ss, ss_first, q_all, kv_buf, out, lsum, att,
    terms, own, landed, passed, proj, mine, stats, q_up, out_up, lsum_up, up_num, up_sum, got_num, got_sum,
    x_sem, gain_sem, w_sem, wo_sem, ag_send, ag_recv, up_sem, side_sem, kv_sem,
    rs_send, rs_recv, st_send, st_recv, tail_sem, down_send, down_recv, back_send, back_recv,
):
    me = lax.axis_index("tp")
    s = lax.axis_index("seq")
    z, c = s // 2, s % 2
    mate = s + 1 - 2 * c
    has_up, has_down = z < levels - 1, z > 0
    top, helper = z == levels - 1, z == levels - 2
    next_row, prev_row = s < 2 * levels - 1, s > 0
    rows, cols = hidden_ref.shape
    chunk_rows, half_rows = rows // PARTS, rows // PARTS // 2
    block, half = rows // 2, rows // 4
    chunks = cols // HEAD_DIM
    ones = jnp.ones((8, HEAD_DIM), F32)
    highest = lax.Precision.HIGHEST
    owners = [xor(me, bits) for bits in range(4)]
    peers = [{"tp": owner} for owner in owners]
    along_x, along_y = peers[1], peers[2]
    qc, kc = heads * HEAD_DIM, kv_heads * HEAD_DIM
    kvc = 2 * kc
    group = heads // kv_heads

    x_loads = []
    for part in range(PARTS):
        span = pl.ds(part * chunk_rows, chunk_rows)
        copy = pltpu.make_async_copy(x_hbm.at[span], buf.at[0, span], x_sem.at[part])
        copy.start()
        x_loads.append(copy)
    gain_loads = []
    for i, ref in enumerate((gain1_hbm, gain2_hbm, gain3_hbm)):
        copy = pltpu.make_async_copy(ref, gains.at[i], gain_sem.at[i])
        copy.start()
        gain_loads.append(copy)

    def weight_loads(key, value, query):
        loads = []
        for slot in range(4):
            span = pl.ds(pl.multiple_of(owners[slot] * cols, cols), cols)
            spec = ((key, 0, kc), (value, kc, kc), (query, kvc, qc))
            loads.append(
                [
                    pltpu.make_async_copy(
                        ref.at[span, :], w.at[slot, :, pl.ds(begin, width)], w_sem.at[slot, i]
                    )
                    for i, (ref, begin, width) in enumerate(spec)
                ]
            )
        return loads

    first_loads = weight_loads(wk_hbm, wv_hbm, wq_hbm)
    wo_loads = []
    for bits in (3, 1, 2, 0):
        span = pl.ds(pl.multiple_of(owners[bits] * cols, cols), cols)
        wo_loads.append(pltpu.make_async_copy(wo_hbm.at[:, span], wo.at[bits], wo_sem.at[bits]))

    barrier = pltpu.get_barrier_semaphore()
    for peer in (*peers[1:], {"seq": mate}):
        pl.semaphore_signal(barrier, inc=1, device_id=peer, device_id_type=MESH)

    @pl.when(has_up)
    def _():
        pl.semaphore_signal(barrier, inc=1, device_id={"seq": s + 2}, device_id_type=MESH)

    @pl.when(has_down)
    def _():
        pl.semaphore_signal(barrier, inc=1, device_id={"seq": s - 2}, device_id_type=MESH)

    @pl.when(has_up & (c == 1))
    def _():
        pl.semaphore_signal(barrier, inc=1, device_id={"seq": s + 1}, device_id_type=MESH)

    @pl.when(has_down & (c == 0))
    def _():
        pl.semaphore_signal(barrier, inc=1, device_id={"seq": s - 1}, device_id_type=MESH)

    far = (has_up & (c == 1)) | (has_down & (c == 0))
    pl.semaphore_wait(
        barrier,
        4 + has_up.astype(jnp.int32) + has_down.astype(jnp.int32) + far.astype(jnp.int32),
    )

    def gather_moves(store, first, count, part, base):
        begin = pl.multiple_of(part * count, count)
        top, bottom = pl.ds(begin, count // 2), pl.ds(begin + count // 2, count // 2)
        spec = (
            (store.at[0, top], store.at[1, top], along_x),
            (store.at[0, bottom], store.at[2, bottom], along_y),
            (store.at[0, bottom], store.at[1, bottom], along_x),
            (store.at[0, top], store.at[2, top], along_y),
            (store.at[1, top], store.at[3, top], along_y),
            (store.at[2, bottom], store.at[3, bottom], along_x),
        )
        at = first + part * 6 + base
        return [
            remote(source, target, ag_send.at[at + i], ag_recv.at[at + i], device)
            for i, (source, target, device) in enumerate(spec)
        ]

    def moves(part):
        return gather_moves(buf, 0, chunk_rows, part, 0)

    def moves2(part):
        return gather_moves(proj, 6 * PARTS, block, part, 0)

    def kv_part(owner, part, count):
        here = pl.ds(pl.multiple_of(part * chunk_rows, chunk_rows), chunk_rows)
        return kv_buf.at[owner, :, pl.ds(0, count), here]

    def up(owner, part, count):
        at, ref = owner * PARTS + part, kv_part(owner, part, count)
        return remote(ref, ref, up_sem.at[at], kv_sem.at[at], {"seq": s + 2})

    def side(owner, part, count):
        at, ref = owner * PARTS + part, kv_part(owner, part, count)
        return remote(ref, ref, side_sem.at[at], kv_sem.at[at], {"seq": mate})

    def lift(owner, part, act):
        @pl.when(z < levels - 2)
        def _():
            act(up(owner, part, kv_heads))

        @pl.when(helper)
        def _():
            act(up(owner, part, keep))

    def launch(copy):
        copy.start()

    def sent(copy):
        copy.wait_send()

    def arrive(owner, part):
        up(owner, part, kv_heads).wait_recv()
        side(owner, part, kv_heads).start()
        lift(owner, part, launch)

    def arrive_top(owner, part):
        up(owner, part, keep).wait_recv()
        side(owner, part, keep).start()

    down_heads = pl.ds(keep * group, group)

    def query_down(part):
        span = pl.ds(pl.multiple_of(part * block, block), block)
        return remote(
            q_all.at[down_heads, span], q_up.at[:, span], down_send.at[part], down_recv.at[part],
            {"seq": s - 2},
        )

    backs = [
        remote(source, target, back_send.at[i], back_recv.at[i], {"seq": s + 2})
        for i, (source, target) in enumerate(((up_sum, got_sum), (up_num, got_num)))
    ]

    def multiply(slot, count, begin, width, fresh):
        product = jnp.dot(
            xg[0:count, :], w[slot, :, begin : begin + width], preferred_element_type=F32
        )
        if fresh:
            acc[0:count, begin : begin + width] = product
        else:
            acc[0:count, begin : begin + width] += product

    def gain_row(which, slot, j):
        return gains[which, pl.ds(owners[slot] * chunks + j, 1), :]

    def prepare(slot, part):
        here = pl.ds(pl.multiple_of(part * chunk_rows, chunk_rows), chunk_rows)
        squares = None
        for j in range(chunks):
            lanes = slice(j * HEAD_DIM, (j + 1) * HEAD_DIM)
            wide = buf[slot, here, lanes].astype(F32)
            squares = wide * wide if squares is None else squares + wide * wide
            proj[slot, here, lanes] = (wide * gain_row(0, slot, j)).astype(BF16)
        if slot == 0:
            ss_first[here, :] = squares
        else:
            ss_first[here, :] += squares

    def row_factor(squares):
        total = jnp.sum(squares, axis=-1, keepdims=True)
        return lax.rsqrt(jnp.broadcast_to(total, squares.shape) * (1.0 / D) + NORM_EPS)

    def rotated(begin, count, factor, span):
        u = acc[0:count, begin : begin + HEAD_DIM] * factor
        turned = pltpu.roll(u, HEAD_DIM // 2, 1)
        return (u * cos_ref[span, :] + turned * sin_ref[span, :]).astype(BF16)

    for copy in x_loads[:1]:
        copy.wait()
    def launch_group(part, some):
        copies = moves(part)
        for i in some:
            copies[i].start()

    launch_group(0, range(4))
    for copy in x_loads[1:]:
        copy.wait()
    launch_group(1, range(2))
    for copy in gain_loads:
        copy.wait()
    for bundle in first_loads:
        for copy in bundle[:2]:
            copy.start()

    def first_part(part, carry):
        with jax.named_scope("first_part"):
            return one_part(part, carry)

    def relay(part):
        copies = moves(part)
        copies[0].wait_recv()
        copies[4].start()
        copies[1].wait_recv()
        copies[5].start()

        @pl.when(part < PARTS - 1)
        def _():
            launch_group(part + 1, (2, 3))

        @pl.when(part < PARTS - 2)
        def _():
            launch_group(part + 2, (0, 1))

    def one_part(part, carry):
        span = pl.ds(pl.multiple_of(part * chunk_rows, chunk_rows), chunk_rows)

        def take(slot):
            prepare(slot, part)

            @pl.when(part == 0)
            def _():
                for copy in first_loads[slot][:2]:
                    copy.wait()

            product = jnp.dot(proj[slot, span, :], w[slot, :, 0:kvc], preferred_element_type=F32)
            if slot == 0:
                acc[0:chunk_rows, 0:kvc] = product
            else:
                acc[0:chunk_rows, 0:kvc] += product

        copies = moves(part)
        take(0)

        @pl.when(part == 0)
        def _():
            relay(0)

        @pl.when(part == PARTS // 4)
        def _():
            for bundle in first_loads:
                bundle[2].start()

        @pl.when(part == PARTS // 2)
        def _():
            for copy in wo_loads:
                copy.start()

        copies[2].wait_recv()
        take(1)
        copies[3].wait_recv()
        take(2)

        @pl.when(part < PARTS - 1)
        def _():
            relay(part + 1)

        @pl.when(part == PARTS // 2)
        def _():
            queries(0)

        def forward(k, carry):
            @pl.when(part >= k)
            def _():
                arrive(s - 2 * k, part - k)

            return carry

        @pl.when(has_up)
        def _():
            lax.fori_loop(1, z + 1, forward, 0)

        copies[4].wait_recv()
        copies[5].wait_recv()
        take(3)
        factor = row_factor(ss_first[span, :])
        for h in range(kv_heads):
            kv_buf[s, 0, h, span, :] = rotated(h * HEAD_DIM, chunk_rows, factor, span)
            place = kc + h * HEAD_DIM
            kv_buf[s, 1, h, span, :] = (
                acc[0:chunk_rows, place : place + HEAD_DIM] * factor
            ).astype(BF16)

        @pl.when((c == 0) | helper)
        def _():
            side(s, part, kv_heads).start()

        lift(s, part, launch)
        return carry

    def queries(which):
        span = pl.ds(pl.multiple_of(which * block, block), block)

        if which == 0:
            for bundle in first_loads:
                bundle[2].wait()

        acc[:, kvc : kvc + qc] = sum(
            jnp.dot(proj[slot, span, :], w[slot, :, kvc : kvc + qc], preferred_element_type=F32)
            for slot in range(4)
        )
        factor = row_factor(ss_first[span, :])
        for h in reversed(range(heads)):
            q_all[h, span, :] = rotated(kvc + h * HEAD_DIM, block, factor, span)

        @pl.when(top)
        def _():
            query_down(which).start()

    lax.fori_loop(0, PARTS, first_part, 0)
    queries(1)

    second_loads = weight_loads(lwk_hbm, lwv_hbm, lwq_hbm)

    def fetch(slot):
        for copy in second_loads[slot]:
            copy.start()

    with jax.named_scope("own"):
        for h in range(kv_heads):
            attend(
                q_all, kv_buf[s, 0, h], kv_buf[s, 1, h], out, lsum, h, group,
                lambda row, col: col <= row, True,
            )

    def visit_heads(owner, begin, end):
        for h in range(begin, end):
            attend(
                q_all, kv_buf[owner, 0, h], kv_buf[owner, 1, h], out, lsum, h, group, None, False
            )

    def visit(owner):
        with jax.named_scope("visit"):
            visit_heads(owner, 0, keep)

            @pl.when(z < levels - 1)
            def _():
                visit_heads(owner, keep, kv_heads)

    def visit_up(owner, first):
        with jax.named_scope("visit_up"):
            attend(
                q_up, kv_buf[owner, 0, keep], kv_buf[owner, 1, keep], out_up, lsum_up, 0, group,
                None, first,
            )

    def send_back():
        for g in range(group):
            up_sum[g] = lax.dot_general(
                ones, lsum_up[g], (((1,), (1,)), ((), ())), precision=highest,
                preferred_element_type=F32,
            )
            up_num[g] = out_up[g].astype(BF16)
        for copy in backs:
            copy.start()

    @pl.when(helper | (c == 1))
    def _():
        for part in range(PARTS):
            side(mate, part, kv_heads).wait_recv()

    @pl.when(c == 1)
    def _():
        with jax.named_scope("mate"):
            visit_heads(s - 1, 0, kv_heads)

    @pl.when(helper)
    def _():
        for part in range(2):
            query_down(part).wait_recv()
        visit_up(s, True)
        visit_up(mate, False)

    def turn(r, carry):
        def level(k, carry):
            part = r - k

            @pl.when((part >= 0) & (part < PARTS))
            def _():
                owner, other = s - 2 * k, mate - 2 * k

                @pl.when(top)
                def _():
                    arrive_top(owner, part)

                @pl.when((r >= PARTS) & has_up)
                def _():
                    arrive(owner, part)

                @pl.when(part == PARTS - 1)
                def _():
                    @pl.when(helper)
                    def _():
                        visit_up(owner, False)
                        for p in range(PARTS):
                            side(other, p, kv_heads).wait_recv()
                        visit_up(other, False)

                        @pl.when(k == z)
                        def _():
                            send_back()

                    def both(j, carry):
                        @pl.when((j == 1) & top)
                        def _():
                            for p in range(PARTS):
                                side(other, p, keep).wait_recv()

                        @pl.when((j == 1) & (z < levels - 2))
                        def _():
                            for p in range(PARTS):
                                side(other, p, kv_heads).wait_recv()

                        visit(owner + j * (other - owner))
                        return carry

                    lax.fori_loop(0, 2, both, 0)

            return carry

        lax.fori_loop(1, z + 1, level, 0)
        return carry

    lax.fori_loop(1, PARTS + z, turn, 0)

    @pl.when(top)
    def _():
        for copy in backs:
            copy.wait_recv()
        for g in range(group):
            column = lax.dot_general(
                got_sum[g], ones * (0.125 / HEAD_DIM), (((0,), (0,)), ((), ())), precision=highest,
                preferred_element_type=F32,
            )
            lsum[keep * group + g] += column
            out[keep * group + g] += got_num[g].astype(F32)

    with jax.named_scope("write_heads"):
        write_heads(att, out, lsum)

    def reduce_moves(part):
        base = part * block
        top, bottom = pl.ds(base, half), pl.ds(base + half, half)
        spec = (
            (terms.at[2, top], along_x),
            (terms.at[2, bottom], along_y),
            (terms.at[0, top], along_x),
            (terms.at[1, bottom], along_y),
            (passed.at[part, 1], along_x),
            (passed.at[part, 0], along_y),
        )
        return [
            remote(
                source, landed.at[part, i], rs_send.at[part * 6 + i], rs_recv.at[part * 6 + i], device
            )
            for i, (source, device) in enumerate(spec)
        ]

    def product(bits, part):
        span = slice(part * block, (part + 1) * block)
        value = jnp.dot(att[span, :], wo[bits], preferred_element_type=F32)
        if bits == 0:
            own[span, :] = value
        else:
            terms[bits - 1, span, :] = value.astype(BF16)

    def pass_on(part):
        copies = reduce_moves(part)
        base = part * block
        copies[0].wait_recv()
        passed[part, 0] = (
            terms[1, base : base + half].astype(F32) + landed[part, 0].astype(F32)
        ).astype(BF16)
        copies[5].start()
        copies[1].wait_recv()
        passed[part, 1] = (
            terms[0, base + half : base + block].astype(F32) + landed[part, 1].astype(F32)
        ).astype(BF16)
        copies[4].start()

    def swaps(part):
        return [
            remote(
                mine.at[part], stats.at[part, bits - 1],
                st_send.at[part * 3 + bits - 1], st_recv.at[part * 3 + bits - 1], peers[bits],
            )
            for bits in (3, 1, 2)
        ]

    def finalize(part):
        copies = reduce_moves(part)
        for i in (2, 3, 5, 4):
            copies[i].wait_recv()
        base = part * block
        span = slice(base, base + block)
        lanes = None
        for j in range(chunks):
            cut = slice(j * HEAD_DIM, (j + 1) * HEAD_DIM)
            above = landed[part, 2, :, cut].astype(F32) + landed[part, 5, :, cut].astype(F32)
            below = landed[part, 3, :, cut].astype(F32) + landed[part, 4, :, cut].astype(F32)
            value = own[span, cut] + jnp.concatenate([above, below], axis=0)
            own[span, cut] = value
            proj[0, span, cut] = value.astype(BF16)
            lanes = value * value if lanes is None else lanes + value * value
        for copy in moves2(part)[:2]:
            copy.start()
        mine[part] = lax.dot_general(
            ones, lanes, (((1,), (1,)), ((), ())), precision=highest, preferred_element_type=F32
        )
        for swap in swaps(part):
            swap.start()
        for copy in moves2(part)[2:4]:
            copy.start()

    def forward_rows(part):
        copies = moves2(part)
        copies[0].wait_recv()
        copies[4].start()
        copies[1].wait_recv()
        copies[5].start()

    def post_factor(part):
        for swap in swaps(part):
            swap.wait_recv()
        summed = mine[part] + stats[part, 0] + stats[part, 1] + stats[part, 2]
        column = lax.dot_general(
            summed, ones * 0.125, (((0,), (0,)), ((), ())), precision=highest,
            preferred_element_type=F32,
        )
        return lax.rsqrt(column * (1.0 / D) + NORM_EPS)

    def take2(slot, part, factor):
        span = slice(part * block, (part + 1) * block)
        squares = None
        for j in range(chunks):
            cut = slice(j * HEAD_DIM, (j + 1) * HEAD_DIM)
            summed = own[span, cut] if slot == 0 else proj[slot, span, cut].astype(F32)
            added = buf[slot, span, cut].astype(F32) + summed * factor * gain_row(1, slot, j)
            rounded = added.astype(BF16)
            if slot == 0:
                hidden_ref[span, cut] = rounded
            wide = rounded.astype(F32)
            squares = wide * wide if squares is None else squares + wide * wide
            xg[:, cut] = (wide * gain_row(2, slot, j)).astype(BF16)
        if slot == 0:
            ss[...] = squares
        else:
            ss[...] += squares
        if part == 1:
            for copy in second_loads[slot]:
                copy.wait()
        multiply(slot, block, 0, kvc, slot == 0)
        multiply(slot, block, kvc, qc, slot == 0)

    def finish2(part):
        span = pl.ds(part * block, block)
        place_rows = pl.ds(WINDOW + part * block, block)
        factor = row_factor(ss[...])
        for h in range(kv_heads):
            kv2[0, h, place_rows, :] = rotated(h * HEAD_DIM, block, factor, span)
            place = kc + h * HEAD_DIM
            kv2[1, h, place_rows, :] = (acc[:, place : place + HEAD_DIM] * factor).astype(BF16)
        for h in range(heads):
            lq_ref[h, span, :] = rotated(kvc + h * HEAD_DIM, block, factor, span)

    tail = remote(
        kv2.at[:, :, pl.ds(rows, WINDOW)], kv2.at[:, :, pl.ds(0, WINDOW)],
        tail_sem.at[0], tail_sem.at[1], {"seq": s + 1},
    )

    def scoped(name, run, *given):
        with jax.named_scope(name):
            return run(*given)

    for copy in wo_loads:
        copy.wait()
    late, soon = 0, 1
    copies = reduce_moves(soon)
    scoped("product", product, 3, soon)
    copies[0].start()
    copies[1].start()
    scoped("product", product, 1, soon)
    copies[2].start()
    scoped("product", product, 2, soon)
    copies[3].start()
    scoped("product", product, 0, soon)
    fetch(0)
    for bits in (3, 1, 2, 0):
        scoped("product", product, bits, late)
    scoped("pass_on", pass_on, soon)
    for copy in reduce_moves(late)[:4]:
        copy.start()
    fetch(1)
    fetch(2)
    fetch(3)
    scoped("finalize", finalize, soon)
    scoped("pass_on", pass_on, late)
    factor = scoped("post_factor", post_factor, soon)
    scoped("take2", take2, 0, soon, factor)
    scoped("forward_rows", forward_rows, soon)
    moves2(soon)[2].wait_recv()
    scoped("take2", take2, 1, soon, factor)
    moves2(soon)[3].wait_recv()
    scoped("take2", take2, 2, soon, factor)
    scoped("finalize", finalize, late)
    moves2(soon)[4].wait_recv()
    moves2(soon)[5].wait_recv()
    scoped("take2", take2, 3, soon, factor)
    scoped("finish2", finish2, soon)

    @pl.when(next_row)
    def _():
        tail.start()

    @pl.when(s == 0)
    def _():
        kv2[:, :, 0:WINDOW, :] = jnp.zeros((2, kv_heads, WINDOW, HEAD_DIM), BF16)

    factor = scoped("post_factor", post_factor, late)
    scoped("take2", take2, 0, late, factor)
    scoped("forward_rows", forward_rows, late)
    moves2(late)[2].wait_recv()
    scoped("take2", take2, 1, late, factor)
    moves2(late)[3].wait_recv()
    scoped("take2", take2, 2, late, factor)
    moves2(late)[4].wait_recv()
    moves2(late)[5].wait_recv()
    scoped("take2", take2, 3, late, factor)
    scoped("finish2", finish2, late)

    @pl.when(prev_row)
    def _():
        tail.wait_recv()

    def drain_first(part, carry):
        for copy in moves(part):
            copy.wait_send()

        lift(s, part, sent)

        @pl.when((c == 0) | helper)
        def _():
            side(s, part, kv_heads).wait_send()

        def drain_level(k, carry):
            lift(s - 2 * k, part, sent)

            @pl.when(has_up)
            def _():
                side(s - 2 * k, part, kv_heads).wait_send()

            @pl.when(top)
            def _():
                side(s - 2 * k, part, keep).wait_send()

            return carry

        lax.fori_loop(1, z + 1, drain_level, 0)
        return carry

    lax.fori_loop(0, PARTS, drain_first, 0)

    @pl.when(helper)
    def _():
        for copy in backs:
            copy.wait_send()

    @pl.when(top)
    def _():
        for part in range(2):
            query_down(part).wait_send()

    for part in range(2):
        for copy in (*reduce_moves(part), *swaps(part), *moves2(part)):
            copy.wait_send()

    @pl.when(next_row)
    def _():
        tail.wait_send()


def fused(x, gains, cos, sin, first, wo, second, count, collective_id):
    rows, cols = x.shape
    wq, wk, wv = first
    heads, kv_heads = wq.shape[1] // HEAD_DIM, wk.shape[1] // HEAD_DIM
    total = wq.shape[1] + 2 * wk.shape[1]
    depth = wo.shape[0]
    group, block = heads // kv_heads, rows // 2
    vmem = pl.BlockSpec(memory_space=VMEM)
    hbm = pl.BlockSpec(memory_space=pltpu.HBM)
    dma = pltpu.SemaphoreType.DMA
    folded = [gain.reshape(-1, HEAD_DIM) for gain in gains]
    far = [x, *folded, wq, wk, wv, wo, *second]
    far = [pltpu.with_memory_space_constraint(array, pltpu.HBM) for array in far]
    return pl.pallas_call(
        functools.partial(fused_kernel, count // 2, heads, kv_heads, kv_heads - 1),
        out_shape=(
            jax.ShapeDtypeStruct((rows, cols), BF16),
            jax.ShapeDtypeStruct((heads, rows, HEAD_DIM), BF16),
            jax.ShapeDtypeStruct((2, kv_heads, WINDOW + rows, HEAD_DIM), BF16),
        ),
        in_specs=[hbm] * 4 + [vmem] * 2 + [hbm] * 7,
        out_specs=(vmem, vmem, vmem),
        scratch_shapes=[
            VMEM((4, rows, cols), BF16),
            VMEM((4, cols, total), BF16),
            VMEM((4, depth, cols), BF16),
            VMEM((3,) + folded[0].shape, F32),
            VMEM((block, cols), BF16),
            VMEM((block, total), F32),
            VMEM((block, HEAD_DIM), F32),
            VMEM((rows, HEAD_DIM), F32),
            VMEM((heads, rows, HEAD_DIM), BF16),
            VMEM((count, 2, kv_heads, rows, HEAD_DIM), BF16),
            VMEM((heads, rows, HEAD_DIM), F32),
            VMEM((heads, rows, HEAD_DIM), F32),
            VMEM((rows, depth), BF16),
            VMEM((3, rows, cols), BF16),
            VMEM((rows, cols), F32),
            VMEM((2, 6, block // 2, cols), BF16),
            VMEM((2, 2, block // 2, cols), BF16),
            VMEM((4, rows, cols), BF16),
            VMEM((2, 8, block), F32),
            VMEM((2, 3, 8, block), F32),
            VMEM((group, rows, HEAD_DIM), BF16),
            VMEM((group, rows, HEAD_DIM), F32),
            VMEM((group, rows, HEAD_DIM), F32),
            VMEM((group, rows, HEAD_DIM), BF16),
            VMEM((group, 8, rows), F32),
            VMEM((group, rows, HEAD_DIM), BF16),
            VMEM((group, 8, rows), F32),
            dma((PARTS,)),
            dma((3,)),
            dma((4, 3)),
            dma((4,)),
            dma((6 * PARTS + 12,)),
            dma((6 * PARTS + 12,)),
            dma((count * PARTS,)),
            dma((count * PARTS,)),
            dma((count * PARTS,)),
            dma((12,)),
            dma((12,)),
            dma((6,)),
            dma((6,)),
            dma((2,)),
            dma((2,)),
            dma((2,)),
            dma((2,)),
            dma((2,)),
        ],
        compiler_params=pltpu.CompilerParams(
            collective_id=collective_id, has_side_effects=True, vmem_limit_bytes=50 * 2**20
        ),
        name="fused",
    )(*far[:4], cos, sin, *far[4:])


def finish_kernel(hid_ref, q_ref, kv_ref, hid_hbm, o_hbm, o_ref, sems):
    rows = hid_ref.shape[0]
    heads, kv_heads = q_ref.shape[0], kv_ref.shape[1]
    group, block = heads // kv_heads, rows // 2
    begins = jnp.where(lax.axis_index("seq") > 0, 0, WINDOW - 1)
    copies = [pltpu.make_async_copy(hid_ref, hid_hbm, sems.at[kv_heads])]
    copies[0].start()
    for h in range(kv_heads):
        for part in range(2):
            q = q_ref[h * group : (h + 1) * group, part * block : (part + 1) * block]
            q = q.reshape(group * block, HEAD_DIM)
            keys = kv_ref[0, h, part * block : part * block + WINDOW + block]
            values = kv_ref[1, h, part * block : part * block + WINDOW + block]
            scores = lax.dot_general(
                q, keys, (((1,), (1,)), ((), ())), preferred_element_type=F32
            )
            weights = jnp.exp2(jnp.tanh(scores * INNER) * OUTER)
            row = lax.broadcasted_iota(jnp.int32, (block, WINDOW + block), 0)
            col = lax.broadcasted_iota(jnp.int32, (block, WINDOW + block), 1)
            least = jnp.maximum(row, begins) if part == 0 else row
            mask = (col > least) & (col <= row + WINDOW)
            weights = jnp.concatenate(
                [jnp.where(mask, weights[g * block : (g + 1) * block], 0.0) for g in range(group)],
                axis=0,
            )
            denominator = jnp.sum(weights, axis=-1, keepdims=True)
            numerator = jnp.dot(weights.astype(BF16), values, preferred_element_type=F32)
            result = (numerator / denominator).astype(BF16)
            for g in range(group):
                head = h * group + g
                o_ref[part * block : (part + 1) * block, head * HEAD_DIM : (head + 1) * HEAD_DIM] = (
                    result[g * block : (g + 1) * block]
                )
        lanes = pl.ds(h * group * HEAD_DIM, group * HEAD_DIM)
        copy = pltpu.make_async_copy(o_ref.at[:, lanes], o_hbm.at[:, lanes], sems.at[h])
        copy.start()
        copies.append(copy)
    for copy in copies:
        copy.wait()


def finish(hidden, q, kv):
    heads, rows, _ = q.shape
    vmem = pl.BlockSpec(memory_space=VMEM)
    hbm = pl.BlockSpec(memory_space=pltpu.HBM)
    shape = jax.ShapeDtypeStruct((rows, heads * HEAD_DIM), BF16)
    return pl.pallas_call(
        finish_kernel,
        out_shape=(jax.ShapeDtypeStruct(hidden.shape, BF16), shape),
        in_specs=[vmem] * 3,
        out_specs=(hbm, hbm),
        scratch_shapes=[
            VMEM(shape.shape, BF16),
            pltpu.SemaphoreType.DMA((kv.shape[1] + 1,)),
        ],
        compiler_params=pltpu.CompilerParams(vmem_limit_bytes=8 * 2**20),
        name="finish",
    )(hidden, q, kv)


def rms_scaled(values, weights):
    widened = values.astype(F32)
    factor = lax.rsqrt(jnp.mean(widened * widened, axis=-1, keepdims=True) + NORM_EPS)
    return widened * factor * weights


def plain_gather_project(x, gain, cos, sin, wq, wk, wv):
    full = lax.all_gather(x, "tp", axis=1, tiled=True)
    normed = rms_scaled(full, gain).astype(BF16)

    def heads_of(weight):
        product = jnp.dot(normed, weight, preferred_element_type=F32)
        return jnp.swapaxes(product.reshape(x.shape[0], -1, HEAD_DIM), 0, 1)

    def rotated(u):
        return (u * cos + jnp.roll(u, HEAD_DIM // 2, axis=-1) * sin).astype(BF16)

    keys, values = rotated(heads_of(wk)), heads_of(wv).astype(BF16)
    return rotated(heads_of(wq)), jnp.stack([keys, values])


def plain_output_project(attended, tokens, gain, wo):
    cols = tokens.shape[1]
    partial_sum = jnp.dot(attended, wo, preferred_element_type=F32).astype(BF16)
    summed = lax.psum(partial_sum, "tp").astype(F32)
    added = rms_scaled(summed, gain)
    mine = lax.dynamic_slice_in_dim(added, lax.axis_index("tp") * cols, cols, 1)
    return (tokens.astype(F32) + mine).astype(BF16)


def local(
    sizes,
    tokens,
    attention_gain,
    query_weight,
    key_weight,
    value_weight,
    output_weight,
    post_gain,
    local_gain,
    local_query_weight,
    local_key_weight,
    local_value_weight,
):
    seq, tp = sizes
    rows, cols = tokens.shape
    places = lax.axis_index("seq") * rows + lax.iota(jnp.int32, rows)
    halfway = HEAD_DIM // 2
    exponents = jnp.arange(halfway, dtype=F32) * (2.0 / HEAD_DIM)
    frequency = jnp.power(F32(10000.0), -exponents)
    angles = places.astype(F32)[:, None] * frequency[None, :]
    cosine, sine = jnp.cos(angles), jnp.sin(angles)
    cos = jnp.concatenate([cosine, cosine], axis=-1)
    sin = jnp.concatenate([-sine, sine], axis=-1)
    first = (query_weight, key_weight, value_weight)
    second = (local_query_weight, local_key_weight, local_value_weight)
    if tp == 4 and cols % HEAD_DIM == 0 and rows == 2 * WINDOW and seq % 2 == 0 and seq > 4:
        gains = (attention_gain, post_gain, local_gain)
        return finish(*fused(tokens, gains, cos, sin, first, output_weight, second, seq, 0))
    lead = plain_gather_project(tokens, attention_gain, cos, sin, *first)
    attended = causal_attention(*lead, seq, 1)
    hidden = plain_output_project(attended, tokens, post_gain, output_weight)
    lq, lkv = plain_gather_project(hidden, local_gain, cos, sin, *second)
    return hidden, window_attention(lq, lkv, seq, 4)


def solution(mesh):
    in_specs = (
        P("seq", "tp"),
        P(),
        P(None, "tp"),
        P(None, "tp"),
        P(None, "tp"),
        P("tp", None),
        P(),
        P(),
        P(None, "tp"),
        P(None, "tp"),
        P(None, "tp"),
    )
    out_specs = (P("seq", "tp"), P("seq", "tp"))
    sizes = (mesh.shape["seq"], mesh.shape["tp"])
    body = functools.partial(local, sizes)
    return jax.shard_map(body, mesh=mesh, in_specs=in_specs, out_specs=out_specs, check_vma=False)
```

```python
import functools
import math

import jax
import jax.numpy as jnp
import numpy as np
from jax import lax
from jax.experimental import pallas as pl
from jax.experimental.pallas import tpu as pltpu
from jax.sharding import PartitionSpec as P

D = 4608
HEADS = 32
HEAD_DIM = 128
WINDOW = 128

SOFT_CAP = 50.0
NORM_EPS = 1e-06
MESH = pl.DeviceIdType.MESH
VMEM = pltpu.VMEM
F32 = jnp.float32
BF16 = jnp.bfloat16
PARTS = 4
INNER = float(D // HEADS) ** (-0.5) / SOFT_CAP
OUTER = SOFT_CAP * math.log2(math.e)


def greet(peers):
    barrier = pltpu.get_barrier_semaphore()
    for peer in peers:
        pl.semaphore_signal(barrier, inc=1, device_id=peer, device_id_type=MESH)
    pl.semaphore_wait(barrier, len(peers))


def remote(source, target, send_sem, recv_sem, device):
    return pltpu.make_async_remote_copy(
        src_ref=source,
        dst_ref=target,
        send_sem=send_sem,
        recv_sem=recv_sem,
        device_id=device,
        device_id_type=MESH,
    )


def xor(index, bits):
    low, high = index % 2, index // 2
    if bits & 1:
        low = 1 - low
    if bits & 2:
        high = 1 - high
    return high * 2 + low


def attend(q_ref, keys, values, acc, lsum, h, group, allowed, first, row_span=None):
    q = q_ref[pl.ds(h * group, group)]
    if row_span is not None:
        q = q[:, row_span[0] : row_span[1]]
    rows = q.shape[1]
    q = q.reshape(group * rows, HEAD_DIM)
    scores = lax.dot_general(q, keys, (((1,), (1,)), ((), ())), preferred_element_type=F32)
    weights = jnp.exp2(jnp.tanh(scores * INNER) * OUTER)
    if allowed is not None:
        count = keys.shape[0]
        row = lax.broadcasted_iota(jnp.int32, (rows, count), 0)
        col = lax.broadcasted_iota(jnp.int32, (rows, count), 1)
        mask = allowed(row, col)
        weights = jnp.concatenate(
            [jnp.where(mask, weights[g * rows : (g + 1) * rows], 0.0) for g in range(group)], axis=0
        )
    lanes = weights[:, :HEAD_DIM]
    for begin in range(HEAD_DIM, keys.shape[0], HEAD_DIM):
        lanes = lanes + weights[:, begin : begin + HEAD_DIM]
    product = jnp.dot(weights.astype(BF16), values, preferred_element_type=F32)
    lanes = lanes.reshape(group, rows, HEAD_DIM)
    product = product.reshape(group, rows, HEAD_DIM)
    heads = pl.ds(h * group, group)
    span = pl.ds(0, rows)
    if first:
        lsum[heads, span] = lanes
        acc[heads, span] = product
    else:
        lsum[heads, span] += lanes
        acc[heads, span] += product


def write_heads(o_ref, acc, lsum):
    for h in range(acc.shape[0]):
        denominator = jnp.sum(lsum[h], axis=-1, keepdims=True)
        o_ref[:, h * HEAD_DIM : (h + 1) * HEAD_DIM] = (acc[h] / denominator).astype(BF16)


def causal_kernel(levels, q_ref, kv_ref, o_ref, buf, acc, lsum, up_sem, side_sem, recv):
    s = lax.axis_index("seq")
    z, c = s // 2, s % 2
    mate = s + 1 - 2 * c
    kv_heads = kv_ref.shape[1]
    group = q_ref.shape[0] // kv_heads
    has_up, has_down = z < levels - 1, z > 0

    barrier = pltpu.get_barrier_semaphore()
    pl.semaphore_signal(barrier, inc=1, device_id={"seq": mate}, device_id_type=MESH)

    @pl.when(has_up)
    def _():
        pl.semaphore_signal(barrier, inc=1, device_id={"seq": s + 2}, device_id_type=MESH)

    @pl.when(has_down)
    def _():
        pl.semaphore_signal(barrier, inc=1, device_id={"seq": s - 2}, device_id_type=MESH)

    pl.semaphore_wait(barrier, 1 + has_up.astype(jnp.int32) + has_down.astype(jnp.int32))

    def up(owner, source):
        return remote(source, buf.at[owner], up_sem.at[owner], recv.at[owner], {"seq": s + 2})

    def side(owner, source):
        return remote(source, buf.at[owner], side_sem.at[owner], recv.at[owner], {"seq": mate})

    @pl.when(has_up)
    def _():
        up(s, kv_ref).start()

    @pl.when(c == 0)
    def _():
        side(s, kv_ref).start()

    def own(h, carry):
        attend(
            q_ref, kv_ref[0, h], kv_ref[1, h], acc, lsum, h, group,
            lambda row, col: col <= row, True,
        )
        return carry

    lax.fori_loop(0, kv_heads, own, 0)

    def visit(owner):
        def body(h, carry):
            attend(
                q_ref, buf[owner, 0, h], buf[owner, 1, h], acc, lsum, h, group, None, False
            )
            return carry

        lax.fori_loop(0, kv_heads, body, 0)

    @pl.when(c == 1)
    def _():
        side(s - 1, buf.at[s - 1]).wait_recv()
        visit(s - 1)

    def level(k, carry):
        owner, other = s - 2 * k, mate - 2 * k
        up(owner, buf.at[owner]).wait_recv()

        @pl.when(has_up)
        def _():
            up(owner, buf.at[owner]).start()

        side(owner, buf.at[owner]).start()
        visit(owner)
        side(other, buf.at[other]).wait_recv()
        visit(other)
        return carry

    lax.fori_loop(1, z + 1, level, 0)
    write_heads(o_ref, acc, lsum)

    @pl.when(has_up)
    def _():
        up(s, kv_ref).wait_send()

    @pl.when(c == 0)
    def _():
        side(s, kv_ref).wait_send()

    def drain(k, carry):
        owner = s - 2 * k

        @pl.when(has_up)
        def _():
            up(owner, buf.at[owner]).wait_send()

        side(owner, buf.at[owner]).wait_send()
        return carry

    lax.fori_loop(1, z + 1, drain, 0)


def causal_attention(q, kv, count, collective_id):
    heads, rows, _ = q.shape
    vmem = pl.BlockSpec(memory_space=VMEM)
    return pl.pallas_call(
        functools.partial(causal_kernel, count // 2),
        out_shape=jax.ShapeDtypeStruct((rows, heads * HEAD_DIM), BF16),
        in_specs=[vmem] * 2,
        out_specs=vmem,
        scratch_shapes=[
            VMEM((count,) + kv.shape, BF16),
            VMEM(q.shape, F32),
            VMEM(q.shape, F32),
            pltpu.SemaphoreType.DMA((count,)),
            pltpu.SemaphoreType.DMA((count,)),
            pltpu.SemaphoreType.DMA((count,)),
        ],
        compiler_params=pltpu.CompilerParams(
            collective_id=collective_id, has_side_effects=True, vmem_limit_bytes=32 * 2**20
        ),
        name="causal_attention",
    )(q, kv)


def window_kernel(count, q_ref, kv_ref, o_ref, tail, acc, lsum, send, recv):
    s = lax.axis_index("seq")
    kv_heads, rows = kv_ref.shape[1], kv_ref.shape[2]
    group = q_ref.shape[0] // kv_heads
    has_next, has_last = s < count - 1, s > 0
    barrier = pltpu.get_barrier_semaphore()

    @pl.when(has_next)
    def _():
        pl.semaphore_signal(barrier, inc=1, device_id={"seq": s + 1}, device_id_type=MESH)

    @pl.when(has_last)
    def _():
        pl.semaphore_signal(barrier, inc=1, device_id={"seq": s - 1}, device_id_type=MESH)

    pl.semaphore_wait(barrier, has_next.astype(jnp.int32) + has_last.astype(jnp.int32))
    copy = remote(
        kv_ref.at[:, :, pl.ds(rows - WINDOW, WINDOW), :], tail, send.at[0], recv.at[0],
        {"seq": s + 1},
    )

    @pl.when(has_next)
    def _():
        copy.start()

    def own(h, carry):
        attend(
            q_ref, kv_ref[0, h], kv_ref[1, h], acc, lsum, h, group,
            lambda row, col: (col <= row) & (row - col < WINDOW), True,
        )
        return carry

    lax.fori_loop(0, kv_heads, own, 0)

    @pl.when(has_last)
    def _():
        copy.wait_recv()

        def body(h, carry):
            attend(
                q_ref, tail[0, h], tail[1, h], acc, lsum, h, group,
                lambda row, col: col > row, False, (0, WINDOW),
            )
            return carry

        lax.fori_loop(0, kv_heads, body, 0)

    write_heads(o_ref, acc, lsum)

    @pl.when(has_next)
    def _():
        copy.wait_send()


def window_attention(q, kv, count, collective_id):
    heads, rows, _ = q.shape
    vmem = pl.BlockSpec(memory_space=VMEM)
    return pl.pallas_call(
        functools.partial(window_kernel, count),
        out_shape=jax.ShapeDtypeStruct((rows, heads * HEAD_DIM), BF16),
        in_specs=[vmem] * 2,
        out_specs=vmem,
        scratch_shapes=[
            VMEM((2, kv.shape[1], WINDOW, HEAD_DIM), BF16),
            VMEM(q.shape, F32),
            VMEM(q.shape, F32),
            pltpu.SemaphoreType.DMA((1,)),
            pltpu.SemaphoreType.DMA((1,)),
        ],
        compiler_params=pltpu.CompilerParams(
            collective_id=collective_id, has_side_effects=True, vmem_limit_bytes=24 * 2**20
        ),
        name="window_attention",
    )(q, kv)


def fused_kernel(
    levels, heads, kv_heads, keep,
    x_hbm, gain1_hbm, gain2_hbm, gain3_hbm, fine_hbm, coarse_hbm,
    wq_hbm, wk_hbm, wv_hbm, wo_hbm, lwq_hbm, lwk_hbm, lwv_hbm,
    hidden_ref, lq_ref, kv2,
    buf, w, wo, gains, xg, acc, ss, ss_first, q_all, kv_buf, out, lsum, att,
    terms, own, landed, passed, proj, mine, stats, cos_ref, sin_ref, fine, coarse, q_up, out_up, lsum_up, up_num, up_sum, got_num, got_sum,
    x_sem, gain_sem, w_sem, wo_sem, ag_send, ag_recv, up_sem, side_sem, kv_sem,
    rs_send, rs_recv, st_send, st_recv, tail_sem, down_send, down_recv, back_send, back_recv,
):
    me = lax.axis_index("tp")
    s = lax.axis_index("seq")
    z, c = s // 2, s % 2
    mate = s + 1 - 2 * c
    has_up, has_down = z < levels - 1, z > 0
    top, helper = z == levels - 1, z == levels - 2
    next_row, prev_row = s < 2 * levels - 1, s > 0
    rows, cols = hidden_ref.shape
    chunk_rows, half_rows = rows // PARTS, rows // PARTS // 2
    block, half = rows // 2, rows // 4
    chunks = cols // HEAD_DIM
    ones = jnp.ones((8, HEAD_DIM), F32)
    highest = lax.Precision.HIGHEST
    owners = [xor(me, bits) for bits in range(4)]
    peers = [{"tp": owner} for owner in owners]
    along_x, along_y = peers[1], peers[2]
    qc, kc = heads * HEAD_DIM, kv_heads * HEAD_DIM
    kvc = 2 * kc
    group = heads // kv_heads

    x_loads = []
    for part in range(PARTS):
        span = pl.ds(part * chunk_rows, chunk_rows)
        copy = pltpu.make_async_copy(x_hbm.at[span], buf.at[0, span], x_sem.at[part])
        copy.start()
        x_loads.append(copy)
    gain_loads = []
    pairs = (
        (gain1_hbm, gains.at[0]), (gain2_hbm, gains.at[1]), (gain3_hbm, gains.at[2]),
        (fine_hbm, fine), (coarse_hbm, coarse),
    )
    for i, (ref, target) in enumerate(pairs):
        copy = pltpu.make_async_copy(ref, target, gain_sem.at[i])
        copy.start()
        gain_loads.append(copy)

    def weight_loads(key, value, query):
        loads = []
        for slot in range(4):
            span = pl.ds(pl.multiple_of(owners[slot] * cols, cols), cols)
            spec = ((key, 0, kc), (value, kc, kc), (query, kvc, qc))
            loads.append(
                [
                    pltpu.make_async_copy(
                        ref.at[span, :], w.at[slot, :, pl.ds(begin, width)], w_sem.at[slot, i]
                    )
                    for i, (ref, begin, width) in enumerate(spec)
                ]
            )
        return loads

    first_loads = weight_loads(wk_hbm, wv_hbm, wq_hbm)
    wo_loads = []
    for bits in (3, 1, 2, 0):
        span = pl.ds(pl.multiple_of(owners[bits] * cols, cols), cols)
        wo_loads.append(pltpu.make_async_copy(wo_hbm.at[:, span], wo.at[bits], wo_sem.at[bits]))

    barrier = pltpu.get_barrier_semaphore()
    for peer in (*peers[1:], {"seq": mate}):
        pl.semaphore_signal(barrier, inc=1, device_id=peer, device_id_type=MESH)

    @pl.when(has_up)
    def _():
        pl.semaphore_signal(barrier, inc=1, device_id={"seq": s + 2}, device_id_type=MESH)

    @pl.when(has_down)
    def _():
        pl.semaphore_signal(barrier, inc=1, device_id={"seq": s - 2}, device_id_type=MESH)

    @pl.when(has_up & (c == 1))
    def _():
        pl.semaphore_signal(barrier, inc=1, device_id={"seq": s + 1}, device_id_type=MESH)

    @pl.when(has_down & (c == 0))
    def _():
        pl.semaphore_signal(barrier, inc=1, device_id={"seq": s - 1}, device_id_type=MESH)

    far = (has_up & (c == 1)) | (has_down & (c == 0))
    pl.semaphore_wait(
        barrier,
        4 + has_up.astype(jnp.int32) + has_down.astype(jnp.int32) + far.astype(jnp.int32),
    )

    def gather_moves(store, first, count, part, base):
        begin = pl.multiple_of(part * count, count)
        top, bottom = pl.ds(begin, count // 2), pl.ds(begin + count // 2, count // 2)
        spec = (
            (store.at[0, top], store.at[1, top], along_x),
            (store.at[0, bottom], store.at[2, bottom], along_y),
            (store.at[0, bottom], store.at[1, bottom], along_x),
            (store.at[0, top], store.at[2, top], along_y),
            (store.at[1, top], store.at[3, top], along_y),
            (store.at[2, bottom], store.at[3, bottom], along_x),
        )
        at = first + part * 6 + base
        return [
            remote(source, target, ag_send.at[at + i], ag_recv.at[at + i], device)
            for i, (source, target, device) in enumerate(spec)
        ]

    def moves(part):
        return gather_moves(buf, 0, chunk_rows, part, 0)

    def moves2(part):
        return gather_moves(proj, 6 * PARTS, block, part, 0)

    def kv_part(owner, part, count):
        here = pl.ds(pl.multiple_of(part * chunk_rows, chunk_rows), chunk_rows)
        return kv_buf.at[owner, :, pl.ds(0, count), here]

    def up(owner, part, count):
        at, ref = owner * PARTS + part, kv_part(owner, part, count)
        return remote(ref, ref, up_sem.at[at], kv_sem.at[at], {"seq": s + 2})

    def side(owner, part, count):
        at, ref = owner * PARTS + part, kv_part(owner, part, count)
        return remote(ref, ref, side_sem.at[at], kv_sem.at[at], {"seq": mate})

    def lift(owner, part, act):
        @pl.when(z < levels - 2)
        def _():
            act(up(owner, part, kv_heads))

        @pl.when(helper)
        def _():
            act(up(owner, part, keep))

    def launch(copy):
        copy.start()

    def sent(copy):
        copy.wait_send()

    def arrive(owner, part):
        with jax.named_scope("arrive"):
            up(owner, part, kv_heads).wait_recv()
            side(owner, part, kv_heads).start()
            lift(owner, part, launch)

    def arrive_top(owner, part):
        with jax.named_scope("arrive_top"):
            up(owner, part, keep).wait_recv()
            side(owner, part, keep).start()

    down_heads = pl.ds(keep * group, group)

    def query_down(part):
        span = pl.ds(pl.multiple_of(part * block, block), block)
        return remote(
            q_all.at[down_heads, span], q_up.at[:, span], down_send.at[part], down_recv.at[part],
            {"seq": s - 2},
        )

    backs = [
        remote(source, target, back_send.at[i], back_recv.at[i], {"seq": s + 2})
        for i, (source, target) in enumerate(
            (
                (up_sum, got_sum),
                (up_num.at[:, pl.ds(block, block)], got_num.at[:, pl.ds(block, block)]),
                (up_num.at[:, pl.ds(0, block)], got_num.at[:, pl.ds(0, block)]),
            )
        )
    ]

    def multiply(slot, count, begin, width, fresh):
        product = jnp.dot(
            xg[0:count, :], w[slot, :, begin : begin + width], preferred_element_type=F32
        )
        if fresh:
            acc[0:count, begin : begin + width] = product
        else:
            acc[0:count, begin : begin + width] += product

    def gain_row(which, slot, j):
        return gains[which, pl.ds(owners[slot] * chunks + j, 1), :]

    def prepare(slot, part):
        here = pl.ds(pl.multiple_of(part * chunk_rows, chunk_rows), chunk_rows)
        squares = None
        for j in range(chunks):
            lanes = slice(j * HEAD_DIM, (j + 1) * HEAD_DIM)
            wide = buf[slot, here, lanes].astype(F32)
            squares = wide * wide if squares is None else squares + wide * wide
            proj[slot, here, lanes] = (wide * gain_row(0, slot, j)).astype(BF16)
        if slot == 0:
            ss_first[here, :] = squares
        else:
            ss_first[here, :] += squares

    def row_factor(squares):
        total = jnp.sum(squares, axis=-1, keepdims=True)
        return lax.rsqrt(jnp.broadcast_to(total, squares.shape) * (1.0 / D) + NORM_EPS)

    def rotated(begin, count, factor, span):
        u = acc[0:count, begin : begin + HEAD_DIM] * factor
        turned = pltpu.roll(u, HEAD_DIM // 2, 1)
        return (u * cos_ref[span, :] + turned * sin_ref[span, :]).astype(BF16)

    for copy in x_loads[:1]:
        copy.wait()
    def launch_group(part, some):
        copies = moves(part)
        for i in some:
            copies[i].start()

    launch_group(0, range(4))
    for copy in x_loads[1:]:
        copy.wait()
    launch_group(1, range(2))
    for copy in gain_loads:
        copy.wait()
    for bundle in first_loads:
        for copy in bundle[:2]:
            copy.start()
    for begin in range(0, rows, 64):
        span = slice(begin, begin + 64)
        cosine, sine = coarse[0, pl.ds(s, 1), :], coarse[1, pl.ds(s, 1), :]
        cos_ref[span, :] = fine[0, span] * cosine - fine[1, span] * sine
        sin_ref[span, :] = fine[1, span] * cosine + fine[0, span] * sine

    def first_part(part, carry):
        with jax.named_scope("first_part"):
            return one_part(part, carry)

    def relay(part):
        copies = moves(part)
        copies[0].wait_recv()
        copies[4].start()
        copies[1].wait_recv()
        copies[5].start()

        @pl.when(part < PARTS - 1)
        def _():
            launch_group(part + 1, (2, 3))

        @pl.when(part < PARTS - 2)
        def _():
            launch_group(part + 2, (0, 1))

    def one_part(part, carry):
        span = pl.ds(pl.multiple_of(part * chunk_rows, chunk_rows), chunk_rows)

        def take(slot):
            prepare(slot, part)

            @pl.when(part == 0)
            def _():
                for copy in first_loads[slot][:2]:
                    copy.wait()

            product = jnp.dot(proj[slot, span, :], w[slot, :, 0:kvc], preferred_element_type=F32)
            if slot == 0:
                acc[0:chunk_rows, 0:kvc] = product
            else:
                acc[0:chunk_rows, 0:kvc] += product

        copies = moves(part)
        take(0)

        @pl.when(part == 0)
        def _():
            relay(0)

        @pl.when(part == PARTS // 4)
        def _():
            for bundle in first_loads:
                bundle[2].start()

        @pl.when(part == PARTS // 2)
        def _():
            for copy in wo_loads:
                copy.start()

        copies[2].wait_recv()
        take(1)
        copies[3].wait_recv()
        take(2)

        @pl.when(part < PARTS - 1)
        def _():
            relay(part + 1)

        @pl.when(part == PARTS // 2)
        def _():
            queries(0)

        copies[4].wait_recv()
        copies[5].wait_recv()
        take(3)
        factor = row_factor(ss_first[span, :])
        for h in range(kv_heads):
            kv_buf[s, 0, h, span, :] = rotated(h * HEAD_DIM, chunk_rows, factor, span)
            place = kc + h * HEAD_DIM
            kv_buf[s, 1, h, span, :] = (
                acc[0:chunk_rows, place : place + HEAD_DIM] * factor
            ).astype(BF16)

        @pl.when((c == 0) | helper)
        def _():
            side(s, part, kv_heads).start()

        lift(s, part, launch)

        def forward(k, carry):
            @pl.when(part >= 2 * k - 1)
            def _():
                arrive(s - 2 * k, part - 2 * k + 1)

            return carry

        @pl.when(has_up)
        def _():
            lax.fori_loop(1, z + 1, forward, 0)

        return carry

    def queries(which):
        span = pl.ds(pl.multiple_of(which * block, block), block)

        if which == 0:
            for bundle in first_loads:
                bundle[2].wait()

        acc[:, kvc : kvc + qc] = sum(
            jnp.dot(proj[slot, span, :], w[slot, :, kvc : kvc + qc], preferred_element_type=F32)
            for slot in range(4)
        )
        factor = row_factor(ss_first[span, :])
        for h in reversed(range(heads)):
            q_all[h, span, :] = rotated(kvc + h * HEAD_DIM, block, factor, span)

        @pl.when(top)
        def _():
            query_down(which).start()

    lax.fori_loop(0, PARTS, first_part, 0)
    queries(1)

    second_loads = weight_loads(lwk_hbm, lwv_hbm, lwq_hbm)

    def fetch(slot):
        for copy in second_loads[slot]:
            copy.start()

    with jax.named_scope("own"):
        for h in range(kv_heads):
            attend(
                q_all, kv_buf[s, 0, h], kv_buf[s, 1, h], out, lsum, h, group,
                lambda row, col: col <= row, True,
            )

    def visit_heads(owner, begin, end, span):
        for h in range(begin, end):
            attend(
                q_all, kv_buf[owner, 0, h, span], kv_buf[owner, 1, h, span], out, lsum, h, group,
                None, False,
            )

    def visit(owner, span):
        with jax.named_scope("visit"):
            @pl.when(top)
            def _():
                visit_heads(owner, 0, keep, span)

            @pl.when(has_up)
            def _():
                visit_heads(owner, 0, kv_heads, span)

    def visit_up(owner, first, span):
        with jax.named_scope("visit_up"):
            attend(
                q_up, kv_buf[owner, 0, keep, span], kv_buf[owner, 1, keep, span], out_up, lsum_up,
                0, group, None, first,
            )

    def send_back():
        for g in range(group):
            up_sum[g] = lax.dot_general(
                ones, lsum_up[g], (((1,), (1,)), ((), ())), precision=highest,
                preferred_element_type=F32,
            )
        for part, copy in ((1, backs[1]), (0, backs[2])):
            span = slice(part * block, (part + 1) * block)
            for g in range(group):
                up_num[g, span] = out_up[g, span].astype(BF16)
            copy.start()
            if part == 1:
                backs[0].start()

    @pl.when(helper | (c == 1))
    def _():
        for part in range(PARTS):
            side(mate, part, kv_heads).wait_recv()

    @pl.when(c == 1)
    def _():
        with jax.named_scope("mate"):
            visit_heads(s - 1, 0, kv_heads, pl.ds(0, rows))

    @pl.when(helper)
    def _():
        for part in range(2):
            query_down(part).wait_recv()
        visit_up(s, True, pl.ds(0, rows))
        visit_up(mate, False, pl.ds(0, rows))

    def turn(r, carry):
        def take_in(k, carry):
            owner, part = s - 2 * k, r - 2 * k + 1

            @pl.when((part >= 0) & (part < PARTS))
            def _():
                @pl.when(top)
                def _():
                    arrive_top(owner, part)

                @pl.when((r >= PARTS) & has_up)
                def _():
                    arrive(owner, part)

            return carry

        def level(k, carry):
            owner, other = s - 2 * k, mate - 2 * k
            whole = pl.ds(0, rows)

            @pl.when(r - 2 * k + 1 == PARTS - 1)
            def _():
                @pl.when(helper)
                def _():
                    visit_up(owner, False, whole)
                    for p in range(PARTS):
                        side(other, p, kv_heads).wait_recv()
                    visit_up(other, False, whole)

                    @pl.when(k == z)
                    def _():
                        send_back()

                def both(j, carry):
                    @pl.when((j == 1) & top)
                    def _():
                        for p in range(PARTS):
                            side(other, p, keep).wait_recv()

                    @pl.when((j == 1) & (z < levels - 2))
                    def _():
                        for p in range(PARTS):
                            side(other, p, kv_heads).wait_recv()

                    visit(owner + j * (other - owner), whole)
                    return carry

                lax.fori_loop(0, 2, both, 0)

            return carry

        lax.fori_loop(1, z + 1, take_in, 0)
        lax.fori_loop(1, z + 1, level, 0)
        return carry

    lax.fori_loop(1, PARTS + 2 * z - 1, turn, 0)

    def write_part(part):
        span = slice(part * block, (part + 1) * block)

        @pl.when(top)
        def _():
            if part == 1:
                backs[0].wait_recv()
            backs[2 - part].wait_recv()
            for g in range(group):
                column = lax.dot_general(
                    got_sum[g, :, span], ones * (0.125 / HEAD_DIM), (((0,), (0,)), ((), ())),
                    precision=highest, preferred_element_type=F32,
                )
                lsum[keep * group + g, span] += column
                out[keep * group + g, span] += got_num[g, span].astype(F32)

        for h in range(heads):
            denominator = jnp.sum(lsum[h, span], axis=-1, keepdims=True)
            att[span, h * HEAD_DIM : (h + 1) * HEAD_DIM] = (out[h, span] / denominator).astype(BF16)

    def reduce_moves(part):
        base = part * block
        top, bottom = pl.ds(base, half), pl.ds(base + half, half)
        spec = (
            (terms.at[2, top], along_x),
            (terms.at[2, bottom], along_y),
            (terms.at[0, top], along_x),
            (terms.at[1, bottom], along_y),
            (passed.at[part, 1], along_x),
            (passed.at[part, 0], along_y),
        )
        return [
            remote(
                source, landed.at[part, i], rs_send.at[part * 6 + i], rs_recv.at[part * 6 + i], device
            )
            for i, (source, device) in enumerate(spec)
        ]

    def product(bits, part):
        span = slice(part * block, (part + 1) * block)
        value = jnp.dot(att[span, :], wo[bits], preferred_element_type=F32)
        if bits == 0:
            own[span, :] = value
        else:
            terms[bits - 1, span, :] = value.astype(BF16)

    def pass_on(part):
        copies = reduce_moves(part)
        base = part * block
        copies[0].wait_recv()
        passed[part, 0] = (
            terms[1, base : base + half].astype(F32) + landed[part, 0].astype(F32)
        ).astype(BF16)
        copies[5].start()
        copies[1].wait_recv()
        passed[part, 1] = (
            terms[0, base + half : base + block].astype(F32) + landed[part, 1].astype(F32)
        ).astype(BF16)
        copies[4].start()

    def swaps(part):
        return [
            remote(
                mine.at[part], stats.at[part, bits - 1],
                st_send.at[part * 3 + bits - 1], st_recv.at[part * 3 + bits - 1], peers[bits],
            )
            for bits in (3, 1, 2)
        ]

    def finalize(part):
        copies = reduce_moves(part)
        for i in (2, 3, 5, 4):
            copies[i].wait_recv()
        base = part * block
        span = slice(base, base + block)
        lanes = None
        for j in range(chunks):
            cut = slice(j * HEAD_DIM, (j + 1) * HEAD_DIM)
            above = landed[part, 2, :, cut].astype(F32) + landed[part, 5, :, cut].astype(F32)
            below = landed[part, 3, :, cut].astype(F32) + landed[part, 4, :, cut].astype(F32)
            value = own[span, cut] + jnp.concatenate([above, below], axis=0)
            own[span, cut] = value
            proj[0, span, cut] = value.astype(BF16)
            lanes = value * value if lanes is None else lanes + value * value
        for copy in moves2(part)[:2]:
            copy.start()
        mine[part] = lax.dot_general(
            ones, lanes, (((1,), (1,)), ((), ())), precision=highest, preferred_element_type=F32
        )
        for swap in swaps(part):
            swap.start()
        for copy in moves2(part)[2:4]:
            copy.start()

    def forward_rows(part):
        copies = moves2(part)
        copies[0].wait_recv()
        copies[4].start()
        copies[1].wait_recv()
        copies[5].start()

    def post_factor(part):
        for swap in swaps(part):
            swap.wait_recv()
        summed = mine[part] + stats[part, 0] + stats[part, 1] + stats[part, 2]
        column = lax.dot_general(
            summed, ones * 0.125, (((0,), (0,)), ((), ())), precision=highest,
            preferred_element_type=F32,
        )
        return lax.rsqrt(column * (1.0 / D) + NORM_EPS)

    def take2(slot, part, factor):
        span = slice(part * block, (part + 1) * block)
        squares = None
        for j in range(chunks):
            cut = slice(j * HEAD_DIM, (j + 1) * HEAD_DIM)
            summed = own[span, cut] if slot == 0 else proj[slot, span, cut].astype(F32)
            added = buf[slot, span, cut].astype(F32) + summed * factor * gain_row(1, slot, j)
            rounded = added.astype(BF16)
            if slot == 0:
                hidden_ref[span, cut] = rounded
            wide = rounded.astype(F32)
            squares = wide * wide if squares is None else squares + wide * wide
            xg[:, cut] = (wide * gain_row(2, slot, j)).astype(BF16)
        if slot == 0:
            ss[...] = squares
        else:
            ss[...] += squares
        if part == 1:
            for copy in second_loads[slot]:
                copy.wait()
        multiply(slot, block, 0, kvc, slot == 0)
        multiply(slot, block, kvc, qc, slot == 0)

    def finish2(part):
        span = pl.ds(part * block, block)
        place_rows = pl.ds(WINDOW + part * block, block)
        factor = row_factor(ss[...])
        for h in range(kv_heads):
            kv2[0, h, place_rows, :] = rotated(h * HEAD_DIM, block, factor, span)
            place = kc + h * HEAD_DIM
            kv2[1, h, place_rows, :] = (acc[:, place : place + HEAD_DIM] * factor).astype(BF16)
        for h in range(heads):
            lq_ref[h, span, :] = rotated(kvc + h * HEAD_DIM, block, factor, span)

    tail = remote(
        kv2.at[:, :, pl.ds(rows, WINDOW)], kv2.at[:, :, pl.ds(0, WINDOW)],
        tail_sem.at[0], tail_sem.at[1], {"seq": s + 1},
    )

    def scoped(name, run, *given):
        with jax.named_scope(name):
            return run(*given)

    for copy in wo_loads:
        copy.wait()
    late, soon = 0, 1
    scoped("write_part", write_part, soon)
    copies = reduce_moves(soon)
    scoped("product", product, 3, soon)
    copies[0].start()
    copies[1].start()
    scoped("product", product, 1, soon)
    copies[2].start()
    scoped("product", product, 2, soon)
    copies[3].start()
    scoped("product", product, 0, soon)
    fetch(0)
    scoped("write_part", write_part, late)
    for bits in (3, 1, 2, 0):
        scoped("product", product, bits, late)
    scoped("pass_on", pass_on, soon)
    for copy in reduce_moves(late)[:4]:
        copy.start()
    fetch(1)
    fetch(2)
    fetch(3)
    scoped("finalize", finalize, soon)
    scoped("pass_on", pass_on, late)
    factor = scoped("post_factor", post_factor, soon)
    scoped("take2", take2, 0, soon, factor)
    scoped("forward_rows", forward_rows, soon)
    moves2(soon)[2].wait_recv()
    scoped("take2", take2, 1, soon, factor)
    moves2(soon)[3].wait_recv()
    scoped("take2", take2, 2, soon, factor)
    scoped("finalize", finalize, late)
    moves2(soon)[4].wait_recv()
    moves2(soon)[5].wait_recv()
    scoped("take2", take2, 3, soon, factor)
    scoped("finish2", finish2, soon)

    @pl.when(next_row)
    def _():
        tail.start()

    @pl.when(s == 0)
    def _():
        kv2[:, :, 0:WINDOW, :] = jnp.zeros((2, kv_heads, WINDOW, HEAD_DIM), BF16)

    factor = scoped("post_factor", post_factor, late)
    scoped("take2", take2, 0, late, factor)
    scoped("forward_rows", forward_rows, late)
    moves2(late)[2].wait_recv()
    scoped("take2", take2, 1, late, factor)
    moves2(late)[3].wait_recv()
    scoped("take2", take2, 2, late, factor)
    moves2(late)[4].wait_recv()
    moves2(late)[5].wait_recv()
    scoped("take2", take2, 3, late, factor)
    scoped("finish2", finish2, late)

    @pl.when(prev_row)
    def _():
        tail.wait_recv()

    def drain_first(part, carry):
        for copy in moves(part):
            copy.wait_send()

        lift(s, part, sent)

        @pl.when((c == 0) | helper)
        def _():
            side(s, part, kv_heads).wait_send()

        def drain_level(k, carry):
            lift(s - 2 * k, part, sent)

            @pl.when(has_up)
            def _():
                side(s - 2 * k, part, kv_heads).wait_send()

            @pl.when(top)
            def _():
                side(s - 2 * k, part, keep).wait_send()

            return carry

        lax.fori_loop(1, z + 1, drain_level, 0)
        return carry

    lax.fori_loop(0, PARTS, drain_first, 0)

    @pl.when(helper)
    def _():
        for copy in backs:
            copy.wait_send()

    @pl.when(top)
    def _():
        for part in range(2):
            query_down(part).wait_send()

    for part in range(2):
        for copy in (*reduce_moves(part), *swaps(part), *moves2(part)):
            copy.wait_send()

    @pl.when(next_row)
    def _():
        tail.wait_send()


def fused(x, gains, first, wo, second, count, collective_id):
    rows, cols = x.shape
    wq, wk, wv = first
    heads, kv_heads = wq.shape[1] // HEAD_DIM, wk.shape[1] // HEAD_DIM
    total = wq.shape[1] + 2 * wk.shape[1]
    depth = wo.shape[0]
    group, block = heads // kv_heads, rows // 2
    vmem = pl.BlockSpec(memory_space=VMEM)
    hbm = pl.BlockSpec(memory_space=pltpu.HBM)
    dma = pltpu.SemaphoreType.DMA
    folded = [gain.reshape(-1, HEAD_DIM) for gain in gains]
    turns = 10000.0 ** (-2.0 * np.arange(HEAD_DIM // 2) / HEAD_DIM)
    turns = np.concatenate([turns, turns])
    sign = np.where(np.arange(HEAD_DIM) < HEAD_DIM // 2, -1.0, 1.0)

    def table(places):
        angles = places[:, None] * turns
        return jnp.asarray(np.stack([np.cos(angles), sign * np.sin(angles)]), F32)

    tables = (table(np.arange(rows)), table(np.arange(count) * rows))
    far = [x, *folded, *tables, wq, wk, wv, wo, *second]
    far = [pltpu.with_memory_space_constraint(array, pltpu.HBM) for array in far]
    return pl.pallas_call(
        functools.partial(fused_kernel, count // 2, heads, kv_heads, kv_heads - 1),
        out_shape=(
            jax.ShapeDtypeStruct((rows, cols), BF16),
            jax.ShapeDtypeStruct((heads, rows, HEAD_DIM), BF16),
            jax.ShapeDtypeStruct((2, kv_heads, WINDOW + rows, HEAD_DIM), BF16),
        ),
        in_specs=[hbm] * 13,
        out_specs=(vmem, vmem, vmem),
        scratch_shapes=[
            VMEM((4, rows, cols), BF16),
            VMEM((4, cols, total), BF16),
            VMEM((4, depth, cols), BF16),
            VMEM((3,) + folded[0].shape, F32),
            VMEM((block, cols), BF16),
            VMEM((block, total), F32),
            VMEM((block, HEAD_DIM), F32),
            VMEM((rows, HEAD_DIM), F32),
            VMEM((heads, rows, HEAD_DIM), BF16),
            VMEM((count, 2, kv_heads, rows, HEAD_DIM), BF16),
            VMEM((heads, rows, HEAD_DIM), F32),
            VMEM((heads, rows, HEAD_DIM), F32),
            VMEM((rows, depth), BF16),
            VMEM((3, rows, cols), BF16),
            VMEM((rows, cols), F32),
            VMEM((2, 6, block // 2, cols), BF16),
            VMEM((2, 2, block // 2, cols), BF16),
            VMEM((4, rows, cols), BF16),
            VMEM((2, 8, block), F32),
            VMEM((2, 3, 8, block), F32),
            VMEM((rows, HEAD_DIM), F32),
            VMEM((rows, HEAD_DIM), F32),
            VMEM((2, rows, HEAD_DIM), F32),
            VMEM((2, count, HEAD_DIM), F32),
            VMEM((group, rows, HEAD_DIM), BF16),
            VMEM((group, rows, HEAD_DIM), F32),
            VMEM((group, rows, HEAD_DIM), F32),
            VMEM((group, rows, HEAD_DIM), BF16),
            VMEM((group, 8, rows), F32),
            VMEM((group, rows, HEAD_DIM), BF16),
            VMEM((group, 8, rows), F32),
            dma((PARTS,)),
            dma((5,)),
            dma((4, 3)),
            dma((4,)),
            dma((6 * PARTS + 12,)),
            dma((6 * PARTS + 12,)),
            dma((count * PARTS,)),
            dma((count * PARTS,)),
            dma((count * PARTS,)),
            dma((12,)),
            dma((12,)),
            dma((6,)),
            dma((6,)),
            dma((2,)),
            dma((2,)),
            dma((2,)),
            dma((3,)),
            dma((3,)),
        ],
        compiler_params=pltpu.CompilerParams(
            collective_id=collective_id, has_side_effects=True, vmem_limit_bytes=50 * 2**20
        ),
        name="fused",
    )(*far)


def finish_kernel(hid_ref, q_ref, kv_ref, hid_hbm, o_hbm, o_ref, sems):
    rows = hid_ref.shape[0]
    heads, kv_heads = q_ref.shape[0], kv_ref.shape[1]
    group, block = heads // kv_heads, rows // 2
    begins = jnp.where(lax.axis_index("seq") > 0, 0, WINDOW - 1)
    copies = [pltpu.make_async_copy(hid_ref, hid_hbm, sems.at[kv_heads])]
    copies[0].start()
    for h in range(kv_heads):
        for part in range(2):
            q = q_ref[h * group : (h + 1) * group, part * block : (part + 1) * block]
            q = q.reshape(group * block, HEAD_DIM)
            keys = kv_ref[0, h, part * block : part * block + WINDOW + block]
            values = kv_ref[1, h, part * block : part * block + WINDOW + block]
            scores = lax.dot_general(
                q, keys, (((1,), (1,)), ((), ())), preferred_element_type=F32
            )
            weights = jnp.exp2(jnp.tanh(scores * INNER) * OUTER)
            row = lax.broadcasted_iota(jnp.int32, (block, WINDOW + block), 0)
            col = lax.broadcasted_iota(jnp.int32, (block, WINDOW + block), 1)
            least = jnp.maximum(row, begins) if part == 0 else row
            mask = (col > least) & (col <= row + WINDOW)
            weights = jnp.concatenate(
                [jnp.where(mask, weights[g * block : (g + 1) * block], 0.0) for g in range(group)],
                axis=0,
            )
            denominator = jnp.sum(weights, axis=-1, keepdims=True)
            numerator = jnp.dot(weights.astype(BF16), values, preferred_element_type=F32)
            result = (numerator / denominator).astype(BF16)
            for g in range(group):
                head = h * group + g
                o_ref[part * block : (part + 1) * block, head * HEAD_DIM : (head + 1) * HEAD_DIM] = (
                    result[g * block : (g + 1) * block]
                )
        lanes = pl.ds(h * group * HEAD_DIM, group * HEAD_DIM)
        copy = pltpu.make_async_copy(o_ref.at[:, lanes], o_hbm.at[:, lanes], sems.at[h])
        copy.start()
        copies.append(copy)
    for copy in copies:
        copy.wait()


def finish(hidden, q, kv):
    heads, rows, _ = q.shape
    vmem = pl.BlockSpec(memory_space=VMEM)
    hbm = pl.BlockSpec(memory_space=pltpu.HBM)
    shape = jax.ShapeDtypeStruct((rows, heads * HEAD_DIM), BF16)
    return pl.pallas_call(
        finish_kernel,
        out_shape=(jax.ShapeDtypeStruct(hidden.shape, BF16), shape),
        in_specs=[vmem] * 3,
        out_specs=(hbm, hbm),
        scratch_shapes=[
            VMEM(shape.shape, BF16),
            pltpu.SemaphoreType.DMA((kv.shape[1] + 1,)),
        ],
        compiler_params=pltpu.CompilerParams(vmem_limit_bytes=8 * 2**20),
        name="finish",
    )(hidden, q, kv)


def rms_scaled(values, weights):
    widened = values.astype(F32)
    factor = lax.rsqrt(jnp.mean(widened * widened, axis=-1, keepdims=True) + NORM_EPS)
    return widened * factor * weights


def plain_gather_project(x, gain, cos, sin, wq, wk, wv):
    full = lax.all_gather(x, "tp", axis=1, tiled=True)
    normed = rms_scaled(full, gain).astype(BF16)

    def heads_of(weight):
        product = jnp.dot(normed, weight, preferred_element_type=F32)
        return jnp.swapaxes(product.reshape(x.shape[0], -1, HEAD_DIM), 0, 1)

    def rotated(u):
        return (u * cos + jnp.roll(u, HEAD_DIM // 2, axis=-1) * sin).astype(BF16)

    keys, values = rotated(heads_of(wk)), heads_of(wv).astype(BF16)
    return rotated(heads_of(wq)), jnp.stack([keys, values])


def plain_output_project(attended, tokens, gain, wo):
    cols = tokens.shape[1]
    partial_sum = jnp.dot(attended, wo, preferred_element_type=F32).astype(BF16)
    summed = lax.psum(partial_sum, "tp").astype(F32)
    added = rms_scaled(summed, gain)
    mine = lax.dynamic_slice_in_dim(added, lax.axis_index("tp") * cols, cols, 1)
    return (tokens.astype(F32) + mine).astype(BF16)


def local(
    sizes,
    tokens,
    attention_gain,
    query_weight,
    key_weight,
    value_weight,
    output_weight,
    post_gain,
    local_gain,
    local_query_weight,
    local_key_weight,
    local_value_weight,
):
    seq, tp = sizes
    rows, cols = tokens.shape
    first = (query_weight, key_weight, value_weight)
    second = (local_query_weight, local_key_weight, local_value_weight)
    if tp == 4 and cols % HEAD_DIM == 0 and rows == 2 * WINDOW and seq % 2 == 0 and seq > 4:
        gains = (attention_gain, post_gain, local_gain)
        return finish(*fused(tokens, gains, first, output_weight, second, seq, 0))
    places = lax.axis_index("seq") * rows + lax.iota(jnp.int32, rows)
    halfway = HEAD_DIM // 2
    exponents = jnp.arange(halfway, dtype=F32) * (2.0 / HEAD_DIM)
    frequency = jnp.power(F32(10000.0), -exponents)
    angles = places.astype(F32)[:, None] * frequency[None, :]
    cosine, sine = jnp.cos(angles), jnp.sin(angles)
    cos = jnp.concatenate([cosine, cosine], axis=-1)
    sin = jnp.concatenate([-sine, sine], axis=-1)
    lead = plain_gather_project(tokens, attention_gain, cos, sin, *first)
    attended = causal_attention(*lead, seq, 1)
    hidden = plain_output_project(attended, tokens, post_gain, output_weight)
    lq, lkv = plain_gather_project(hidden, local_gain, cos, sin, *second)
    return hidden, window_attention(lq, lkv, seq, 4)


def solution(mesh):
    in_specs = (
        P("seq", "tp"),
        P(),
        P(None, "tp"),
        P(None, "tp"),
        P(None, "tp"),
        P("tp", None),
        P(),
        P(),
        P(None, "tp"),
        P(None, "tp"),
        P(None, "tp"),
    )
    out_specs = (P("seq", "tp"), P("seq", "tp"))
    sizes = (mesh.shape["seq"], mesh.shape["tp"])
    body = functools.partial(local, sizes)
    return jax.shard_map(body, mesh=mesh, in_specs=in_specs, out_specs=out_specs, check_vma=False)
```

```python
import functools
import math
import types

import jax
import jax.numpy as jnp
import numpy as np
from jax import lax
from jax.experimental import pallas as pl
from jax.experimental.pallas import tpu as pltpu
from jax.sharding import PartitionSpec as P

D = 4608
HEADS = 32
HEAD_DIM = 128
WINDOW = 128

SOFT_CAP = 50.0
NORM_EPS = 1e-06
MESH = pl.DeviceIdType.MESH
VMEM = pltpu.VMEM
F32 = jnp.float32
BF16 = jnp.bfloat16
PARTS = 4
HANDED = 16
INNER = float(D // HEADS) ** (-0.5) / SOFT_CAP
OUTER = SOFT_CAP * math.log2(math.e)


def greet(peers):
    barrier = pltpu.get_barrier_semaphore()
    for peer in peers:
        pl.semaphore_signal(barrier, inc=1, device_id=peer, device_id_type=MESH)
    pl.semaphore_wait(barrier, len(peers))


def remote(source, target, send_sem, recv_sem, device):
    return pltpu.make_async_remote_copy(
        src_ref=source,
        dst_ref=target,
        send_sem=send_sem,
        recv_sem=recv_sem,
        device_id=device,
        device_id_type=MESH,
    )


def xor(index, bits):
    low, high = index % 2, index // 2
    if bits & 1:
        low = 1 - low
    if bits & 2:
        high = 1 - high
    return high * 2 + low


def attend(q_ref, keys, values, acc, lsum, h, group, allowed, first, row_span=None):
    q = q_ref[pl.ds(h * group, group)]
    if row_span is not None:
        q = q[:, row_span[0] : row_span[1]]
    rows = q.shape[1]
    q = q.reshape(group * rows, HEAD_DIM)
    scores = lax.dot_general(q, keys, (((1,), (1,)), ((), ())), preferred_element_type=F32)
    weights = jnp.exp2(jnp.tanh(scores * INNER) * OUTER)
    if allowed is not None:
        count = keys.shape[0]
        row = lax.broadcasted_iota(jnp.int32, (rows, count), 0)
        col = lax.broadcasted_iota(jnp.int32, (rows, count), 1)
        mask = allowed(row, col)
        weights = jnp.concatenate(
            [jnp.where(mask, weights[g * rows : (g + 1) * rows], 0.0) for g in range(group)], axis=0
        )
    lanes = weights[:, :HEAD_DIM]
    for begin in range(HEAD_DIM, keys.shape[0], HEAD_DIM):
        lanes = lanes + weights[:, begin : begin + HEAD_DIM]
    product = jnp.dot(weights.astype(BF16), values, preferred_element_type=F32)
    lanes = lanes.reshape(group, rows, HEAD_DIM)
    product = product.reshape(group, rows, HEAD_DIM)
    heads = pl.ds(h * group, group)
    span = pl.ds(0, rows)
    if first:
        lsum[heads, span] = lanes
        acc[heads, span] = product
    else:
        lsum[heads, span] += lanes
        acc[heads, span] += product


def write_heads(o_ref, acc, lsum):
    for h in range(acc.shape[0]):
        denominator = jnp.sum(lsum[h], axis=-1, keepdims=True)
        o_ref[:, h * HEAD_DIM : (h + 1) * HEAD_DIM] = (acc[h] / denominator).astype(BF16)


def causal_kernel(levels, q_ref, kv_ref, o_ref, buf, acc, lsum, up_sem, side_sem, recv):
    s = lax.axis_index("seq")
    z, c = s // 2, s % 2
    mate = s + 1 - 2 * c
    kv_heads = kv_ref.shape[1]
    group = q_ref.shape[0] // kv_heads
    has_up, has_down = z < levels - 1, z > 0

    barrier = pltpu.get_barrier_semaphore()
    pl.semaphore_signal(barrier, inc=1, device_id={"seq": mate}, device_id_type=MESH)

    @pl.when(has_up)
    def _():
        pl.semaphore_signal(barrier, inc=1, device_id={"seq": s + 2}, device_id_type=MESH)

    @pl.when(has_down)
    def _():
        pl.semaphore_signal(barrier, inc=1, device_id={"seq": s - 2}, device_id_type=MESH)

    pl.semaphore_wait(barrier, 1 + has_up.astype(jnp.int32) + has_down.astype(jnp.int32))

    def up(owner, source):
        return remote(source, buf.at[owner], up_sem.at[owner], recv.at[owner], {"seq": s + 2})

    def side(owner, source):
        return remote(source, buf.at[owner], side_sem.at[owner], recv.at[owner], {"seq": mate})

    @pl.when(has_up)
    def _():
        up(s, kv_ref).start()

    @pl.when(c == 0)
    def _():
        side(s, kv_ref).start()

    def own(h, carry):
        attend(
            q_ref, kv_ref[0, h], kv_ref[1, h], acc, lsum, h, group,
            lambda row, col: col <= row, True,
        )
        return carry

    lax.fori_loop(0, kv_heads, own, 0)

    def visit(owner):
        def body(h, carry):
            attend(
                q_ref, buf[owner, 0, h], buf[owner, 1, h], acc, lsum, h, group, None, False
            )
            return carry

        lax.fori_loop(0, kv_heads, body, 0)

    @pl.when(c == 1)
    def _():
        side(s - 1, buf.at[s - 1]).wait_recv()
        visit(s - 1)

    def level(k, carry):
        owner, other = s - 2 * k, mate - 2 * k
        up(owner, buf.at[owner]).wait_recv()

        @pl.when(has_up)
        def _():
            up(owner, buf.at[owner]).start()

        side(owner, buf.at[owner]).start()
        visit(owner)
        side(other, buf.at[other]).wait_recv()
        visit(other)
        return carry

    lax.fori_loop(1, z + 1, level, 0)
    write_heads(o_ref, acc, lsum)

    @pl.when(has_up)
    def _():
        up(s, kv_ref).wait_send()

    @pl.when(c == 0)
    def _():
        side(s, kv_ref).wait_send()

    def drain(k, carry):
        owner = s - 2 * k

        @pl.when(has_up)
        def _():
            up(owner, buf.at[owner]).wait_send()

        side(owner, buf.at[owner]).wait_send()
        return carry

    lax.fori_loop(1, z + 1, drain, 0)


def causal_attention(q, kv, count, collective_id):
    heads, rows, _ = q.shape
    vmem = pl.BlockSpec(memory_space=VMEM)
    return pl.pallas_call(
        functools.partial(causal_kernel, count // 2),
        out_shape=jax.ShapeDtypeStruct((rows, heads * HEAD_DIM), BF16),
        in_specs=[vmem] * 2,
        out_specs=vmem,
        scratch_shapes=[
            VMEM((count,) + kv.shape, BF16),
            VMEM(q.shape, F32),
            VMEM(q.shape, F32),
            pltpu.SemaphoreType.DMA((count,)),
            pltpu.SemaphoreType.DMA((count,)),
            pltpu.SemaphoreType.DMA((count,)),
        ],
        compiler_params=pltpu.CompilerParams(
            collective_id=collective_id, has_side_effects=True, vmem_limit_bytes=32 * 2**20
        ),
        name="causal_attention",
    )(q, kv)


def window_kernel(count, q_ref, kv_ref, o_ref, tail, acc, lsum, send, recv):
    s = lax.axis_index("seq")
    kv_heads, rows = kv_ref.shape[1], kv_ref.shape[2]
    group = q_ref.shape[0] // kv_heads
    has_next, has_last = s < count - 1, s > 0
    barrier = pltpu.get_barrier_semaphore()

    @pl.when(has_next)
    def _():
        pl.semaphore_signal(barrier, inc=1, device_id={"seq": s + 1}, device_id_type=MESH)

    @pl.when(has_last)
    def _():
        pl.semaphore_signal(barrier, inc=1, device_id={"seq": s - 1}, device_id_type=MESH)

    pl.semaphore_wait(barrier, has_next.astype(jnp.int32) + has_last.astype(jnp.int32))
    copy = remote(
        kv_ref.at[:, :, pl.ds(rows - WINDOW, WINDOW), :], tail, send.at[0], recv.at[0],
        {"seq": s + 1},
    )

    @pl.when(has_next)
    def _():
        copy.start()

    def own(h, carry):
        attend(
            q_ref, kv_ref[0, h], kv_ref[1, h], acc, lsum, h, group,
            lambda row, col: (col <= row) & (row - col < WINDOW), True,
        )
        return carry

    lax.fori_loop(0, kv_heads, own, 0)

    @pl.when(has_last)
    def _():
        copy.wait_recv()

        def body(h, carry):
            attend(
                q_ref, tail[0, h], tail[1, h], acc, lsum, h, group,
                lambda row, col: col > row, False, (0, WINDOW),
            )
            return carry

        lax.fori_loop(0, kv_heads, body, 0)

    write_heads(o_ref, acc, lsum)

    @pl.when(has_next)
    def _():
        copy.wait_send()


def window_attention(q, kv, count, collective_id):
    heads, rows, _ = q.shape
    vmem = pl.BlockSpec(memory_space=VMEM)
    return pl.pallas_call(
        functools.partial(window_kernel, count),
        out_shape=jax.ShapeDtypeStruct((rows, heads * HEAD_DIM), BF16),
        in_specs=[vmem] * 2,
        out_specs=vmem,
        scratch_shapes=[
            VMEM((2, kv.shape[1], WINDOW, HEAD_DIM), BF16),
            VMEM(q.shape, F32),
            VMEM(q.shape, F32),
            pltpu.SemaphoreType.DMA((1,)),
            pltpu.SemaphoreType.DMA((1,)),
        ],
        compiler_params=pltpu.CompilerParams(
            collective_id=collective_id, has_side_effects=True, vmem_limit_bytes=24 * 2**20
        ),
        name="window_attention",
    )(q, kv)


def fused_kernel(
    levels, heads, kv_heads, keep,
    x_hbm, gain1_hbm, gain2_hbm, gain3_hbm, fine_hbm, coarse_hbm,
    wq_hbm, wk_hbm, wv_hbm, wo_hbm, lwq_hbm, lwk_hbm, lwv_hbm,
    hidden_ref, lq_ref, kv2,
    buf, w, wo, gains, xg, acc, ss, ss_first, q_all, kv_buf, out, lsum, att,
    terms, own, landed, passed, proj, mine, stats, cos_ref, sin_ref, fine, coarse,
    e_buf, e_att, e_terms, e_own, e_landed, e_passed, e_proj, e_xg, e_acc, e_ss, e_cos, e_sin,
    e_hid, e_q, e_kv, r_hid, r_q, r_kv, q_up, out_up, lsum_up, up_num, up_sum, got_num, got_sum,
    x_sem, gain_sem, w_sem, wo_sem, ag_send, ag_recv, up_sem, side_sem, kv_sem,
    st_send, st_recv, tail_sem, down_send, down_recv, back_send, back_recv,
    hand_send, hand_recv,
):
    me = lax.axis_index("tp")
    s = lax.axis_index("seq")
    z, c = s // 2, s % 2
    mate = s + 1 - 2 * c
    has_up, has_down = z < levels - 1, z > 0
    top, helper = z == levels - 1, z == levels - 2
    giver, taker = z >= levels // 2, z < levels // 2
    partner = {"seq": 2 * (levels - 1 - z) + c}
    next_row, prev_row = s < 2 * levels - 1, s > 0
    rows, cols = hidden_ref.shape
    chunk_rows, half_rows = rows // PARTS, rows // PARTS // 2
    block, half = rows // 2, rows // 4
    chunks = cols // HEAD_DIM
    ones = jnp.ones((8, HEAD_DIM), F32)
    highest = lax.Precision.HIGHEST
    owners = [xor(me, bits) for bits in range(4)]
    peers = [{"tp": owner} for owner in owners]
    along_x, along_y = peers[1], peers[2]
    qc, kc = heads * HEAD_DIM, kv_heads * HEAD_DIM
    kvc = 2 * kc
    group = heads // kv_heads

    x_loads = []
    for part in range(PARTS):
        span = pl.ds(part * chunk_rows, chunk_rows)
        copy = pltpu.make_async_copy(x_hbm.at[span], buf.at[0, span], x_sem.at[part])
        copy.start()
        x_loads.append(copy)
    gain_loads = []
    pairs = (
        (gain1_hbm, gains.at[0]), (gain2_hbm, gains.at[1]), (gain3_hbm, gains.at[2]),
        (fine_hbm, fine), (coarse_hbm, coarse),
    )
    for i, (ref, target) in enumerate(pairs):
        copy = pltpu.make_async_copy(ref, target, gain_sem.at[i])
        copy.start()
        gain_loads.append(copy)

    def weight_loads(key, value, query):
        loads = []
        for slot in range(4):
            span = pl.ds(pl.multiple_of(owners[slot] * cols, cols), cols)
            spec = ((key, 0, kc), (value, kc, kc), (query, kvc, qc))
            loads.append(
                [
                    pltpu.make_async_copy(
                        ref.at[span, :], w.at[slot, :, pl.ds(begin, width)], w_sem.at[slot, i]
                    )
                    for i, (ref, begin, width) in enumerate(spec)
                ]
            )
        return loads

    first_loads = weight_loads(wk_hbm, wv_hbm, wq_hbm)
    wo_loads = []
    for bits in (3, 1, 2, 0):
        span = pl.ds(pl.multiple_of(owners[bits] * cols, cols), cols)
        wo_loads.append(pltpu.make_async_copy(wo_hbm.at[:, span], wo.at[bits], wo_sem.at[bits]))

    barrier = pltpu.get_barrier_semaphore()
    for peer in (*peers[1:], {"seq": mate}):
        pl.semaphore_signal(barrier, inc=1, device_id=peer, device_id_type=MESH)

    @pl.when(has_up)
    def _():
        pl.semaphore_signal(barrier, inc=1, device_id={"seq": s + 2}, device_id_type=MESH)

    @pl.when(has_down)
    def _():
        pl.semaphore_signal(barrier, inc=1, device_id={"seq": s - 2}, device_id_type=MESH)

    @pl.when(has_up & (c == 1))
    def _():
        pl.semaphore_signal(barrier, inc=1, device_id={"seq": s + 1}, device_id_type=MESH)

    @pl.when(has_down & (c == 0))
    def _():
        pl.semaphore_signal(barrier, inc=1, device_id={"seq": s - 1}, device_id_type=MESH)

    far = (has_up & (c == 1)) | (has_down & (c == 0))
    pl.semaphore_wait(
        barrier,
        4 + has_up.astype(jnp.int32) + has_down.astype(jnp.int32) + far.astype(jnp.int32),
    )

    def gather_moves(store, first, count, part, base):
        begin = pl.multiple_of(part * count, count)
        top, bottom = pl.ds(begin, count // 2), pl.ds(begin + count // 2, count // 2)
        spec = (
            (store.at[0, top], store.at[1, top], along_x),
            (store.at[0, bottom], store.at[2, bottom], along_y),
            (store.at[0, bottom], store.at[1, bottom], along_x),
            (store.at[0, top], store.at[2, top], along_y),
            (store.at[1, top], store.at[3, top], along_y),
            (store.at[2, bottom], store.at[3, bottom], along_x),
        )
        at = first + part * 6 + base
        return [
            remote(source, target, ag_send.at[at + i], ag_recv.at[at + i], device)
            for i, (source, target, device) in enumerate(spec)
        ]

    def moves(part):
        return gather_moves(buf, 0, chunk_rows, part, 0)

    def kv_part(owner, part, count):
        here = pl.ds(pl.multiple_of(part * chunk_rows, chunk_rows), chunk_rows)
        return kv_buf.at[owner, :, pl.ds(0, count), here]

    def up(owner, part, count):
        at, ref = owner * PARTS + part, kv_part(owner, part, count)
        held = owner // 2 * PARTS + part
        return remote(ref, ref, up_sem.at[held], kv_sem.at[at], {"seq": s + 2})

    def side(owner, part, count):
        at, ref = owner * PARTS + part, kv_part(owner, part, count)
        held = owner // 2 * PARTS + part
        return remote(ref, ref, side_sem.at[held], kv_sem.at[at], {"seq": mate})

    def lift(owner, part, act):
        @pl.when(z < levels - 2)
        def _():
            act(up(owner, part, kv_heads))

        @pl.when(helper)
        def _():
            act(up(owner, part, keep))

    def launch(copy):
        copy.start()

    def sent(copy):
        copy.wait_send()

    def arrive(owner, part):
        with jax.named_scope("arrive"):
            up(owner, part, kv_heads).wait_recv()
            side(owner, part, kv_heads).start()
            lift(owner, part, launch)

    def arrive_top(owner, part):
        with jax.named_scope("arrive_top"):
            up(owner, part, keep).wait_recv()
            side(owner, part, keep).start()

    down_heads = pl.ds(keep * group, group)

    def query_down(part):
        span = pl.ds(pl.multiple_of(part * block, block), block)
        return remote(
            q_all.at[down_heads, span], q_up.at[:, span], down_send.at[part], down_recv.at[part],
            {"seq": s - 2},
        )

    backs = [
        remote(source, target, back_send.at[i], back_recv.at[i], {"seq": s + 2})
        for i, (source, target) in enumerate(
            (
                (up_sum, got_sum),
                (up_num.at[:, pl.ds(block, block)], got_num.at[:, pl.ds(block, block)]),
                (up_num.at[:, pl.ds(0, block)], got_num.at[:, pl.ds(0, block)]),
            )
        )
    ]

    def multiply(slot, count, begin, width, fresh):
        product = jnp.dot(
            xg[0:count, :], w[slot, :, begin : begin + width], preferred_element_type=F32
        )
        if fresh:
            acc[0:count, begin : begin + width] = product
        else:
            acc[0:count, begin : begin + width] += product

    def gain_row(which, slot, j):
        return gains[which, pl.ds(owners[slot] * chunks + j, 1), :]

    def prepare(slot, part):
        here = pl.ds(pl.multiple_of(part * chunk_rows, chunk_rows), chunk_rows)
        squares = None
        for j in range(chunks):
            lanes = slice(j * HEAD_DIM, (j + 1) * HEAD_DIM)
            wide = buf[slot, here, lanes].astype(F32)
            squares = wide * wide if squares is None else squares + wide * wide
            proj[slot, here, lanes] = (wide * gain_row(0, slot, j)).astype(BF16)
        if slot == 0:
            ss_first[here, :] = squares
        else:
            ss_first[here, :] += squares

    def row_factor(squares):
        total = jnp.sum(squares, axis=-1, keepdims=True)
        return lax.rsqrt(jnp.broadcast_to(total, squares.shape) * (1.0 / D) + NORM_EPS)

    def rotated(begin, count, factor, span):
        u = acc[0:count, begin : begin + HEAD_DIM] * factor
        turned = pltpu.roll(u, HEAD_DIM // 2, 1)
        return (u * cos_ref[span, :] + turned * sin_ref[span, :]).astype(BF16)

    for copy in x_loads[:1]:
        copy.wait()
    def launch_group(part, some):
        copies = moves(part)
        for i in some:
            copies[i].start()

    launch_group(0, range(4))
    for copy in x_loads[1:]:
        copy.wait()
    launch_group(1, range(2))
    for copy in gain_loads:
        copy.wait()
    for bundle in first_loads:
        for copy in bundle[:2]:
            copy.start()
    for begin in range(0, rows, 64):
        span = slice(begin, begin + 64)
        cosine, sine = coarse[0, pl.ds(s, 1), :], coarse[1, pl.ds(s, 1), :]
        cos_ref[span, :] = fine[0, span] * cosine - fine[1, span] * sine
        sin_ref[span, :] = fine[1, span] * cosine + fine[0, span] * sine
    for i in range(2):
        span = slice(i * HANDED, (i + 1) * HANDED)
        here = slice(i * half, i * half + HANDED)
        cosine, sine = coarse[0, pl.ds(partner["seq"], 1), :], coarse[1, pl.ds(partner["seq"], 1), :]
        e_cos[span, :] = fine[0, here] * cosine - fine[1, here] * sine
        e_sin[span, :] = fine[1, here] * cosine + fine[0, here] * sine

    def first_part(part, carry):
        with jax.named_scope("first_part"):
            return one_part(part, carry)

    def relay(part):
        copies = moves(part)
        copies[0].wait_recv()
        copies[4].start()
        copies[1].wait_recv()
        copies[5].start()

        @pl.when(part < PARTS - 1)
        def _():
            launch_group(part + 1, (2, 3))

        @pl.when(part < PARTS - 2)
        def _():
            launch_group(part + 2, (0, 1))

    def one_part(part, carry):
        span = pl.ds(pl.multiple_of(part * chunk_rows, chunk_rows), chunk_rows)

        def take(slot):
            prepare(slot, part)

            @pl.when(part == 0)
            def _():
                for copy in first_loads[slot][:2]:
                    copy.wait()

            product = jnp.dot(proj[slot, span, :], w[slot, :, 0:kvc], preferred_element_type=F32)
            if slot == 0:
                acc[0:chunk_rows, 0:kvc] = product
            else:
                acc[0:chunk_rows, 0:kvc] += product

        copies = moves(part)
        take(0)

        @pl.when(part == 0)
        def _():
            relay(0)

        @pl.when(part == PARTS // 4)
        def _():
            for bundle in first_loads:
                bundle[2].start()

        @pl.when(part == PARTS // 2)
        def _():
            for copy in wo_loads:
                copy.start()

        copies[2].wait_recv()
        take(1)
        copies[3].wait_recv()
        take(2)

        @pl.when(part < PARTS - 1)
        def _():
            relay(part + 1)

        @pl.when(part == PARTS // 2)
        def _():
            queries(0)

        copies[4].wait_recv()
        copies[5].wait_recv()
        take(3)
        factor = row_factor(ss_first[span, :])
        for h in range(kv_heads):
            kv_buf[s, 0, h, span, :] = rotated(h * HEAD_DIM, chunk_rows, factor, span)
            place = kc + h * HEAD_DIM
            kv_buf[s, 1, h, span, :] = (
                acc[0:chunk_rows, place : place + HEAD_DIM] * factor
            ).astype(BF16)

        @pl.when((c == 0) | helper)
        def _():
            side(s, part, kv_heads).start()

        lift(s, part, launch)

        def forward(k, carry):
            @pl.when(part >= 2 * k - 1)
            def _():
                arrive(s - 2 * k, part - 2 * k + 1)

            return carry

        @pl.when(has_up)
        def _():
            lax.fori_loop(1, z + 1, forward, 0)

        return carry

    def queries(which):
        span = pl.ds(pl.multiple_of(which * block, block), block)

        if which == 0:
            for bundle in first_loads:
                bundle[2].wait()

        acc[:, kvc : kvc + qc] = sum(
            jnp.dot(proj[slot, span, :], w[slot, :, kvc : kvc + qc], preferred_element_type=F32)
            for slot in range(4)
        )
        factor = row_factor(ss_first[span, :])
        for h in reversed(range(heads)):
            q_all[h, span, :] = rotated(kvc + h * HEAD_DIM, block, factor, span)

        @pl.when(top)
        def _():
            query_down(which).start()

    lax.fori_loop(0, PARTS, first_part, 0)
    queries(1)

    def hand(source, target, i):
        return remote(source, target, hand_send.at[i], hand_recv.at[i], partner)

    rows_given = [pl.ds(i * half, HANDED) for i in range(2)]
    rows_taken = [pl.ds(i * HANDED, HANDED) for i in range(2)]
    token_hands = [
        hand(buf.at[:, rows_given[i]], e_buf.at[:, rows_taken[i]], i) for i in range(2)
    ]
    att_hands = [hand(att.at[rows_given[i]], e_att.at[rows_taken[i]], 2 + i) for i in range(2)]
    returns = [
        hand(source, target, 4 + i)
        for i, (source, target) in enumerate(((e_hid, r_hid), (e_q, r_q), (e_kv, r_kv)))
    ]

    second_loads = weight_loads(lwk_hbm, lwv_hbm, lwq_hbm)

    def fetch(slot):
        for copy in second_loads[slot]:
            copy.start()

    with jax.named_scope("own"):
        for h in range(kv_heads):
            attend(
                q_all, kv_buf[s, 0, h], kv_buf[s, 1, h], out, lsum, h, group,
                lambda row, col: col <= row, True,
            )

    def visit_heads(owner, begin, end, span):
        for h in range(begin, end):
            attend(
                q_all, kv_buf[owner, 0, h, span], kv_buf[owner, 1, h, span], out, lsum, h, group,
                None, False,
            )

    def visit(owner, span):
        with jax.named_scope("visit"):
            @pl.when(top)
            def _():
                visit_heads(owner, 0, keep, span)

            @pl.when(has_up)
            def _():
                visit_heads(owner, 0, kv_heads, span)

    def visit_up(owner, first, span):
        with jax.named_scope("visit_up"):
            attend(
                q_up, kv_buf[owner, 0, keep, span], kv_buf[owner, 1, keep, span], out_up, lsum_up,
                0, group, None, first,
            )

    def send_back():
        for g in range(group):
            up_sum[g] = lax.dot_general(
                ones, lsum_up[g], (((1,), (1,)), ((), ())), precision=highest,
                preferred_element_type=F32,
            )
        for part, copy in ((1, backs[1]), (0, backs[2])):
            span = slice(part * block, (part + 1) * block)
            for g in range(group):
                up_num[g, span] = out_up[g, span].astype(BF16)
            copy.start()
            if part == 1:
                backs[0].start()

    @pl.when(helper | (c == 1))
    def _():
        for part in range(PARTS):
            side(mate, part, kv_heads).wait_recv()

    @pl.when(c == 1)
    def _():
        with jax.named_scope("mate"):
            visit_heads(s - 1, 0, kv_heads, pl.ds(0, rows))

    @pl.when(helper)
    def _():
        for part in range(2):
            query_down(part).wait_recv()
        visit_up(s, True, pl.ds(0, rows))
        visit_up(mate, False, pl.ds(0, rows))

    def turn(r, carry):
        def take_in(k, carry):
            owner, part = s - 2 * k, r - 2 * k + 1

            @pl.when((part >= 0) & (part < PARTS))
            def _():
                @pl.when(top)
                def _():
                    arrive_top(owner, part)

                @pl.when((r >= PARTS) & has_up)
                def _():
                    arrive(owner, part)

            return carry

        def level(k, carry):
            owner, other = s - 2 * k, mate - 2 * k
            whole = pl.ds(0, rows)

            @pl.when(r - 2 * k + 1 == PARTS - 1)
            def _():
                @pl.when(helper)
                def _():
                    visit_up(owner, False, whole)
                    for p in range(PARTS):
                        side(other, p, kv_heads).wait_recv()
                    visit_up(other, False, whole)

                    @pl.when(k == z)
                    def _():
                        send_back()

                def both(j, carry):
                    @pl.when((j == 1) & top)
                    def _():
                        for p in range(PARTS):
                            side(other, p, keep).wait_recv()

                    @pl.when((j == 1) & (z < levels - 2))
                    def _():
                        for p in range(PARTS):
                            side(other, p, kv_heads).wait_recv()

                    visit(owner + j * (other - owner), whole)
                    return carry

                lax.fori_loop(0, 2, both, 0)

            return carry

        lax.fori_loop(1, z + 1, take_in, 0)
        lax.fori_loop(1, z + 1, level, 0)
        return carry

    lax.fori_loop(1, PARTS + 2 * z - 1, turn, 0)

    def write_part(part):
        span = slice(part * block, (part + 1) * block)

        @pl.when(top)
        def _():
            if part == 1:
                backs[0].wait_recv()
            backs[2 - part].wait_recv()
            for g in range(group):
                column = lax.dot_general(
                    got_sum[g, :, span], ones * (0.125 / HEAD_DIM), (((0,), (0,)), ((), ())),
                    precision=highest, preferred_element_type=F32,
                )
                lsum[keep * group + g, span] += column
                out[keep * group + g, span] += got_num[g, span].astype(F32)

        for h in range(heads):
            denominator = jnp.sum(lsum[h, span], axis=-1, keepdims=True)
            att[span, h * HEAD_DIM : (h + 1) * HEAD_DIM] = (out[h, span] / denominator).astype(BF16)

    def own_piece(part):
        return types.SimpleNamespace(
            base=part * block, count=block, shared=part == 0, att=att, terms=terms, own=own,
            landed=landed.at[part], passed=passed.at[part], proj=proj, tok=buf,
            mine=mine.at[part], stats=stats.at[part], rs=part * 6, ag=18 + part * 6,
            st=part * 3, xg=xg, acc=acc, ss=ss, cos=cos_ref, sin=sin_ref, hid=hidden_ref,
            q=lq_ref, kv=kv2, kv_base=WINDOW + part * block,
        )

    soon, late = own_piece(1), own_piece(0)
    extra = types.SimpleNamespace(
        base=0, count=2 * HANDED, shared=False, att=e_att, terms=e_terms, own=e_own,
        landed=e_landed, passed=e_passed, proj=e_proj, tok=e_buf, mine=mine.at[2],
        stats=stats.at[2], rs=12, ag=30, st=6, xg=e_xg, acc=e_acc, ss=e_ss,
        cos=e_cos, sin=e_sin, hid=e_hid, q=e_q, kv=e_kv, kv_base=0,
    )

    def reduce_moves(p, trim):
        mid = p.count // 2
        top_rows = pl.ds(p.base + trim, mid - trim)
        low_rows = pl.ds(p.base + mid + trim, mid - trim)
        cut = pl.ds(trim, mid - trim)
        spec = (
            (p.terms.at[2, top_rows], along_x),
            (p.terms.at[2, low_rows], along_y),
            (p.terms.at[0, top_rows], along_x),
            (p.terms.at[1, low_rows], along_y),
            (p.passed.at[1, cut], along_x),
            (p.passed.at[0, cut], along_y),
        )
        return [
            remote(
                source, p.landed.at[i, cut], ag_send.at[p.rs + i], ag_recv.at[p.rs + i], device
            )
            for i, (source, device) in enumerate(spec)
        ]

    def gather2(p, trim):
        mid = p.count // 2
        top_rows = pl.ds(p.base + trim, mid - trim)
        low_rows = pl.ds(p.base + mid + trim, mid - trim)
        spec = (
            (0, 1, top_rows, along_x),
            (0, 2, low_rows, along_y),
            (0, 1, low_rows, along_x),
            (0, 2, top_rows, along_y),
            (1, 3, top_rows, along_y),
            (2, 3, low_rows, along_x),
        )
        return [
            remote(
                p.proj.at[source, span], p.proj.at[target, span],
                ag_send.at[p.ag + i], ag_recv.at[p.ag + i], device,
            )
            for i, (source, target, span, device) in enumerate(spec)
        ]

    def received(copy):
        copy.wait_recv()

    def each(make, p, picks, act):
        def run(trim):
            copies = make(p, trim)
            for i in picks:
                act(copies[i])

        if p.shared:
            pl.when(giver)(lambda: run(HANDED))
            pl.when(taker)(lambda: run(0))
        else:
            run(0)

    def product(bits, p):
        span = slice(p.base, p.base + p.count)
        value = jnp.dot(p.att[span, :], wo[bits], preferred_element_type=F32)
        if bits == 0:
            p.own[span, :] = value
        else:
            p.terms[bits - 1, span, :] = value.astype(BF16)

    def send_products(p):
        product(3, p)
        each(reduce_moves, p, (0, 1), launch)
        product(1, p)
        each(reduce_moves, p, (2,), launch)
        product(2, p)
        each(reduce_moves, p, (3,), launch)
        product(0, p)

    def pass_on(p):
        mid = p.count // 2
        each(reduce_moves, p, (0,), received)
        p.passed[0] = (
            p.terms[1, p.base : p.base + mid].astype(F32) + p.landed[0].astype(F32)
        ).astype(BF16)
        each(reduce_moves, p, (5,), launch)
        each(reduce_moves, p, (1,), received)
        p.passed[1] = (
            p.terms[0, p.base + mid : p.base + p.count].astype(F32) + p.landed[1].astype(F32)
        ).astype(BF16)
        each(reduce_moves, p, (4,), launch)

    def swaps(p):
        return [
            remote(
                p.mine, p.stats.at[bits - 1],
                st_send.at[p.st + bits - 1], st_recv.at[p.st + bits - 1], peers[bits],
            )
            for bits in (3, 1, 2)
        ]

    def finalize(p):
        each(reduce_moves, p, (2, 3, 5, 4), received)
        span = slice(p.base, p.base + p.count)
        lanes = None
        for j in range(chunks):
            cut = slice(j * HEAD_DIM, (j + 1) * HEAD_DIM)
            above = p.landed[2, :, cut].astype(F32) + p.landed[5, :, cut].astype(F32)
            below = p.landed[3, :, cut].astype(F32) + p.landed[4, :, cut].astype(F32)
            value = p.own[span, cut] + jnp.concatenate([above, below], axis=0)
            p.own[span, cut] = value
            p.proj[0, span, cut] = value.astype(BF16)
            lanes = value * value if lanes is None else lanes + value * value
        each(gather2, p, (0, 1), launch)
        if p.count < block:
            lanes = jnp.concatenate([lanes, jnp.zeros((block - p.count, HEAD_DIM), F32)], axis=0)
        p.mine[...] = lax.dot_general(
            ones, lanes, (((1,), (1,)), ((), ())), precision=highest, preferred_element_type=F32
        )
        for swap in swaps(p):
            swap.start()

    def forward_rows(p):
        each(gather2, p, (0,), received)
        each(gather2, p, (4,), launch)
        each(gather2, p, (1,), received)
        each(gather2, p, (5,), launch)

    def post_factor(p):
        for swap in swaps(p):
            swap.wait_recv()
        summed = p.mine[...] + p.stats[0] + p.stats[1] + p.stats[2]
        column = lax.dot_general(
            summed, ones * 0.125, (((0,), (0,)), ((), ())), precision=highest,
            preferred_element_type=F32,
        )
        return lax.rsqrt(column[0 : p.count] * (1.0 / D) + NORM_EPS)

    def take2(slot, p, factor):
        arrivals = ((), (2,), (3,), (4, 5))[slot]
        each(gather2, p, arrivals, received)
        span = slice(p.base, p.base + p.count)
        squares = None
        for j in range(chunks):
            cut = slice(j * HEAD_DIM, (j + 1) * HEAD_DIM)
            summed = p.own[span, cut] if slot == 0 else p.proj[slot, span, cut].astype(F32)
            added = p.tok[slot, span, cut].astype(F32) + summed * factor * gain_row(1, slot, j)
            rounded = added.astype(BF16)
            if slot == 0:
                p.hid[span, cut] = rounded
            wide = rounded.astype(F32)
            squares = wide * wide if squares is None else squares + wide * wide
            p.xg[:, cut] = (wide * gain_row(2, slot, j)).astype(BF16)
        if slot == 0:
            p.ss[...] = squares
        else:
            p.ss[...] += squares
        if p is soon:
            for copy in second_loads[slot]:
                copy.wait()
        for begin, width in ((0, kvc), (kvc, qc)):
            value = jnp.dot(
                p.xg[...], w[slot, :, begin : begin + width], preferred_element_type=F32
            )
            if slot == 0:
                p.acc[:, begin : begin + width] = value
            else:
                p.acc[:, begin : begin + width] += value

    def finish2(p):
        span = slice(p.base, p.base + p.count)
        place_rows = slice(p.kv_base, p.kv_base + p.count)
        factor = row_factor(p.ss[...])

        def spun(begin):
            u = p.acc[:, begin : begin + HEAD_DIM] * factor
            turned = pltpu.roll(u, HEAD_DIM // 2, 1)
            return (u * p.cos[span, :] + turned * p.sin[span, :]).astype(BF16)

        for h in range(kv_heads):
            p.kv[0, h, place_rows, :] = spun(h * HEAD_DIM)
            place = kc + h * HEAD_DIM
            p.kv[1, h, place_rows, :] = (p.acc[:, place : place + HEAD_DIM] * factor).astype(BF16)
        for h in range(heads):
            p.q[h, span, :] = spun(kvc + h * HEAD_DIM)

    tail = remote(
        kv2.at[:, :, pl.ds(rows, WINDOW)], kv2.at[:, :, pl.ds(0, WINDOW)],
        tail_sem.at[0], tail_sem.at[1], {"seq": s + 1},
    )

    def scoped(name, run, *given):
        with jax.named_scope(name):
            return run(*given)

    def drain_early():
        def drain_first(part, carry):
            lift(s, part, sent)

            @pl.when((c == 0) | helper)
            def _():
                side(s, part, kv_heads).wait_send()

            def drain_level(k, carry):
                lift(s - 2 * k, part, sent)

                @pl.when(has_up)
                def _():
                    side(s - 2 * k, part, kv_heads).wait_send()

                @pl.when(top)
                def _():
                    side(s - 2 * k, part, keep).wait_send()

                return carry

            lax.fori_loop(1, z + 1, drain_level, 0)
            return carry

        lax.fori_loop(0, PARTS, drain_first, 0)

        @pl.when(helper)
        def _():
            for copy in backs:
                copy.wait_send()

        @pl.when(top)
        def _():
            for part in range(2):
                query_down(part).wait_send()


    def drain_pair(p):
        each(reduce_moves, p, range(6), sent)
        if p is not late:
            each(gather2, p, range(6), sent)
            for swap in swaps(p):
                swap.wait_send()

    for copy in wo_loads:
        copy.wait()

    def drain_moves(part, carry):
        for copy in moves(part):
            copy.wait_send()

        return carry

    lax.fori_loop(0, PARTS, drain_moves, 0)
    scoped("write_part", write_part, 1)
    scoped("send_products", send_products, soon)
    fetch(0)
    scoped("write_part", write_part, 0)

    @pl.when(giver)
    def _():
        for copy in (*att_hands, *token_hands):
            copy.start()

    for bits in (3, 1, 2, 0):
        product(bits, late)
    scoped("pass_on", pass_on, soon)
    each(reduce_moves, late, (0, 1, 2, 3), launch)
    fetch(1)
    fetch(2)
    fetch(3)
    with jax.named_scope("early_drain"):
        drain_early()
    scoped("finalize", finalize, soon)
    each(gather2, soon, (2, 3), launch)
    scoped("pass_on", pass_on, late)
    factor = scoped("post_factor", post_factor, soon)

    @pl.when(taker)
    def _():
        with jax.named_scope("extra_products"):
            for copy in att_hands:
                copy.wait_recv()
            send_products(extra)

    scoped("take2", take2, 0, soon, factor)
    scoped("forward_rows", forward_rows, soon)
    scoped("take2", take2, 1, soon, factor)
    scoped("take2", take2, 2, soon, factor)

    @pl.when(giver)
    def _():
        scoped("finalize", finalize, late)
        each(gather2, late, (2, 3), launch)

    @pl.when(taker)
    def _():
        scoped("extra_pass_on", pass_on, extra)

    scoped("take2", take2, 3, soon, factor)
    scoped("finish2", finish2, soon)

    @pl.when(next_row)
    def _():
        tail.start()

    @pl.when(s == 0)
    def _():
        kv2[:, :, 0:WINDOW, :] = jnp.zeros((2, kv_heads, WINDOW, HEAD_DIM), BF16)

    @pl.when(taker)
    def _():
        scoped("extra_finalize", finalize, extra)
        each(gather2, extra, (2, 3), launch)
        scoped("finalize", finalize, late)

    drain_pair(soon)

    @pl.when(giver)
    def _():
        for copy in (*token_hands, *att_hands):
            copy.wait_send()

    factor = scoped("post_factor", post_factor, late)
    scoped("take2", take2, 0, late, factor)

    @pl.when(taker)
    def _():
        scoped("extra_forward", forward_rows, extra)
        each(gather2, late, (2, 3), launch)

    scoped("forward_rows", forward_rows, late)

    @pl.when(taker)
    def _():
        with jax.named_scope("extra_take"):
            extra_factor = post_factor(extra)
            for copy in token_hands:
                copy.wait_recv()
            for slot in range(4):
                take2(slot, extra, extra_factor)
                if slot == 0:
                    returns[0].start()
            finish2(extra)
            for copy in returns[1:]:
                copy.start()
            drain_pair(extra)

    scoped("take2", take2, 1, late, factor)
    scoped("take2", take2, 2, late, factor)
    drain_pair(late)
    scoped("take2", take2, 3, late, factor)
    scoped("finish2", finish2, late)

    @pl.when(giver)
    def _():
        with jax.named_scope("extra_return"):
            for copy in returns:
                copy.wait_recv()
            for i in range(2):
                here = slice(i * half, i * half + HANDED)
                there = slice(i * HANDED, (i + 1) * HANDED)
                kv_here = slice(WINDOW + i * half, WINDOW + i * half + HANDED)
                hidden_ref[here, :] = r_hid[there, :]
                lq_ref[:, here, :] = r_q[:, there, :]
                kv2[:, :, kv_here, :] = r_kv[:, :, there, :]

    @pl.when(prev_row)
    def _():
        with jax.named_scope("tail_wait"):
            tail.wait_recv()

    with jax.named_scope("drain"):
        each(gather2, late, range(6), sent)
        for swap in swaps(late):
            swap.wait_send()

        @pl.when(taker)
        def _():
            for copy in returns:
                copy.wait_send()

    @pl.when(next_row)
    def _():
        tail.wait_send()


def fused(x, gains, first, wo, second, count, collective_id):
    rows, cols = x.shape
    wq, wk, wv = first
    heads, kv_heads = wq.shape[1] // HEAD_DIM, wk.shape[1] // HEAD_DIM
    total = wq.shape[1] + 2 * wk.shape[1]
    depth = wo.shape[0]
    group, block, extra = heads // kv_heads, rows // 2, 2 * HANDED
    vmem = pl.BlockSpec(memory_space=VMEM)
    hbm = pl.BlockSpec(memory_space=pltpu.HBM)
    dma = pltpu.SemaphoreType.DMA
    folded = [gain.reshape(-1, HEAD_DIM) for gain in gains]
    turns = 10000.0 ** (-2.0 * np.arange(HEAD_DIM // 2) / HEAD_DIM)
    turns = np.concatenate([turns, turns])
    sign = np.where(np.arange(HEAD_DIM) < HEAD_DIM // 2, -1.0, 1.0)

    def table(places):
        angles = places[:, None] * turns
        return jnp.asarray(np.stack([np.cos(angles), sign * np.sin(angles)]), F32)

    tables = (table(np.arange(rows)), table(np.arange(count) * rows))
    far = [x, *folded, *tables, wq, wk, wv, wo, *second]
    far = [pltpu.with_memory_space_constraint(array, pltpu.HBM) for array in far]
    return pl.pallas_call(
        functools.partial(fused_kernel, count // 2, heads, kv_heads, kv_heads - 1),
        out_shape=(
            jax.ShapeDtypeStruct((rows, cols), BF16),
            jax.ShapeDtypeStruct((heads, rows, HEAD_DIM), BF16),
            jax.ShapeDtypeStruct((2, kv_heads, WINDOW + rows, HEAD_DIM), BF16),
        ),
        in_specs=[hbm] * 13,
        out_specs=(vmem, vmem, vmem),
        scratch_shapes=[
            VMEM((4, rows, cols), BF16),
            VMEM((4, cols, total), BF16),
            VMEM((4, depth, cols), BF16),
            VMEM((3,) + folded[0].shape, F32),
            VMEM((block, cols), BF16),
            VMEM((block, total), F32),
            VMEM((block, HEAD_DIM), F32),
            VMEM((rows, HEAD_DIM), F32),
            VMEM((heads, rows, HEAD_DIM), BF16),
            VMEM((count, 2, kv_heads, rows, HEAD_DIM), BF16),
            VMEM((heads, rows, HEAD_DIM), F32),
            VMEM((heads, rows, HEAD_DIM), F32),
            VMEM((rows, depth), BF16),
            VMEM((3, rows, cols), BF16),
            VMEM((rows, cols), F32),
            VMEM((2, 6, block // 2, cols), BF16),
            VMEM((2, 2, block // 2, cols), BF16),
            VMEM((4, rows, cols), BF16),
            VMEM((3, 8, block), F32),
            VMEM((3, 3, 8, block), F32),
            VMEM((rows, HEAD_DIM), F32),
            VMEM((rows, HEAD_DIM), F32),
            VMEM((2, rows, HEAD_DIM), F32),
            VMEM((2, count, HEAD_DIM), F32),
            VMEM((4, extra, cols), BF16),
            VMEM((extra, depth), BF16),
            VMEM((3, extra, cols), BF16),
            VMEM((extra, cols), F32),
            VMEM((6, HANDED, cols), BF16),
            VMEM((2, HANDED, cols), BF16),
            VMEM((4, extra, cols), BF16),
            VMEM((extra, cols), BF16),
            VMEM((extra, total), F32),
            VMEM((extra, HEAD_DIM), F32),
            VMEM((extra, HEAD_DIM), F32),
            VMEM((extra, HEAD_DIM), F32),
            VMEM((extra, cols), BF16),
            VMEM((heads, extra, HEAD_DIM), BF16),
            VMEM((2, kv_heads, extra, HEAD_DIM), BF16),
            VMEM((extra, cols), BF16),
            VMEM((heads, extra, HEAD_DIM), BF16),
            VMEM((2, kv_heads, extra, HEAD_DIM), BF16),
            VMEM((group, rows, HEAD_DIM), BF16),
            VMEM((group, rows, HEAD_DIM), F32),
            VMEM((group, rows, HEAD_DIM), F32),
            VMEM((group, rows, HEAD_DIM), BF16),
            VMEM((group, 8, rows), F32),
            VMEM((group, rows, HEAD_DIM), BF16),
            VMEM((group, 8, rows), F32),
            dma((PARTS,)),
            dma((5,)),
            dma((4, 3)),
            dma((4,)),
            dma((max(6 * PARTS, 36),)),
            dma((max(6 * PARTS, 36),)),
            dma((count // 2 * PARTS,)),
            dma((count // 2 * PARTS,)),
            dma((count * PARTS,)),
            dma((9,)),
            dma((9,)),
            dma((2,)),
            dma((2,)),
            dma((2,)),
            dma((3,)),
            dma((3,)),
            dma((7,)),
            dma((7,)),
        ],
        compiler_params=pltpu.CompilerParams(
            collective_id=collective_id, has_side_effects=True, vmem_limit_bytes=50 * 2**20
        ),
        name="fused",
    )(*far)


def finish_kernel(hid_ref, q_ref, kv_ref, hid_hbm, o_hbm, o_ref, sems):
    rows = hid_ref.shape[0]
    heads, kv_heads = q_ref.shape[0], kv_ref.shape[1]
    group, block = heads // kv_heads, rows // 2
    begins = jnp.where(lax.axis_index("seq") > 0, 0, WINDOW - 1)
    copies = [pltpu.make_async_copy(hid_ref, hid_hbm, sems.at[kv_heads])]
    copies[0].start()
    for h in range(kv_heads):
        for part in range(2):
            q = q_ref[h * group : (h + 1) * group, part * block : (part + 1) * block]
            q = q.reshape(group * block, HEAD_DIM)
            keys = kv_ref[0, h, part * block : part * block + WINDOW + block]
            values = kv_ref[1, h, part * block : part * block + WINDOW + block]
            scores = lax.dot_general(
                q, keys, (((1,), (1,)), ((), ())), preferred_element_type=F32
            )
            weights = jnp.exp2(jnp.tanh(scores * INNER) * OUTER)
            row = lax.broadcasted_iota(jnp.int32, (block, WINDOW + block), 0)
            col = lax.broadcasted_iota(jnp.int32, (block, WINDOW + block), 1)
            least = jnp.maximum(row, begins) if part == 0 else row
            mask = (col > least) & (col <= row + WINDOW)
            weights = jnp.concatenate(
                [jnp.where(mask, weights[g * block : (g + 1) * block], 0.0) for g in range(group)],
                axis=0,
            )
            denominator = jnp.sum(weights, axis=-1, keepdims=True)
            numerator = jnp.dot(weights.astype(BF16), values, preferred_element_type=F32)
            result = (numerator / denominator).astype(BF16)
            for g in range(group):
                head = h * group + g
                o_ref[part * block : (part + 1) * block, head * HEAD_DIM : (head + 1) * HEAD_DIM] = (
                    result[g * block : (g + 1) * block]
                )
        lanes = pl.ds(h * group * HEAD_DIM, group * HEAD_DIM)
        copy = pltpu.make_async_copy(o_ref.at[:, lanes], o_hbm.at[:, lanes], sems.at[h])
        copy.start()
        copies.append(copy)
    for copy in copies:
        copy.wait()


def finish(hidden, q, kv):
    heads, rows, _ = q.shape
    vmem = pl.BlockSpec(memory_space=VMEM)
    hbm = pl.BlockSpec(memory_space=pltpu.HBM)
    shape = jax.ShapeDtypeStruct((rows, heads * HEAD_DIM), BF16)
    return pl.pallas_call(
        finish_kernel,
        out_shape=(jax.ShapeDtypeStruct(hidden.shape, BF16), shape),
        in_specs=[vmem] * 3,
        out_specs=(hbm, hbm),
        scratch_shapes=[
            VMEM(shape.shape, BF16),
            pltpu.SemaphoreType.DMA((kv.shape[1] + 1,)),
        ],
        compiler_params=pltpu.CompilerParams(vmem_limit_bytes=8 * 2**20),
        name="finish",
    )(hidden, q, kv)


def rms_scaled(values, weights):
    widened = values.astype(F32)
    factor = lax.rsqrt(jnp.mean(widened * widened, axis=-1, keepdims=True) + NORM_EPS)
    return widened * factor * weights


def plain_gather_project(x, gain, cos, sin, wq, wk, wv):
    full = lax.all_gather(x, "tp", axis=1, tiled=True)
    normed = rms_scaled(full, gain).astype(BF16)

    def heads_of(weight):
        product = jnp.dot(normed, weight, preferred_element_type=F32)
        return jnp.swapaxes(product.reshape(x.shape[0], -1, HEAD_DIM), 0, 1)

    def rotated(u):
        return (u * cos + jnp.roll(u, HEAD_DIM // 2, axis=-1) * sin).astype(BF16)

    keys, values = rotated(heads_of(wk)), heads_of(wv).astype(BF16)
    return rotated(heads_of(wq)), jnp.stack([keys, values])


def plain_output_project(attended, tokens, gain, wo):
    cols = tokens.shape[1]
    partial_sum = jnp.dot(attended, wo, preferred_element_type=F32).astype(BF16)
    summed = lax.psum(partial_sum, "tp").astype(F32)
    added = rms_scaled(summed, gain)
    mine = lax.dynamic_slice_in_dim(added, lax.axis_index("tp") * cols, cols, 1)
    return (tokens.astype(F32) + mine).astype(BF16)


def local(
    sizes,
    tokens,
    attention_gain,
    query_weight,
    key_weight,
    value_weight,
    output_weight,
    post_gain,
    local_gain,
    local_query_weight,
    local_key_weight,
    local_value_weight,
):
    seq, tp = sizes
    rows, cols = tokens.shape
    first = (query_weight, key_weight, value_weight)
    second = (local_query_weight, local_key_weight, local_value_weight)
    if tp == 4 and cols % HEAD_DIM == 0 and rows == 2 * WINDOW and seq % 4 == 0 and seq > 4:
        gains = (attention_gain, post_gain, local_gain)
        return finish(*fused(tokens, gains, first, output_weight, second, seq, 0))
    places = lax.axis_index("seq") * rows + lax.iota(jnp.int32, rows)
    halfway = HEAD_DIM // 2
    exponents = jnp.arange(halfway, dtype=F32) * (2.0 / HEAD_DIM)
    frequency = jnp.power(F32(10000.0), -exponents)
    angles = places.astype(F32)[:, None] * frequency[None, :]
    cosine, sine = jnp.cos(angles), jnp.sin(angles)
    cos = jnp.concatenate([cosine, cosine], axis=-1)
    sin = jnp.concatenate([-sine, sine], axis=-1)
    lead = plain_gather_project(tokens, attention_gain, cos, sin, *first)
    attended = causal_attention(*lead, seq, 1)
    hidden = plain_output_project(attended, tokens, post_gain, output_weight)
    lq, lkv = plain_gather_project(hidden, local_gain, cos, sin, *second)
    return hidden, window_attention(lq, lkv, seq, 4)


def solution(mesh):
    in_specs = (
        P("seq", "tp"),
        P(),
        P(None, "tp"),
        P(None, "tp"),
        P(None, "tp"),
        P("tp", None),
        P(),
        P(),
        P(None, "tp"),
        P(None, "tp"),
        P(None, "tp"),
    )
    out_specs = (P("seq", "tp"), P("seq", "tp"))
    sizes = (mesh.shape["seq"], mesh.shape["tp"])
    body = functools.partial(local, sizes)
    return jax.shard_map(body, mesh=mesh, in_specs=in_specs, out_specs=out_specs, check_vma=False)
```

```python
import functools
import math
import types

import jax
import jax.numpy as jnp
import numpy as np
from jax import lax
from jax.experimental import pallas as pl
from jax.experimental.pallas import tpu as pltpu
from jax.sharding import PartitionSpec as P

D = 4608
HEADS = 32
HEAD_DIM = 128
WINDOW = 128

SOFT_CAP = 50.0
NORM_EPS = 1e-06
MESH = pl.DeviceIdType.MESH
VMEM = pltpu.VMEM
F32 = jnp.float32
BF16 = jnp.bfloat16
PARTS = 4
HANDED = 16
INNER = float(D // HEADS) ** (-0.5) / SOFT_CAP
OUTER = SOFT_CAP * math.log2(math.e)


def greet(peers):
    barrier = pltpu.get_barrier_semaphore()
    for peer in peers:
        pl.semaphore_signal(barrier, inc=1, device_id=peer, device_id_type=MESH)
    pl.semaphore_wait(barrier, len(peers))


def remote(source, target, send_sem, recv_sem, device):
    return pltpu.make_async_remote_copy(
        src_ref=source,
        dst_ref=target,
        send_sem=send_sem,
        recv_sem=recv_sem,
        device_id=device,
        device_id_type=MESH,
    )


def xor(index, bits):
    low, high = index % 2, index // 2
    if bits & 1:
        low = 1 - low
    if bits & 2:
        high = 1 - high
    return high * 2 + low


def attend(q_ref, keys, values, acc, lsum, h, group, allowed, first, row_span=None):
    q = q_ref[pl.ds(h * group, group)]
    if row_span is not None:
        q = q[:, row_span[0] : row_span[1]]
    rows = q.shape[1]
    q = q.reshape(group * rows, HEAD_DIM)
    scores = lax.dot_general(q, keys, (((1,), (1,)), ((), ())), preferred_element_type=F32)
    weights = jnp.exp2(jnp.tanh(scores * INNER) * OUTER)
    if allowed is not None:
        count = keys.shape[0]
        row = lax.broadcasted_iota(jnp.int32, (rows, count), 0)
        col = lax.broadcasted_iota(jnp.int32, (rows, count), 1)
        mask = allowed(row, col)
        weights = jnp.concatenate(
            [jnp.where(mask, weights[g * rows : (g + 1) * rows], 0.0) for g in range(group)], axis=0
        )
    lanes = weights[:, :HEAD_DIM]
    for begin in range(HEAD_DIM, keys.shape[0], HEAD_DIM):
        lanes = lanes + weights[:, begin : begin + HEAD_DIM]
    product = jnp.dot(weights.astype(BF16), values, preferred_element_type=F32)
    lanes = lanes.reshape(group, rows, HEAD_DIM)
    product = product.reshape(group, rows, HEAD_DIM)
    heads = pl.ds(h * group, group)
    span = pl.ds(0, rows)
    if first:
        lsum[heads, span] = lanes
        acc[heads, span] = product
    else:
        lsum[heads, span] += lanes
        acc[heads, span] += product


def write_heads(o_ref, acc, lsum):
    for h in range(acc.shape[0]):
        denominator = jnp.sum(lsum[h], axis=-1, keepdims=True)
        o_ref[:, h * HEAD_DIM : (h + 1) * HEAD_DIM] = (acc[h] / denominator).astype(BF16)


def causal_kernel(levels, q_ref, kv_ref, o_ref, buf, acc, lsum, up_sem, side_sem, recv):
    s = lax.axis_index("seq")
    z, c = s // 2, s % 2
    mate = s + 1 - 2 * c
    kv_heads = kv_ref.shape[1]
    group = q_ref.shape[0] // kv_heads
    has_up, has_down = z < levels - 1, z > 0

    barrier = pltpu.get_barrier_semaphore()
    pl.semaphore_signal(barrier, inc=1, device_id={"seq": mate}, device_id_type=MESH)

    @pl.when(has_up)
    def _():
        pl.semaphore_signal(barrier, inc=1, device_id={"seq": s + 2}, device_id_type=MESH)

    @pl.when(has_down)
    def _():
        pl.semaphore_signal(barrier, inc=1, device_id={"seq": s - 2}, device_id_type=MESH)

    pl.semaphore_wait(barrier, 1 + has_up.astype(jnp.int32) + has_down.astype(jnp.int32))

    def up(owner, source):
        return remote(source, buf.at[owner], up_sem.at[owner], recv.at[owner], {"seq": s + 2})

    def side(owner, source):
        return remote(source, buf.at[owner], side_sem.at[owner], recv.at[owner], {"seq": mate})

    @pl.when(has_up)
    def _():
        up(s, kv_ref).start()

    @pl.when(c == 0)
    def _():
        side(s, kv_ref).start()

    def own(h, carry):
        attend(
            q_ref, kv_ref[0, h], kv_ref[1, h], acc, lsum, h, group,
            lambda row, col: col <= row, True,
        )
        return carry

    lax.fori_loop(0, kv_heads, own, 0)

    def visit(owner):
        def body(h, carry):
            attend(
                q_ref, buf[owner, 0, h], buf[owner, 1, h], acc, lsum, h, group, None, False
            )
            return carry

        lax.fori_loop(0, kv_heads, body, 0)

    @pl.when(c == 1)
    def _():
        side(s - 1, buf.at[s - 1]).wait_recv()
        visit(s - 1)

    def level(k, carry):
        owner, other = s - 2 * k, mate - 2 * k
        up(owner, buf.at[owner]).wait_recv()

        @pl.when(has_up)
        def _():
            up(owner, buf.at[owner]).start()

        side(owner, buf.at[owner]).start()
        visit(owner)
        side(other, buf.at[other]).wait_recv()
        visit(other)
        return carry

    lax.fori_loop(1, z + 1, level, 0)
    write_heads(o_ref, acc, lsum)

    @pl.when(has_up)
    def _():
        up(s, kv_ref).wait_send()

    @pl.when(c == 0)
    def _():
        side(s, kv_ref).wait_send()

    def drain(k, carry):
        owner = s - 2 * k

        @pl.when(has_up)
        def _():
            up(owner, buf.at[owner]).wait_send()

        side(owner, buf.at[owner]).wait_send()
        return carry

    lax.fori_loop(1, z + 1, drain, 0)


def causal_attention(q, kv, count, collective_id):
    heads, rows, _ = q.shape
    vmem = pl.BlockSpec(memory_space=VMEM)
    return pl.pallas_call(
        functools.partial(causal_kernel, count // 2),
        out_shape=jax.ShapeDtypeStruct((rows, heads * HEAD_DIM), BF16),
        in_specs=[vmem] * 2,
        out_specs=vmem,
        scratch_shapes=[
            VMEM((count,) + kv.shape, BF16),
            VMEM(q.shape, F32),
            VMEM(q.shape, F32),
            pltpu.SemaphoreType.DMA((count,)),
            pltpu.SemaphoreType.DMA((count,)),
            pltpu.SemaphoreType.DMA((count,)),
        ],
        compiler_params=pltpu.CompilerParams(
            collective_id=collective_id, has_side_effects=True, vmem_limit_bytes=32 * 2**20
        ),
        name="causal_attention",
    )(q, kv)


def window_kernel(count, q_ref, kv_ref, o_ref, tail, acc, lsum, send, recv):
    s = lax.axis_index("seq")
    kv_heads, rows = kv_ref.shape[1], kv_ref.shape[2]
    group = q_ref.shape[0] // kv_heads
    has_next, has_last = s < count - 1, s > 0
    barrier = pltpu.get_barrier_semaphore()

    @pl.when(has_next)
    def _():
        pl.semaphore_signal(barrier, inc=1, device_id={"seq": s + 1}, device_id_type=MESH)

    @pl.when(has_last)
    def _():
        pl.semaphore_signal(barrier, inc=1, device_id={"seq": s - 1}, device_id_type=MESH)

    pl.semaphore_wait(barrier, has_next.astype(jnp.int32) + has_last.astype(jnp.int32))
    copy = remote(
        kv_ref.at[:, :, pl.ds(rows - WINDOW, WINDOW), :], tail, send.at[0], recv.at[0],
        {"seq": s + 1},
    )

    @pl.when(has_next)
    def _():
        copy.start()

    def own(h, carry):
        attend(
            q_ref, kv_ref[0, h], kv_ref[1, h], acc, lsum, h, group,
            lambda row, col: (col <= row) & (row - col < WINDOW), True,
        )
        return carry

    lax.fori_loop(0, kv_heads, own, 0)

    @pl.when(has_last)
    def _():
        copy.wait_recv()

        def body(h, carry):
            attend(
                q_ref, tail[0, h], tail[1, h], acc, lsum, h, group,
                lambda row, col: col > row, False, (0, WINDOW),
            )
            return carry

        lax.fori_loop(0, kv_heads, body, 0)

    write_heads(o_ref, acc, lsum)

    @pl.when(has_next)
    def _():
        copy.wait_send()


def window_attention(q, kv, count, collective_id):
    heads, rows, _ = q.shape
    vmem = pl.BlockSpec(memory_space=VMEM)
    return pl.pallas_call(
        functools.partial(window_kernel, count),
        out_shape=jax.ShapeDtypeStruct((rows, heads * HEAD_DIM), BF16),
        in_specs=[vmem] * 2,
        out_specs=vmem,
        scratch_shapes=[
            VMEM((2, kv.shape[1], WINDOW, HEAD_DIM), BF16),
            VMEM(q.shape, F32),
            VMEM(q.shape, F32),
            pltpu.SemaphoreType.DMA((1,)),
            pltpu.SemaphoreType.DMA((1,)),
        ],
        compiler_params=pltpu.CompilerParams(
            collective_id=collective_id, has_side_effects=True, vmem_limit_bytes=24 * 2**20
        ),
        name="window_attention",
    )(q, kv)


def fused_kernel(
    levels, heads, kv_heads, keep,
    x_hbm, gain1_hbm, gain2_hbm, gain3_hbm, fine_hbm, coarse_hbm,
    wq_hbm, wk_hbm, wv_hbm, wo_hbm, lwq_hbm, lwk_hbm, lwv_hbm,
    hidden_ref, lq_ref, kv2,
    buf, w, wo, gains, xg, acc, ss, ss_first, q_all, kv_buf, out, lsum, att,
    terms, own, landed, passed, proj, mine, stats, cos_ref, sin_ref, fine, coarse,
    e_buf, e_att, e_terms, e_own, e_landed, e_passed, e_proj, e_xg, e_acc, e_ss, e_cos, e_sin,
    e_factor, e_hid, e_q, e_kv, r_hid, r_q, r_kv, q_up, out_up, lsum_up, up_num, up_sum, got_num, got_sum,
    x_sem, gain_sem, w_sem, wo_sem, out_sem, ag_recv, up_sem, side_sem, kv_sem,
    st_send, st_recv, tail_sem, down_send, down_recv, back_send, back_recv,
    hand_send, hand_recv,
):
    me = lax.axis_index("tp")
    s = lax.axis_index("seq")
    z, c = s // 2, s % 2
    mate = s + 1 - 2 * c
    has_up, has_down = z < levels - 1, z > 0
    top, helper = z == levels - 1, z == levels - 2
    giver, taker = z >= levels // 2, z < levels // 2
    partner = {"seq": 2 * (levels - 1 - z) + c}
    next_row, prev_row = s < 2 * levels - 1, s > 0
    rows, cols = hidden_ref.shape
    chunk_rows, half_rows = rows // PARTS, rows // PARTS // 2
    block, half = rows // 2, rows // 4
    chunks = cols // HEAD_DIM
    ones = jnp.ones((8, HEAD_DIM), F32)
    highest = lax.Precision.HIGHEST
    owners = [xor(me, bits) for bits in range(4)]
    peers = [{"tp": owner} for owner in owners]
    along_x, along_y = peers[1], peers[2]
    qc, kc = heads * HEAD_DIM, kv_heads * HEAD_DIM
    kvc = 2 * kc
    group = heads // kv_heads

    x_loads = []
    for part in range(PARTS):
        span = pl.ds(part * chunk_rows, chunk_rows)
        copy = pltpu.make_async_copy(x_hbm.at[span], buf.at[0, span], x_sem.at[part])
        copy.start()
        x_loads.append(copy)
    gain_loads = []
    pairs = (
        (gain1_hbm, gains.at[0]), (gain2_hbm, gains.at[1]), (gain3_hbm, gains.at[2]),
        (fine_hbm, fine), (coarse_hbm, coarse),
    )
    for i, (ref, target) in enumerate(pairs):
        copy = pltpu.make_async_copy(ref, target, gain_sem.at[i])
        copy.start()
        gain_loads.append(copy)

    def weight_loads(key, value, query):
        loads = []
        for slot in range(4):
            span = pl.ds(pl.multiple_of(owners[slot] * cols, cols), cols)
            spec = ((key, 0, kc), (value, kc, kc), (query, kvc, qc))
            loads.append(
                [
                    pltpu.make_async_copy(
                        ref.at[span, :], w.at[slot, :, pl.ds(begin, width)], w_sem.at[slot, i]
                    )
                    for i, (ref, begin, width) in enumerate(spec)
                ]
            )
        return loads

    first_loads = weight_loads(wk_hbm, wv_hbm, wq_hbm)
    wo_loads = []
    for bits in (3, 1, 2, 0):
        span = pl.ds(pl.multiple_of(owners[bits] * cols, cols), cols)
        wo_loads.append(pltpu.make_async_copy(wo_hbm.at[:, span], wo.at[bits], wo_sem.at[bits]))

    barrier = pltpu.get_barrier_semaphore()
    for peer in (*peers[1:], {"seq": mate}):
        pl.semaphore_signal(barrier, inc=1, device_id=peer, device_id_type=MESH)

    @pl.when(has_up)
    def _():
        pl.semaphore_signal(barrier, inc=1, device_id={"seq": s + 2}, device_id_type=MESH)

    @pl.when(has_down)
    def _():
        pl.semaphore_signal(barrier, inc=1, device_id={"seq": s - 2}, device_id_type=MESH)

    @pl.when(has_up & (c == 1))
    def _():
        pl.semaphore_signal(barrier, inc=1, device_id={"seq": s + 1}, device_id_type=MESH)

    @pl.when(has_down & (c == 0))
    def _():
        pl.semaphore_signal(barrier, inc=1, device_id={"seq": s - 1}, device_id_type=MESH)

    far = (has_up & (c == 1)) | (has_down & (c == 0))
    pl.semaphore_wait(
        barrier,
        4 + has_up.astype(jnp.int32) + has_down.astype(jnp.int32) + far.astype(jnp.int32),
    )

    def all_sent(ref, sem):
        remote(ref, ref, sem, sem, along_x).wait_send()

    def gather_moves(store, first, count, part, base):
        begin = pl.multiple_of(part * count, count)
        top, bottom = pl.ds(begin, count // 2), pl.ds(begin + count // 2, count // 2)
        spec = (
            (store.at[0, top], store.at[1, top], along_x),
            (store.at[0, bottom], store.at[2, bottom], along_y),
            (store.at[0, bottom], store.at[1, bottom], along_x),
            (store.at[0, top], store.at[2, top], along_y),
            (store.at[1, top], store.at[3, top], along_y),
            (store.at[2, bottom], store.at[3, bottom], along_x),
        )
        at = first + part * 6 + base
        return [
            remote(source, target, out_sem.at[part], ag_recv.at[at + i], device)
            for i, (source, target, device) in enumerate(spec)
        ]

    def moves(part):
        return gather_moves(buf, 0, chunk_rows, part, 0)

    def kv_part(owner, part, count):
        here = pl.ds(pl.multiple_of(part * chunk_rows, chunk_rows), chunk_rows)
        return kv_buf.at[owner, :, pl.ds(0, count), here]

    def up(owner, part, count):
        at, ref = owner // 2 * PARTS + part, kv_part(owner, part, count)
        return remote(ref, ref, up_sem.at[owner // 2], kv_sem.at[at], {"seq": s + 2})

    def side(owner, part, count):
        at, ref = levels * PARTS + owner // 2, kv_part(owner, part, count)
        return remote(ref, ref, side_sem.at[owner // 2], kv_sem.at[at], {"seq": mate})

    def whole_block(owner, count):
        return kv_buf.at[owner, :, pl.ds(0, count)]

    def side_landed(owner, count):
        ref, at = whole_block(owner, count), levels * PARTS + owner // 2
        remote(ref, ref, side_sem.at[owner // 2], kv_sem.at[at], {"seq": mate}).wait_recv()

    def lift(owner, part, act):
        @pl.when(z < levels - 2)
        def _():
            act(up(owner, part, kv_heads))

        @pl.when(helper)
        def _():
            act(up(owner, part, keep))

    def launch(copy):
        copy.start()

    def sent(copy):
        copy.wait_send()

    def arrive(owner, part):
        with jax.named_scope("arrive"):
            up(owner, part, kv_heads).wait_recv()
            side(owner, part, kv_heads).start()
            lift(owner, part, launch)

    def arrive_top(owner, part):
        with jax.named_scope("arrive_top"):
            up(owner, part, keep).wait_recv()
            side(owner, part, keep).start()

    down_heads = pl.ds(keep * group, group)

    def query_down(part):
        span = pl.ds(pl.multiple_of(part * block, block), block)
        return remote(
            q_all.at[down_heads, span], q_up.at[:, span], down_send.at[part], down_recv.at[part],
            {"seq": s - 2},
        )

    backs = [
        remote(source, target, back_send.at[i], back_recv.at[i], {"seq": s + 2})
        for i, (source, target) in enumerate(
            (
                (up_sum, got_sum),
                (up_num.at[:, pl.ds(block, block)], got_num.at[:, pl.ds(block, block)]),
                (up_num.at[:, pl.ds(0, block)], got_num.at[:, pl.ds(0, block)]),
            )
        )
    ]

    def multiply(slot, count, begin, width, fresh):
        product = jnp.dot(
            xg[0:count, :], w[slot, :, begin : begin + width], preferred_element_type=F32
        )
        if fresh:
            acc[0:count, begin : begin + width] = product
        else:
            acc[0:count, begin : begin + width] += product

    def gain_row(which, slot, j):
        return gains[which, pl.ds(owners[slot] * chunks + j, 1), :]

    def prepare(slot, part):
        here = pl.ds(pl.multiple_of(part * chunk_rows, chunk_rows), chunk_rows)
        squares = None
        for j in range(chunks):
            lanes = slice(j * HEAD_DIM, (j + 1) * HEAD_DIM)
            wide = buf[slot, here, lanes].astype(F32)
            squares = wide * wide if squares is None else squares + wide * wide
            proj[slot, here, lanes] = (wide * gain_row(0, slot, j)).astype(BF16)
        if slot == 0:
            ss_first[here, :] = squares
        else:
            ss_first[here, :] += squares

    def row_factor(squares):
        total = jnp.sum(squares, axis=-1, keepdims=True)
        return lax.rsqrt(jnp.broadcast_to(total, squares.shape) * (1.0 / D) + NORM_EPS)

    def rotated(begin, count, factor, span):
        u = acc[0:count, begin : begin + HEAD_DIM] * factor
        turned = pltpu.roll(u, HEAD_DIM // 2, 1)
        return (u * cos_ref[span, :] + turned * sin_ref[span, :]).astype(BF16)

    for copy in x_loads[:1]:
        copy.wait()
    def launch_group(part, some):
        copies = moves(part)
        for i in some:
            copies[i].start()

    launch_group(0, range(4))
    for copy in x_loads[1:]:
        copy.wait()
    launch_group(1, range(2))
    for copy in gain_loads:
        copy.wait()
    for bundle in first_loads:
        for copy in bundle[:2]:
            copy.start()
    for begin in range(0, rows, 64):
        span = slice(begin, begin + 64)
        cosine, sine = coarse[0, pl.ds(s, 1), :], coarse[1, pl.ds(s, 1), :]
        cos_ref[span, :] = fine[0, span] * cosine - fine[1, span] * sine
        sin_ref[span, :] = fine[1, span] * cosine + fine[0, span] * sine
    for i in range(2):
        span = slice(i * HANDED, (i + 1) * HANDED)
        here = slice(i * half, i * half + HANDED)
        cosine, sine = coarse[0, pl.ds(partner["seq"], 1), :], coarse[1, pl.ds(partner["seq"], 1), :]
        e_cos[span, :] = fine[0, here] * cosine - fine[1, here] * sine
        e_sin[span, :] = fine[1, here] * cosine + fine[0, here] * sine

    def first_part(part, carry):
        with jax.named_scope("first_part"):
            return one_part(part, carry)

    def relay(part):
        copies = moves(part)
        copies[0].wait_recv()
        copies[4].start()
        copies[1].wait_recv()
        copies[5].start()

        @pl.when(part < PARTS - 1)
        def _():
            launch_group(part + 1, (2, 3))

        @pl.when(part < PARTS - 2)
        def _():
            launch_group(part + 2, (0, 1))

    def one_part(part, carry):
        span = pl.ds(pl.multiple_of(part * chunk_rows, chunk_rows), chunk_rows)

        def take(slot):
            prepare(slot, part)

            @pl.when(part == 0)
            def _():
                for copy in first_loads[slot][:2]:
                    copy.wait()

            product = jnp.dot(proj[slot, span, :], w[slot, :, 0:kvc], preferred_element_type=F32)
            if slot == 0:
                acc[0:chunk_rows, 0:kvc] = product
            else:
                acc[0:chunk_rows, 0:kvc] += product

        copies = moves(part)
        take(0)

        @pl.when(part == 0)
        def _():
            relay(0)

        @pl.when(part == PARTS // 4)
        def _():
            for bundle in first_loads:
                bundle[2].start()

        @pl.when(part == PARTS // 2)
        def _():
            for copy in wo_loads:
                copy.start()

        copies[2].wait_recv()
        take(1)
        copies[3].wait_recv()
        take(2)

        @pl.when(part < PARTS - 1)
        def _():
            relay(part + 1)

        @pl.when(part == PARTS // 2)
        def _():
            queries(0)

        copies[4].wait_recv()
        copies[5].wait_recv()
        take(3)
        factor = row_factor(ss_first[span, :])
        for h in range(kv_heads):
            kv_buf[s, 0, h, span, :] = rotated(h * HEAD_DIM, chunk_rows, factor, span)
            place = kc + h * HEAD_DIM
            kv_buf[s, 1, h, span, :] = (
                acc[0:chunk_rows, place : place + HEAD_DIM] * factor
            ).astype(BF16)

        @pl.when((c == 0) | helper)
        def _():
            side(s, part, kv_heads).start()

        lift(s, part, launch)

        def forward(k, carry):
            @pl.when(part >= 2 * k - 1)
            def _():
                arrive(s - 2 * k, part - 2 * k + 1)

            return carry

        @pl.when(has_up)
        def _():
            lax.fori_loop(1, z + 1, forward, 0)

        return carry

    def queries(which):
        span = pl.ds(pl.multiple_of(which * block, block), block)

        if which == 0:
            for bundle in first_loads:
                bundle[2].wait()

        acc[:, kvc : kvc + qc] = sum(
            jnp.dot(proj[slot, span, :], w[slot, :, kvc : kvc + qc], preferred_element_type=F32)
            for slot in range(4)
        )
        factor = row_factor(ss_first[span, :])
        for h in reversed(range(heads)):
            q_all[h, span, :] = rotated(kvc + h * HEAD_DIM, block, factor, span)

        @pl.when(top)
        def _():
            query_down(which).start()

    lax.fori_loop(0, PARTS, first_part, 0)
    queries(1)

    def hand(source, target, i):
        return remote(source, target, hand_send.at[i], hand_recv.at[i], partner)

    rows_given = [pl.ds(i * half, HANDED) for i in range(2)]
    rows_taken = [pl.ds(i * HANDED, HANDED) for i in range(2)]
    token_hands = [
        hand(buf.at[:, rows_given[i]], e_buf.at[:, rows_taken[i]], i) for i in range(2)
    ]
    att_hands = [hand(att.at[rows_given[i]], e_att.at[rows_taken[i]], 2 + i) for i in range(2)]
    returns = [
        hand(source, target, 4 + i)
        for i, (source, target) in enumerate(((e_hid, r_hid), (e_q, r_q), (e_kv, r_kv)))
    ]

    second_loads = weight_loads(lwk_hbm, lwv_hbm, lwq_hbm)

    def fetch(slot):
        for copy in second_loads[slot]:
            copy.start()

    with jax.named_scope("own"):
        for h in range(kv_heads):
            attend(
                q_all, kv_buf[s, 0, h], kv_buf[s, 1, h], out, lsum, h, group,
                lambda row, col: col <= row, True,
            )

    def visit_heads(owner, begin, end, span):
        for h in range(begin, end):
            attend(
                q_all, kv_buf[owner, 0, h, span], kv_buf[owner, 1, h, span], out, lsum, h, group,
                None, False,
            )

    def visit(owner, span):
        with jax.named_scope("visit"):
            @pl.when(top)
            def _():
                visit_heads(owner, 0, keep, span)

            @pl.when(has_up)
            def _():
                visit_heads(owner, 0, kv_heads, span)

    def visit_up(owner, first, span):
        with jax.named_scope("visit_up"):
            attend(
                q_up, kv_buf[owner, 0, keep, span], kv_buf[owner, 1, keep, span], out_up, lsum_up,
                0, group, None, first,
            )

    def send_back():
        for g in range(group):
            up_sum[g] = lax.dot_general(
                ones, lsum_up[g], (((1,), (1,)), ((), ())), precision=highest,
                preferred_element_type=F32,
            )
        for part, copy in ((1, backs[1]), (0, backs[2])):
            span = slice(part * block, (part + 1) * block)
            for g in range(group):
                up_num[g, span] = out_up[g, span].astype(BF16)
            copy.start()
            if part == 1:
                backs[0].start()

    @pl.when(helper | (c == 1))
    def _():
        side_landed(mate, kv_heads)

    @pl.when(c == 1)
    def _():
        with jax.named_scope("mate"):
            visit_heads(s - 1, 0, kv_heads, pl.ds(0, rows))

    @pl.when(helper)
    def _():
        for part in range(2):
            query_down(part).wait_recv()
        visit_up(s, True, pl.ds(0, rows))
        visit_up(mate, False, pl.ds(0, rows))

    def turn(r, carry):
        def take_in(k, carry):
            owner, part = s - 2 * k, r - 2 * k + 1

            @pl.when((part >= 0) & (part < PARTS))
            def _():
                @pl.when(top)
                def _():
                    arrive_top(owner, part)

                @pl.when((r >= PARTS) & has_up)
                def _():
                    arrive(owner, part)

            return carry

        def level(k, carry):
            owner, other = s - 2 * k, mate - 2 * k
            whole = pl.ds(0, rows)

            @pl.when(r - 2 * k + 1 == PARTS - 1)
            def _():
                @pl.when(helper)
                def _():
                    visit_up(owner, False, whole)
                    side_landed(other, kv_heads)
                    visit_up(other, False, whole)

                    @pl.when(k == z)
                    def _():
                        send_back()

                def both(j, carry):
                    @pl.when((j == 1) & top)
                    def _():
                        side_landed(other, keep)

                    @pl.when((j == 1) & (z < levels - 2))
                    def _():
                        side_landed(other, kv_heads)

                    visit(owner + j * (other - owner), whole)
                    return carry

                lax.fori_loop(0, 2, both, 0)

            return carry

        lax.fori_loop(1, z + 1, take_in, 0)
        lax.fori_loop(1, z + 1, level, 0)
        return carry

    lax.fori_loop(1, PARTS + 2 * z - 1, turn, 0)

    def write_part(part):
        span = slice(part * block, (part + 1) * block)

        @pl.when(top)
        def _():
            if part == 1:
                backs[0].wait_recv()
            backs[2 - part].wait_recv()
            for g in range(group):
                column = lax.dot_general(
                    got_sum[g, :, span], ones * (0.125 / HEAD_DIM), (((0,), (0,)), ((), ())),
                    precision=highest, preferred_element_type=F32,
                )
                lsum[keep * group + g, span] += column
                out[keep * group + g, span] += got_num[g, span].astype(F32)

        for h in range(heads):
            denominator = jnp.sum(lsum[h, span], axis=-1, keepdims=True)
            att[span, h * HEAD_DIM : (h + 1) * HEAD_DIM] = (out[h, span] / denominator).astype(BF16)

    def own_piece(part):
        return types.SimpleNamespace(
            base=part * block, count=block, shared=part == 0, att=att, terms=terms, own=own,
            landed=landed.at[part], passed=passed.at[part], proj=proj, tok=buf,
            mine=mine.at[part], stats=stats.at[part], rs=part * 6, ag=18 + part * 6,
            st=part * 3, xg=xg, acc=acc, ss=ss, cos=cos_ref, sin=sin_ref, hid=hidden_ref,
            q=lq_ref, kv=kv2, kv_base=WINDOW + part * block,
        )

    soon, late = own_piece(1), own_piece(0)
    extra = types.SimpleNamespace(
        base=0, count=2 * HANDED, shared=False, att=e_att, terms=e_terms, own=e_own,
        landed=e_landed, passed=e_passed, proj=e_proj, tok=e_buf, mine=mine.at[2],
        stats=stats.at[2], rs=12, ag=30, st=6, xg=e_xg, acc=e_acc, ss=e_ss,
        cos=e_cos, sin=e_sin, hid=e_hid, q=e_q, kv=e_kv, kv_base=0,
    )

    def reduce_moves(p, trim):
        mid = p.count // 2
        top_rows = pl.ds(p.base + trim, mid - trim)
        low_rows = pl.ds(p.base + mid + trim, mid - trim)
        cut = pl.ds(trim, mid - trim)
        spec = (
            (p.terms.at[2, top_rows], along_x),
            (p.terms.at[2, low_rows], along_y),
            (p.terms.at[0, top_rows], along_x),
            (p.terms.at[1, low_rows], along_y),
            (p.passed.at[1, cut], along_x),
            (p.passed.at[0, cut], along_y),
        )
        return [
            remote(
                source, p.landed.at[i, cut], out_sem.at[p.rs // 6], ag_recv.at[p.rs + i], device
            )
            for i, (source, device) in enumerate(spec)
        ]

    def gather2(p, trim):
        mid = p.count // 2
        top_rows = pl.ds(p.base + trim, mid - trim)
        low_rows = pl.ds(p.base + mid + trim, mid - trim)
        spec = (
            (0, 1, top_rows, along_x),
            (0, 2, low_rows, along_y),
            (0, 1, low_rows, along_x),
            (0, 2, top_rows, along_y),
            (1, 3, top_rows, along_y),
            (2, 3, low_rows, along_x),
        )
        return [
            remote(
                p.proj.at[source, span], p.proj.at[target, span],
                out_sem.at[p.ag // 6], ag_recv.at[p.ag + i], device,
            )
            for i, (source, target, span, device) in enumerate(spec)
        ]

    def received(copy):
        copy.wait_recv()

    def each(make, p, picks, act):
        def run(trim):
            copies = make(p, trim)
            for i in picks:
                act(copies[i])

        if p.shared:
            pl.when(giver)(lambda: run(HANDED))
            pl.when(taker)(lambda: run(0))
        else:
            run(0)

    def product(bits, p):
        span = slice(p.base, p.base + p.count)
        value = jnp.dot(p.att[span, :], wo[bits], preferred_element_type=F32)
        if bits == 0:
            p.own[span, :] = value
        else:
            p.terms[bits - 1, span, :] = value.astype(BF16)

    def send_products(p):
        product(3, p)
        each(reduce_moves, p, (0, 1), launch)
        product(1, p)
        each(reduce_moves, p, (2,), launch)
        product(2, p)
        each(reduce_moves, p, (3,), launch)
        product(0, p)

    def pass_on(p):
        mid = p.count // 2
        each(reduce_moves, p, (0,), received)
        p.passed[0] = (
            p.terms[1, p.base : p.base + mid].astype(F32) + p.landed[0].astype(F32)
        ).astype(BF16)
        each(reduce_moves, p, (5,), launch)
        each(reduce_moves, p, (1,), received)
        p.passed[1] = (
            p.terms[0, p.base + mid : p.base + p.count].astype(F32) + p.landed[1].astype(F32)
        ).astype(BF16)
        each(reduce_moves, p, (4,), launch)

    def swaps(p):
        return [
            remote(
                p.mine, p.stats.at[bits - 1],
                st_send.at[p.st // 3], st_recv.at[p.st + bits - 1], peers[bits],
            )
            for bits in (3, 1, 2)
        ]

    def finalize(p):
        each(reduce_moves, p, (2, 3, 5, 4), received)
        span = slice(p.base, p.base + p.count)
        lanes = None
        for j in range(chunks):
            cut = slice(j * HEAD_DIM, (j + 1) * HEAD_DIM)
            above = p.landed[2, :, cut].astype(F32) + p.landed[5, :, cut].astype(F32)
            below = p.landed[3, :, cut].astype(F32) + p.landed[4, :, cut].astype(F32)
            value = p.own[span, cut] + jnp.concatenate([above, below], axis=0)
            p.own[span, cut] = value
            p.proj[0, span, cut] = value.astype(BF16)
            lanes = value * value if lanes is None else lanes + value * value
        each(gather2, p, (0, 1), launch)
        if p.count < block:
            lanes = jnp.concatenate([lanes, jnp.zeros((block - p.count, HEAD_DIM), F32)], axis=0)
        p.mine[...] = lax.dot_general(
            ones, lanes, (((1,), (1,)), ((), ())), precision=highest, preferred_element_type=F32
        )
        for swap in swaps(p):
            swap.start()

    def forward_rows(p):
        each(gather2, p, (0,), received)
        each(gather2, p, (4,), launch)
        each(gather2, p, (1,), received)
        each(gather2, p, (5,), launch)

    def post_factor(p):
        for swap in swaps(p):
            swap.wait_recv()
        summed = p.mine[...] + p.stats[0] + p.stats[1] + p.stats[2]
        column = lax.dot_general(
            summed, ones * 0.125, (((0,), (0,)), ((), ())), precision=highest,
            preferred_element_type=F32,
        )
        return lax.rsqrt(column[0 : p.count] * (1.0 / D) + NORM_EPS)

    def take2(slot, p, factor):
        arrivals = ((), (2,), (3,), (4, 5))[slot]
        each(gather2, p, arrivals, received)
        span = slice(p.base, p.base + p.count)
        squares = None
        for j in range(chunks):
            cut = slice(j * HEAD_DIM, (j + 1) * HEAD_DIM)
            summed = p.own[span, cut] if slot == 0 else p.proj[slot, span, cut].astype(F32)
            added = p.tok[slot, span, cut].astype(F32) + summed * factor * gain_row(1, slot, j)
            rounded = added.astype(BF16)
            if slot == 0:
                p.hid[span, cut] = rounded
            wide = rounded.astype(F32)
            squares = wide * wide if squares is None else squares + wide * wide
            p.xg[:, cut] = (wide * gain_row(2, slot, j)).astype(BF16)
        if slot == 0:
            p.ss[...] = squares
        else:
            p.ss[...] += squares
        if p is soon:
            for copy in second_loads[slot]:
                copy.wait()
        for begin, width in ((0, kvc), (kvc, qc)):
            value = jnp.dot(
                p.xg[...], w[slot, :, begin : begin + width], preferred_element_type=F32
            )
            if slot == 0:
                p.acc[:, begin : begin + width] = value
            else:
                p.acc[:, begin : begin + width] += value

    def finish2(p):
        span = slice(p.base, p.base + p.count)
        place_rows = slice(p.kv_base, p.kv_base + p.count)
        factor = row_factor(p.ss[...])

        def spun(begin):
            u = p.acc[:, begin : begin + HEAD_DIM] * factor
            turned = pltpu.roll(u, HEAD_DIM // 2, 1)
            return (u * p.cos[span, :] + turned * p.sin[span, :]).astype(BF16)

        for h in range(kv_heads):
            p.kv[0, h, place_rows, :] = spun(h * HEAD_DIM)
            place = kc + h * HEAD_DIM
            p.kv[1, h, place_rows, :] = (p.acc[:, place : place + HEAD_DIM] * factor).astype(BF16)
        for h in range(heads):
            p.q[h, span, :] = spun(kvc + h * HEAD_DIM)

    tail = remote(
        kv2.at[:, :, pl.ds(rows, WINDOW)], kv2.at[:, :, pl.ds(0, WINDOW)],
        tail_sem.at[0], tail_sem.at[1], {"seq": s + 1},
    )

    def scoped(name, run, *given):
        with jax.named_scope(name):
            return run(*given)

    def drain_early():
        def drain_level(k, carry):
            owner = s - 2 * k

            @pl.when(z < levels - 2)
            def _():
                all_sent(whole_block(owner, kv_heads), up_sem.at[owner // 2])

            @pl.when(helper)
            def _():
                all_sent(whole_block(owner, keep), up_sem.at[owner // 2])

            @pl.when(has_up & ((k > 0) | (c == 0) | helper))
            def _():
                all_sent(whole_block(owner, kv_heads), side_sem.at[owner // 2])

            @pl.when(top & (k > 0))
            def _():
                all_sent(whole_block(owner, keep), side_sem.at[owner // 2])

            @pl.when(top & (k == 0) & (c == 0))
            def _():
                all_sent(whole_block(owner, kv_heads), side_sem.at[owner // 2])

            return carry

        lax.fori_loop(0, z + 1, drain_level, 0)

        @pl.when(helper)
        def _():
            for copy in backs:
                copy.wait_send()

        @pl.when(top)
        def _():
            for part in range(2):
                query_down(part).wait_send()


    def drain_one(p, store, at):
        def run(trim):
            span = pl.ds(p.base, p.count - 2 * trim)
            all_sent(store.at[pl.ds(0, 3), span], out_sem.at[at // 6])

        if p.shared:
            pl.when(giver)(lambda: run(HANDED))
            pl.when(taker)(lambda: run(0))
        else:
            run(0)

    def drain_pair(p):
        drain_one(p, p.terms, p.rs)
        if p is not late:
            drain_one(p, p.proj, p.ag)
            all_sent(p.stats, st_send.at[p.st // 3])

    for copy in wo_loads:
        copy.wait()

    def drain_moves(part, carry):
        begin = pl.multiple_of(part * chunk_rows, chunk_rows)
        all_sent(buf.at[pl.ds(0, 3), pl.ds(begin, chunk_rows)], out_sem.at[part])
        return carry

    lax.fori_loop(0, PARTS, drain_moves, 0)
    scoped("write_part", write_part, 1)
    scoped("send_products", send_products, soon)
    fetch(0)
    scoped("write_part", write_part, 0)

    @pl.when(giver)
    def _():
        for copy in (*att_hands, *token_hands):
            copy.start()

    for bits in (3, 1, 2, 0):
        product(bits, late)
    scoped("pass_on", pass_on, soon)
    each(reduce_moves, late, (0, 1, 2, 3), launch)
    fetch(1)
    fetch(2)
    fetch(3)
    with jax.named_scope("early_drain"):
        drain_early()
    scoped("finalize", finalize, soon)
    each(gather2, soon, (2, 3), launch)
    scoped("pass_on", pass_on, late)
    factor = scoped("post_factor", post_factor, soon)

    @pl.when(taker)
    def _():
        with jax.named_scope("extra_products"):
            for copy in att_hands:
                copy.wait_recv()
            send_products(extra)

    scoped("take2", take2, 0, soon, factor)
    scoped("forward_rows", forward_rows, soon)
    scoped("take2", take2, 1, soon, factor)
    scoped("take2", take2, 2, soon, factor)

    @pl.when(giver)
    def _():
        scoped("finalize", finalize, late)
        each(gather2, late, (2, 3), launch)

    @pl.when(taker)
    def _():
        scoped("extra_pass_on", pass_on, extra)

    scoped("take2", take2, 3, soon, factor)
    scoped("finish2", finish2, soon)

    @pl.when(next_row)
    def _():
        tail.start()

    @pl.when(s == 0)
    def _():
        kv2[:, :, 0:WINDOW, :] = jnp.zeros((2, kv_heads, WINDOW, HEAD_DIM), BF16)

    @pl.when(taker)
    def _():
        scoped("extra_finalize", finalize, extra)
        each(gather2, extra, (2, 3), launch)
        scoped("finalize", finalize, late)
        scoped("extra_forward", forward_rows, extra)
        each(gather2, late, (2, 3), launch)
        with jax.named_scope("extra_take"):
            for copy in token_hands:
                copy.wait_recv()
            extra_factor = post_factor(extra)
            for slot in range(3):
                take2(slot, extra, extra_factor)
                if slot == 0:
                    returns[0].start()
            e_factor[...] = extra_factor

    scoped("forward_rows", forward_rows, late)

    @pl.when(taker)
    def _():
        with jax.named_scope("extra_last"):
            take2(3, extra, e_factor[...])
            finish2(extra)
            for copy in returns[1:]:
                copy.start()
            drain_pair(extra)

    drain_pair(soon)

    @pl.when(giver)
    def _():
        for copy in (*token_hands, *att_hands):
            copy.wait_send()

    factor = scoped("post_factor", post_factor, late)
    scoped("take2", take2, 0, late, factor)

    scoped("take2", take2, 1, late, factor)
    scoped("take2", take2, 2, late, factor)
    drain_pair(late)
    scoped("take2", take2, 3, late, factor)
    scoped("finish2", finish2, late)

    @pl.when(giver)
    def _():
        with jax.named_scope("extra_return"):
            for copy in returns:
                copy.wait_recv()
            for i in range(2):
                here = slice(i * half, i * half + HANDED)
                there = slice(i * HANDED, (i + 1) * HANDED)
                kv_here = slice(WINDOW + i * half, WINDOW + i * half + HANDED)
                hidden_ref[here, :] = r_hid[there, :]
                lq_ref[:, here, :] = r_q[:, there, :]
                kv2[:, :, kv_here, :] = r_kv[:, :, there, :]

    @pl.when(prev_row)
    def _():
        with jax.named_scope("tail_wait"):
            tail.wait_recv()

    with jax.named_scope("drain"):
        drain_one(late, proj, late.ag)
        all_sent(late.stats, st_send.at[late.st // 3])

        @pl.when(taker)
        def _():
            for copy in returns:
                copy.wait_send()

    @pl.when(next_row)
    def _():
        tail.wait_send()


def fused(x, gains, first, wo, second, count, collective_id):
    rows, cols = x.shape
    wq, wk, wv = first
    heads, kv_heads = wq.shape[1] // HEAD_DIM, wk.shape[1] // HEAD_DIM
    total = wq.shape[1] + 2 * wk.shape[1]
    depth = wo.shape[0]
    group, block, extra = heads // kv_heads, rows // 2, 2 * HANDED
    vmem = pl.BlockSpec(memory_space=VMEM)
    hbm = pl.BlockSpec(memory_space=pltpu.HBM)
    dma = pltpu.SemaphoreType.DMA
    folded = [gain.reshape(-1, HEAD_DIM) for gain in gains]
    turns = 10000.0 ** (-2.0 * np.arange(HEAD_DIM // 2) / HEAD_DIM)
    turns = np.concatenate([turns, turns])
    sign = np.where(np.arange(HEAD_DIM) < HEAD_DIM // 2, -1.0, 1.0)

    def table(places):
        angles = places[:, None] * turns
        return jnp.asarray(np.stack([np.cos(angles), sign * np.sin(angles)]), F32)

    tables = (table(np.arange(rows)), table(np.arange(count) * rows))
    far = [x, *folded, *tables, wq, wk, wv, wo, *second]
    far = [pltpu.with_memory_space_constraint(array, pltpu.HBM) for array in far]
    return pl.pallas_call(
        functools.partial(fused_kernel, count // 2, heads, kv_heads, kv_heads - 1),
        out_shape=(
            jax.ShapeDtypeStruct((rows, cols), BF16),
            jax.ShapeDtypeStruct((heads, rows, HEAD_DIM), BF16),
            jax.ShapeDtypeStruct((2, kv_heads, WINDOW + rows, HEAD_DIM), BF16),
        ),
        in_specs=[hbm] * 13,
        out_specs=(vmem, vmem, vmem),
        scratch_shapes=[
            VMEM((4, rows, cols), BF16),
            VMEM((4, cols, total), BF16),
            VMEM((4, depth, cols), BF16),
            VMEM((3,) + folded[0].shape, F32),
            VMEM((block, cols), BF16),
            VMEM((block, total), F32),
            VMEM((block, HEAD_DIM), F32),
            VMEM((rows, HEAD_DIM), F32),
            VMEM((heads, rows, HEAD_DIM), BF16),
            VMEM((count, 2, kv_heads, rows, HEAD_DIM), BF16),
            VMEM((heads, rows, HEAD_DIM), F32),
            VMEM((heads, rows, HEAD_DIM), F32),
            VMEM((rows, depth), BF16),
            VMEM((3, rows, cols), BF16),
            VMEM((rows, cols), F32),
            VMEM((2, 6, block // 2, cols), BF16),
            VMEM((2, 2, block // 2, cols), BF16),
            VMEM((4, rows, cols), BF16),
            VMEM((3, 8, block), F32),
            VMEM((3, 3, 8, block), F32),
            VMEM((rows, HEAD_DIM), F32),
            VMEM((rows, HEAD_DIM), F32),
            VMEM((2, rows, HEAD_DIM), F32),
            VMEM((2, count, HEAD_DIM), F32),
            VMEM((4, extra, cols), BF16),
            VMEM((extra, depth), BF16),
            VMEM((3, extra, cols), BF16),
            VMEM((extra, cols), F32),
            VMEM((6, HANDED, cols), BF16),
            VMEM((2, HANDED, cols), BF16),
            VMEM((4, extra, cols), BF16),
            VMEM((extra, cols), BF16),
            VMEM((extra, total), F32),
            VMEM((extra, HEAD_DIM), F32),
            VMEM((extra, HEAD_DIM), F32),
            VMEM((extra, HEAD_DIM), F32),
            VMEM((extra, HEAD_DIM), F32),
            VMEM((extra, cols), BF16),
            VMEM((heads, extra, HEAD_DIM), BF16),
            VMEM((2, kv_heads, extra, HEAD_DIM), BF16),
            VMEM((extra, cols), BF16),
            VMEM((heads, extra, HEAD_DIM), BF16),
            VMEM((2, kv_heads, extra, HEAD_DIM), BF16),
            VMEM((group, rows, HEAD_DIM), BF16),
            VMEM((group, rows, HEAD_DIM), F32),
            VMEM((group, rows, HEAD_DIM), F32),
            VMEM((group, rows, HEAD_DIM), BF16),
            VMEM((group, 8, rows), F32),
            VMEM((group, rows, HEAD_DIM), BF16),
            VMEM((group, 8, rows), F32),
            dma((PARTS,)),
            dma((5,)),
            dma((4, 3)),
            dma((4,)),
            dma((6,)),
            dma((max(6 * PARTS, 36),)),
            dma((count // 2,)),
            dma((count // 2,)),
            dma((count // 2 * (PARTS + 1),)),
            dma((3,)),
            dma((9,)),
            dma((2,)),
            dma((2,)),
            dma((2,)),
            dma((3,)),
            dma((3,)),
            dma((7,)),
            dma((7,)),
        ],
        compiler_params=pltpu.CompilerParams(
            collective_id=collective_id, has_side_effects=True, vmem_limit_bytes=50 * 2**20
        ),
        name="fused",
    )(*far)


def finish_kernel(hid_ref, q_ref, kv_ref, hid_hbm, o_hbm, o_ref, sems):
    rows = hid_ref.shape[0]
    heads, kv_heads = q_ref.shape[0], kv_ref.shape[1]
    group, block = heads // kv_heads, rows // 2
    begins = jnp.where(lax.axis_index("seq") > 0, 0, WINDOW - 1)
    copies = [pltpu.make_async_copy(hid_ref, hid_hbm, sems.at[kv_heads])]
    copies[0].start()
    for h in range(kv_heads):
        for part in range(2):
            q = q_ref[h * group : (h + 1) * group, part * block : (part + 1) * block]
            q = q.reshape(group * block, HEAD_DIM)
            keys = kv_ref[0, h, part * block : part * block + WINDOW + block]
            values = kv_ref[1, h, part * block : part * block + WINDOW + block]
            scores = lax.dot_general(
                q, keys, (((1,), (1,)), ((), ())), preferred_element_type=F32
            )
            weights = jnp.exp2(jnp.tanh(scores * INNER) * OUTER)
            row = lax.broadcasted_iota(jnp.int32, (block, WINDOW + block), 0)
            col = lax.broadcasted_iota(jnp.int32, (block, WINDOW + block), 1)
            least = jnp.maximum(row, begins) if part == 0 else row
            mask = (col > least) & (col <= row + WINDOW)
            weights = jnp.concatenate(
                [jnp.where(mask, weights[g * block : (g + 1) * block], 0.0) for g in range(group)],
                axis=0,
            )
            denominator = jnp.sum(weights, axis=-1, keepdims=True)
            numerator = jnp.dot(weights.astype(BF16), values, preferred_element_type=F32)
            result = (numerator / denominator).astype(BF16)
            for g in range(group):
                head = h * group + g
                o_ref[part * block : (part + 1) * block, head * HEAD_DIM : (head + 1) * HEAD_DIM] = (
                    result[g * block : (g + 1) * block]
                )
        lanes = pl.ds(h * group * HEAD_DIM, group * HEAD_DIM)
        copy = pltpu.make_async_copy(o_ref.at[:, lanes], o_hbm.at[:, lanes], sems.at[h])
        copy.start()
        copies.append(copy)
    for copy in copies:
        copy.wait()


def finish(hidden, q, kv):
    heads, rows, _ = q.shape
    vmem = pl.BlockSpec(memory_space=VMEM)
    hbm = pl.BlockSpec(memory_space=pltpu.HBM)
    shape = jax.ShapeDtypeStruct((rows, heads * HEAD_DIM), BF16)
    return pl.pallas_call(
        finish_kernel,
        out_shape=(jax.ShapeDtypeStruct(hidden.shape, BF16), shape),
        in_specs=[vmem] * 3,
        out_specs=(hbm, hbm),
        scratch_shapes=[
            VMEM(shape.shape, BF16),
            pltpu.SemaphoreType.DMA((kv.shape[1] + 1,)),
        ],
        compiler_params=pltpu.CompilerParams(vmem_limit_bytes=8 * 2**20),
        name="finish",
    )(hidden, q, kv)


def rms_scaled(values, weights):
    widened = values.astype(F32)
    factor = lax.rsqrt(jnp.mean(widened * widened, axis=-1, keepdims=True) + NORM_EPS)
    return widened * factor * weights


def plain_gather_project(x, gain, cos, sin, wq, wk, wv):
    full = lax.all_gather(x, "tp", axis=1, tiled=True)
    normed = rms_scaled(full, gain).astype(BF16)

    def heads_of(weight):
        product = jnp.dot(normed, weight, preferred_element_type=F32)
        return jnp.swapaxes(product.reshape(x.shape[0], -1, HEAD_DIM), 0, 1)

    def rotated(u):
        return (u * cos + jnp.roll(u, HEAD_DIM // 2, axis=-1) * sin).astype(BF16)

    keys, values = rotated(heads_of(wk)), heads_of(wv).astype(BF16)
    return rotated(heads_of(wq)), jnp.stack([keys, values])


def plain_output_project(attended, tokens, gain, wo):
    cols = tokens.shape[1]
    partial_sum = jnp.dot(attended, wo, preferred_element_type=F32).astype(BF16)
    summed = lax.psum(partial_sum, "tp").astype(F32)
    added = rms_scaled(summed, gain)
    mine = lax.dynamic_slice_in_dim(added, lax.axis_index("tp") * cols, cols, 1)
    return (tokens.astype(F32) + mine).astype(BF16)


def local(
    sizes,
    tokens,
    attention_gain,
    query_weight,
    key_weight,
    value_weight,
    output_weight,
    post_gain,
    local_gain,
    local_query_weight,
    local_key_weight,
    local_value_weight,
):
    seq, tp = sizes
    rows, cols = tokens.shape
    first = (query_weight, key_weight, value_weight)
    second = (local_query_weight, local_key_weight, local_value_weight)
    if tp == 4 and cols % HEAD_DIM == 0 and rows == 2 * WINDOW and seq % 4 == 0 and seq > 4:
        gains = (attention_gain, post_gain, local_gain)
        return finish(*fused(tokens, gains, first, output_weight, second, seq, 0))
    places = lax.axis_index("seq") * rows + lax.iota(jnp.int32, rows)
    halfway = HEAD_DIM // 2
    exponents = jnp.arange(halfway, dtype=F32) * (2.0 / HEAD_DIM)
    frequency = jnp.power(F32(10000.0), -exponents)
    angles = places.astype(F32)[:, None] * frequency[None, :]
    cosine, sine = jnp.cos(angles), jnp.sin(angles)
    cos = jnp.concatenate([cosine, cosine], axis=-1)
    sin = jnp.concatenate([-sine, sine], axis=-1)
    lead = plain_gather_project(tokens, attention_gain, cos, sin, *first)
    attended = causal_attention(*lead, seq, 1)
    hidden = plain_output_project(attended, tokens, post_gain, output_weight)
    lq, lkv = plain_gather_project(hidden, local_gain, cos, sin, *second)
    return hidden, window_attention(lq, lkv, seq, 4)


def solution(mesh):
    in_specs = (
        P("seq", "tp"),
        P(),
        P(None, "tp"),
        P(None, "tp"),
        P(None, "tp"),
        P("tp", None),
        P(),
        P(),
        P(None, "tp"),
        P(None, "tp"),
        P(None, "tp"),
    )
    out_specs = (P("seq", "tp"), P("seq", "tp"))
    sizes = (mesh.shape["seq"], mesh.shape["tp"])
    body = functools.partial(local, sizes)
    return jax.shard_map(body, mesh=mesh, in_specs=in_specs, out_specs=out_specs, check_vma=False)
```
